32 devices in a mesh: section: 2 (over x), shard: 4 (over z), rep: 4 (over y, core).
Axes of the slice: x: 2, y: 2, z: 4, core: 2. Of those that a mesh axis runs over, the one named last changes fastest.
Arguments:
- latents: bfloat16 [32, 256, 1152], P(('shard', 'rep')), may hold values from -81 to 81
- cond: bfloat16 [32, 1152], P(('shard', 'rep')), may hold values from -6 to 6
- modulation_weight: bfloat16 [2, 1152, 6912], P('section', 'shard'), may hold values from -0.1875 to 0.1875
- query_key_value_weight: bfloat16 [2, 1152, 3456], P('section', 'shard'), may hold values from -0.1875 to 0.1875
- attention_output_weight: bfloat16 [2, 1152, 1152], P('section', 'shard'), may hold values from -1.5 to 1.5
- feed_first_weight: bfloat16 [2, 1152, 4608], P('section', 'shard'), may hold values from -0.1875 to 0.1875
- feed_second_weight: bfloat16 [2, 4608, 1152], P('section', 'shard'), may hold values from -0.09375 to 0.09375
- cotangent: bfloat16 [32, 256, 1152], P(('shard', 'rep')), may hold values from -6 to 6
Outputs:
- boundary: float32 [2, 32, 256, 1152], P('section', ('shard', 'rep'))
- grad_cond: float32 [32, 1152], P(('shard', 'rep'))
- grad_ada: float32 [2, 1152, 6912], P('section', 'shard')
- grad_qkv: float32 [2, 1152, 3456], P('section', 'shard')
- grad_out: float32 [2, 1152, 1152], P('section', 'shard')
- grad_fc1: float32 [2, 1152, 4608], P('section', 'shard')
- grad_fc2: float32 [2, 4608, 1152], P('section', 'shard')
The draws below stay inside these ranges and needn't reach their ends.
All inputs are finite; a program needn't handle non-finite values.
Results may differ from the reference program's by a relative error of at most 0.03.
Values may be sent and summed in bfloat16 or wider, within the bound.
A program may use at most 384 MiB of HBM per device.

```python
import math
import jax
import jax.numpy as jnp
from jax import lax

D = 1152
HEADS = 16
HEAD_DIM = 72
FF = 4608
S = 256
LATENTS = 32


def draw_latents(key, part):
    row_key, col_key, base_key = jax.random.split(jax.random.fold_in(key, 11), 3)
    row_scale = jnp.exp(jax.random.uniform(row_key, (LATENTS, S, 1), jnp.float32) * math.log(10.0))
    col_scale = jnp.exp(jax.random.uniform(col_key, (1, 1, D), jnp.float32, -0.7, 0.7))
    base = jax.random.truncated_normal(base_key, -4.0, 4.0, (LATENTS, S, D), jnp.float32)
    return (base * row_scale * col_scale).astype(jnp.bfloat16)


def level_of(own_key, dims, cuts, least, high):
    def one(position, blocks):
        heights = jax.random.uniform(jax.random.fold_in(jax.random.fold_in(own_key, 6), position), (blocks,), jnp.float32, least / len(cuts), high / len(cuts))
        return jnp.repeat(jnp.exp(heights), dims[position] // blocks).reshape((-1,) + (1,) * (len(dims) - position - 1))

    level = one(*cuts[0])
    for cut in cuts[1:]:
        level = level * one(*cut)
    return level


def centred(stream_key, extent, width, reach, shards=(), kind=jnp.bfloat16):
    array = width * jax.random.normal(stream_key, extent, jnp.float32)
    if shards:
        array = array * level_of(stream_key, extent, shards, -0.22, 0.18)
    return jnp.clip(array, -reach, reach).astype(kind)


def setup_inputs(seed: int = 0) -> dict:
    key_list = jax.random.split(jax.random.key(seed), 9)
    latents = draw_latents(jax.random.fold_in(key_list[8], 71), 0)
    cond = centred(key_list[1], (LATENTS, D), 1.0, 6.0, ((0, 16),))
    modulation_weight = centred(key_list[2], (2, D, 6 * D), D ** -0.5, 0.1875, ((0, 2), (1, 4)))
    query_key_value_weight = centred(key_list[3], (2, D, 3 * D), D ** -0.5, 0.1875, ((0, 2), (1, 4)))
    attention_output_weight = centred(key_list[4], (2, D, D), (D // 64) ** -0.5, 1.5, ((0, 2), (1, 4)))
    feed_first_weight = centred(key_list[5], (2, D, FF), D ** -0.5, 0.1875, ((0, 2), (1, 4)))
    feed_second_weight = centred(key_list[6], (2, FF, D), FF ** -0.5, 0.09375, ((0, 2), (1, 4)))
    cotangent = centred(key_list[7], (LATENTS, S, D), 1.0, 6.0, ((0, 16),))
    return dict(latents=latents, cond=cond, modulation_weight=modulation_weight, query_key_value_weight=query_key_value_weight, attention_output_weight=attention_output_weight, feed_first_weight=feed_first_weight, feed_second_weight=feed_second_weight, cotangent=cotangent)


@jax.custom_vjp
def low(v):
    return lax.optimization_barrier(v.astype(jnp.bfloat16)).astype(jnp.float32)

@jax.custom_vjp
def low_back(v):
    return v

def low_keep(v):
    return (low(v), None)

def low_pass(kept, grad):
    return (grad,)

def back_keep(v):
    return (v, None)

def back_low(kept, grad):
    return (low(grad),)
low.defvjp(low_keep, low_pass)
low_back.defvjp(back_keep, back_low)
precise = lax.Precision.HIGHEST
epsilon = 1e-06

def norm_rows(values):
    center = values - lax.optimization_barrier(jnp.mean(values, axis=-1, keepdims=True))
    return center * lax.rsqrt(lax.optimization_barrier(jnp.mean(center * center, axis=-1, keepdims=True)) + epsilon)

def diffusion_block_layer(input_rows, condition_activation, modulation_weight, query_key_value_weight, attention_output_weight, feed_first_weight, feed_second_weight):
    batch_size, length, model_width = input_rows.shape
    modulation = low_back(jnp.dot(condition_activation, modulation_weight, precision=precise))[:, None, :]
    shift_one, scale_one, gate_one, shift_two, scale_two, gate_two = jnp.split(modulation, 6, axis=-1)
    first_in = low(norm_rows(input_rows) * (1.0 + scale_one) + shift_one)
    project = low_back(low(jnp.einsum('bsd,de->bse', first_in, query_key_value_weight, precision=precise)))
    project = project.reshape(batch_size, length, 3, HEADS, HEAD_DIM)
    queries = project[:, :, 0]
    keys_all = project[:, :, 1]
    values_all = project[:, :, 2]
    scores = jnp.einsum('bqhe,bkhe->bhqk', queries, keys_all, precision=precise) * HEAD_DIM ** (-0.5)
    scores = low_back(scores)
    attn_probs = low(jax.nn.softmax(scores, axis=-1))
    attended = jnp.einsum('bhqk,bkhe->bqhe', attn_probs, values_all, precision=precise)
    attended = low_back(low(attended.reshape(batch_size, length, model_width)))
    branch = low_back(jnp.einsum('bsd,de->bse', attended, attention_output_weight, precision=precise))
    middle_state = input_rows + gate_one * branch
    second_in = low(norm_rows(middle_state) * (1.0 + scale_two) + shift_two)
    hidden_pre = low_back(jnp.einsum('bsd,df->bsf', second_in, feed_first_weight, precision=precise))
    hidden = low(jax.nn.gelu(hidden_pre, approximate=True))
    feed_out = low_back(jnp.einsum('bsf,fd->bsd', hidden, feed_second_weight, precision=precise))
    return middle_state + gate_two * feed_out

def two_layers(input_rows, cond_in, parameter_list):
    condition_activation = low(jax.nn.silu(cond_in))
    middle_state = low_back(low(diffusion_block_layer(input_rows, condition_activation, *[parameter[0] for parameter in parameter_list])))
    return diffusion_block_layer(middle_state, condition_activation, *[parameter[1] for parameter in parameter_list])

def reference(latents, cond, modulation_weight, query_key_value_weight, attention_output_weight, feed_first_weight, feed_second_weight, cotangent):
    parameter_list = tuple((parameter.astype(jnp.float32) for parameter in (modulation_weight, query_key_value_weight, attention_output_weight, feed_first_weight, feed_second_weight)))
    group_size = math.gcd(LATENTS, 16)
    group_count = LATENTS // group_size
    input_rows = latents.astype(jnp.float32).reshape(group_count, group_size, S, D)
    conds = cond.astype(jnp.float32).reshape(group_count, group_size, D)
    cotans = cotangent.astype(jnp.float32).reshape(group_count, group_size, S, D)

    def accumulate(totals, pieces):
        part_in, part_cond, part_cot = pieces
        result, pullback = jax.vjp(two_layers, part_in, part_cond, parameter_list)
        grad_in, grad_cond, grad_params = pullback(part_cot)
        totals = tuple((total + extra for total, extra in zip(totals, grad_params)))
        return (totals, (result, grad_in, grad_cond))
    starting = tuple((jnp.zeros(parameter.shape, jnp.float32) for parameter in parameter_list))
    totals, (results, grads_in, grads_cond) = lax.scan(accumulate, starting, (input_rows, conds, cotans))
    boundary = jnp.stack([grads_in.reshape(LATENTS, S, D), results.reshape(LATENTS, S, D)])
    return (boundary, grads_cond.reshape(LATENTS, D), totals[0], totals[1], totals[2], totals[3], totals[4])
```

```python
import jax
import jax.numpy as jnp
from jax import lax
from jax.sharding import PartitionSpec as P

D = 1152
HEADS = 16
HEAD_DIM = 72
S = 256


epsilon = 1e-06
low = jnp.bfloat16


def center_scale(values):
    center = values - jnp.mean(values, axis=-1, keepdims=True)
    scale = lax.rsqrt(jnp.mean(center * center, axis=-1, keepdims=True) + epsilon)
    return center * scale, scale


def norm_back(normed, scale, grad):
    mean_grad = jnp.mean(grad, axis=-1, keepdims=True)
    mean_dot = jnp.mean(grad * normed, axis=-1, keepdims=True)
    return (grad - mean_grad - normed * mean_dot) * scale


def gelu_tanh(values):
    return jax.nn.gelu(values, approximate=True)


def matmul(left, right):
    return jnp.dot(left, right, preferred_element_type=jnp.float32)


def matmul_t(left, right):
    return lax.dot_general(
        left, right, (((1,), (1,)), ((), ())), preferred_element_type=jnp.float32
    )


def forward_layer(input_rows, modulation, weights):
    query_key_value_weight, attention_output_weight, feed_first_weight, feed_second_weight = weights
    batch_size, length, model_width = input_rows.shape
    tokens = batch_size * length
    shift_one, scale_one, gate_one, shift_two, scale_two, gate_two = modulation
    normed_one, inv_one = center_scale(input_rows)
    first_in = (normed_one * (1.0 + scale_one) + shift_one).astype(low).reshape(tokens, model_width)
    project = (
        matmul(first_in, query_key_value_weight)
        .astype(low)
        .reshape(batch_size, length, 3, HEADS, HEAD_DIM)
    )
    factor = HEAD_DIM ** (-0.5)
    scores = (
        jnp.einsum(
            "bqhe,bkhe->bhqk",
            project[:, :, 0],
            project[:, :, 1],
            preferred_element_type=jnp.float32,
        )
        * factor
    )
    attn_probs = jax.nn.softmax(scores, axis=-1)
    probs_low = attn_probs.astype(low)
    attended = jnp.einsum(
        "bhqk,bkhe->bqhe", probs_low, project[:, :, 2], preferred_element_type=jnp.float32
    )
    attended = attended.astype(low).reshape(tokens, model_width)
    branch = matmul(attended, attention_output_weight).reshape(batch_size, length, model_width)
    middle_state = input_rows + gate_one * branch
    normed_two, inv_two = center_scale(middle_state)
    second_in = (
        (normed_two * (1.0 + scale_two) + shift_two).astype(low).reshape(tokens, model_width)
    )
    hidden_pre = matmul(second_in, feed_first_weight)
    hidden = gelu_tanh(hidden_pre).astype(low)
    feed_out = matmul(hidden, feed_second_weight).reshape(batch_size, length, model_width)
    result = middle_state + gate_two * feed_out
    kept = (
        first_in,
        project,
        attn_probs,
        probs_low,
        attended,
        branch,
        middle_state,
        second_in,
        hidden_pre,
        hidden,
        feed_out,
    )
    return result, kept


def backward_layer(input_rows, modulation, weights, kept, grad_result):
    query_key_value_weight, attention_output_weight, feed_first_weight, feed_second_weight = weights
    (
        first_in,
        project,
        attn_probs,
        probs_low,
        attended,
        branch,
        middle_state,
        second_in,
        hidden_pre,
        hidden,
        feed_out,
    ) = kept
    batch_size, length, model_width = input_rows.shape
    tokens = batch_size * length
    shift_one, scale_one, gate_one, shift_two, scale_two, gate_two = modulation
    grad_gate_two = jnp.sum(grad_result * feed_out, axis=1)
    grad_feed = (gate_two * grad_result).astype(low).reshape(tokens, model_width)
    grad_hidden = matmul_t(grad_feed, feed_second_weight)
    _, gelu_back = jax.vjp(gelu_tanh, hidden_pre)
    grad_pre = gelu_back(grad_hidden)[0].astype(low)
    grad_second = matmul_t(grad_pre, feed_first_weight).reshape(batch_size, length, model_width)
    normed_two, inv_two = center_scale(middle_state)
    grad_shift_two = jnp.sum(grad_second, axis=1)
    grad_scale_two = jnp.sum(grad_second * normed_two, axis=1)
    grad_middle = grad_result + norm_back(normed_two, inv_two, grad_second * (1.0 + scale_two))
    grad_gate_one = jnp.sum(grad_middle * branch, axis=1)
    grad_branch = (gate_one * grad_middle).astype(low).reshape(tokens, model_width)
    grad_att = (
        matmul_t(grad_branch, attention_output_weight)
        .astype(low)
        .reshape(batch_size, length, HEADS, HEAD_DIM)
    )
    queries = project[:, :, 0]
    keys_all = project[:, :, 1]
    values_all = project[:, :, 2]
    grad_probs = jnp.einsum(
        "bqhe,bkhe->bhqk", grad_att, values_all, preferred_element_type=jnp.float32
    )
    grad_values = jnp.einsum(
        "bhqk,bqhe->bkhe", probs_low, grad_att, preferred_element_type=jnp.float32
    )
    grad_scores = attn_probs * (
        grad_probs - jnp.sum(grad_probs * attn_probs, axis=-1, keepdims=True)
    )
    grad_scores = grad_scores.astype(low)
    factor = HEAD_DIM ** (-0.5)
    grad_queries = (
        jnp.einsum("bhqk,bkhe->bqhe", grad_scores, keys_all, preferred_element_type=jnp.float32)
        * factor
    )
    grad_keys = (
        jnp.einsum("bhqk,bqhe->bkhe", grad_scores, queries, preferred_element_type=jnp.float32)
        * factor
    )
    grad_project = jnp.stack([grad_queries, grad_keys, grad_values], axis=2)
    grad_project = grad_project.astype(low).reshape(tokens, 3 * model_width)
    grad_first = matmul_t(grad_project, query_key_value_weight).reshape(
        batch_size, length, model_width
    )
    normed_one, inv_one = center_scale(input_rows)
    grad_shift_one = jnp.sum(grad_first, axis=1)
    grad_scale_one = jnp.sum(grad_first * normed_one, axis=1)
    grad_inputs = grad_middle + norm_back(normed_one, inv_one, grad_first * (1.0 + scale_one))
    grad_mod = jnp.concatenate(
        [
            grad_shift_one,
            grad_scale_one,
            grad_gate_one,
            grad_shift_two,
            grad_scale_two,
            grad_gate_two,
        ],
        axis=-1,
    ).astype(low)
    pairs = (
        (hidden, grad_feed),
        (second_in, grad_pre),
        (attended, grad_branch),
        (first_in, grad_project),
    )
    return grad_inputs, grad_mod, pairs


def bits_of(count):
    bits = count.bit_length() - 1
    assert 1 << bits == count
    return bits


def swap(value, axis, bit):
    count = lax.axis_size(axis)
    return lax.ppermute(value, axis, [(i, i ^ (1 << bit)) for i in range(count)])


def reduce_rows(left, right, reps_first):
    shard_bits = bits_of(lax.axis_size("shard"))
    rep_bits = bits_of(lax.axis_size("rep"))
    shard_stages = [("shard", bit) for bit in range(shard_bits)]
    rep_stages = [("rep", bit) for bit in range(rep_bits)]
    if reps_first:
        stages = rep_stages + shard_stages
    else:
        stages = rep_stages[:1] + shard_stages + rep_stages[1:]
    names = [("shard", bit) for bit in reversed(range(shard_bits))]
    names += [("rep", bit) for bit in reversed(range(rep_bits))]
    tokens, depth = left.shape
    inner = depth >> len(names)
    part = None
    for axis, bit in stages:
        place = names.index((axis, bit))
        mine = (lax.axis_index(axis) >> bit) & 1
        if part is None:
            spread = left.T.reshape((2,) * len(names) + (inner, tokens))
            away = lax.dynamic_index_in_dim(spread, 1 - mine, place, keepdims=False)
            stay = lax.dynamic_index_in_dim(spread, mine, place, keepdims=False)
            away = matmul(away.reshape(-1, tokens), right).astype(low)
            came = swap(away, axis, bit)
            part = (matmul(stay.reshape(-1, tokens), right) + came.astype(jnp.float32)).astype(low)
            names.pop(place)
            part = part.reshape((2,) * len(names) + (inner, right.shape[1]))
        else:
            away = lax.dynamic_index_in_dim(part, 1 - mine, place, keepdims=False)
            stay = lax.dynamic_index_in_dim(part, mine, place, keepdims=False)
            came = swap(away, axis, bit)
            part = (stay.astype(jnp.float32) + came.astype(jnp.float32)).astype(low)
            names.pop(place)
    whole = lax.all_gather(part, "rep", axis=0, tiled=True)
    return whole.astype(jnp.float32)


def exchange_shards(blocks):
    count = lax.axis_size("shard")
    me = lax.axis_index("shard")
    came = [lax.dynamic_index_in_dim(blocks, me, 0, keepdims=False)]
    for step in range(1, count):
        block = lax.dynamic_index_in_dim(blocks, (me + step) % count, 0, keepdims=False)
        came.append(
            lax.ppermute(block, "shard", [(i, (i + step) % count) for i in range(count)])
        )
    return came


def gather_rows(shard):
    reps = lax.axis_size("rep")
    rows = shard.shape[0] // reps
    own = lax.dynamic_slice_in_dim(shard, lax.axis_index("rep") * rows, rows, 0)
    return lax.all_gather(own, ("shard", "rep"), axis=0, tiled=True)


def body(
    latents,
    cond,
    modulation_weight,
    query_key_value_weight,
    attention_output_weight,
    feed_first_weight,
    feed_second_weight,
    cotangent,
):
    first_section = lax.axis_index("section") == 0
    shard = lax.axis_index("shard")
    rep = lax.axis_index("rep")
    shards = lax.axis_size("shard")
    reps = lax.axis_size("rep")
    batch = latents.shape[0]
    modulation_weight = modulation_weight[0]
    rows = modulation_weight.shape[0]

    cond_float = cond.astype(jnp.float32)
    act = jax.nn.silu(cond_float).astype(low)
    came = exchange_shards(act.reshape(batch, shards, rows).transpose(1, 0, 2))
    partial = matmul(jnp.concatenate(came, axis=0), modulation_weight)
    partial = partial.reshape(shards, batch, -1)
    total = partial[0]
    for step in range(1, shards):
        total = total + lax.ppermute(
            partial[step], "shard", [(i, (i - step) % shards) for i in range(shards)]
        )
    modulation = jnp.split(total[:, None, :], 6, axis=-1)

    weights = (
        gather_rows(query_key_value_weight[0]),
        gather_rows(attention_output_weight[0]),
        gather_rows(feed_first_weight[0]),
        gather_rows(feed_second_weight[0]),
    )

    early, _ = forward_layer(latents.astype(jnp.float32), modulation, weights)
    incoming = lax.ppermute(early.astype(low), "section", [(0, 1)])
    layer_in = jnp.where(first_section, latents, incoming).astype(jnp.float32)
    result, kept = forward_layer(layer_in, modulation, weights)
    own_cot = cotangent.astype(jnp.float32)
    early_grad, _, _ = backward_layer(layer_in, modulation, weights, kept, own_cot)
    returning = lax.ppermute(early_grad.astype(low), "section", [(1, 0)])
    grad_result = jnp.where(first_section, returning, cotangent).astype(jnp.float32)
    grad_in, grad_mod, pairs = backward_layer(layer_in, modulation, weights, kept, grad_result)
    grad_fc2 = reduce_rows(*pairs[0], True)
    grad_fc1 = reduce_rows(*pairs[1], False)
    grad_out = reduce_rows(*pairs[2], True)
    grad_qkv = reduce_rows(*pairs[3], True)

    boundary = jnp.where(first_section, grad_in, result)[None]

    packed = jnp.concatenate([grad_mod, act], axis=-1)
    packed = lax.all_gather(packed, ("shard", "rep"), axis=0, tiled=True)
    all_mod = packed[:, : grad_mod.shape[1]]
    all_act = packed[:, grad_mod.shape[1] :]
    act_rows = lax.dynamic_slice_in_dim(all_act, shard * rows, rows, 1)
    grad_ada = lax.dot_general(
        act_rows, all_mod, (((0,), (0,)), ((), ())), preferred_element_type=jnp.float32
    )
    own_mod = lax.dynamic_index_in_dim(
        all_mod.reshape(shards, reps, batch, -1), rep, 1, keepdims=False
    ).reshape(shards * batch, -1)
    act_grad = matmul_t(own_mod, modulation_weight)
    act_grad = act_grad + lax.ppermute(act_grad, "section", [(0, 1), (1, 0)])
    act_grad = lax.all_gather(act_grad.reshape(shards, batch, rows), "shard", axis=0)
    act_grad = lax.dynamic_index_in_dim(act_grad, shard, 1, keepdims=False)
    act_total = act_grad.transpose(1, 0, 2).reshape(batch, shards * rows)
    _, silu_back = jax.vjp(jax.nn.silu, cond_float)
    grad_cond = silu_back(act_total)[0]
    return (
        boundary,
        grad_cond,
        grad_ada[None],
        grad_qkv[None],
        grad_out[None],
        grad_fc1[None],
        grad_fc2[None],
    )


def solution(mesh):
    in_specs = (
        P(("shard", "rep"), None, None),
        P(("shard", "rep"), None),
        P("section", "shard", None),
        P("section", "shard", None),
        P("section", "shard", None),
        P("section", "shard", None),
        P("section", "shard", None),
        P(("shard", "rep"), None, None),
    )
    out_specs = (
        P("section", ("shard", "rep"), None, None),
        P(("shard", "rep"), None),
        P("section", "shard", None),
        P("section", "shard", None),
        P("section", "shard", None),
        P("section", "shard", None),
        P("section", "shard", None),
    )
    return jax.shard_map(body, mesh=mesh, in_specs=in_specs, out_specs=out_specs, check_vma=False)
```

```python
import functools

import jax
import jax.numpy as jnp
from jax import lax
from jax.experimental import pallas as pl
from jax.experimental.pallas import tpu as pltpu
from jax.sharding import PartitionSpec as P

D = 1152
HEADS = 16
HEAD_DIM = 72
LANES = 128


epsilon = 1e-06
low = jnp.bfloat16


NT=(((1,),(1,)),((),())); TN=(((0,),(0,)),((),()))
def dot(a,b,dims=(((1,),(0,)),((),()))):
    return lax.dot_general(a,b,dims,preferred_element_type=jnp.float32)
def windows():
    for head in range(HEADS):
        start=head*HEAD_DIM; stop=start+HEAD_DIM
        first=start//LANES*LANES; last=-(-stop//LANES)*LANES
        yield first,last,start-first,stop-first
def head_mask(rows,first,last,begin,end):
    lane=lax.broadcasted_iota(jnp.int32,(rows,last-first),1)
    return (lane>=begin)&(lane<end)
def attention_kernel(project_ref,out_ref):
    rows=out_ref.shape[0]
    for first,last,begin,end in windows():
        mask=head_mask(rows,first,last,begin,end)
        q=project_ref[:,first:last]; k=project_ref[:,D+first:D+last]; v=project_ref[:,2*D+first:2*D+last]
        q=jnp.where(mask,q,jnp.zeros_like(q))
        s=dot(q,k,NT)*(HEAD_DIM**-0.5)
        e=jnp.exp(s-jnp.max(s,axis=1,keepdims=True))
        p=(e/jnp.sum(e,axis=1,keepdims=True)).astype(low)
        o=dot(p,v).astype(low)
        out_ref[:,first:last]=jnp.where(mask,o,out_ref[:,first:last])
def attention_back_kernel(project_ref,grad_ref,out_ref):
    rows=grad_ref.shape[0]; factor=HEAD_DIM**-0.5
    for first,last,begin,end in windows():
        mask=head_mask(rows,first,last,begin,end)
        q=project_ref[:,first:last]; k=project_ref[:,D+first:D+last]; v=project_ref[:,2*D+first:2*D+last]
        g=grad_ref[:,first:last]
        s=dot(jnp.where(mask,k,jnp.zeros_like(k)),q,NT)*factor
        e=jnp.exp(s-jnp.max(s,axis=0,keepdims=True))
        p=e/jnp.sum(e,axis=0,keepdims=True)
        dp=dot(jnp.where(mask,v,jnp.zeros_like(v)),g,NT)
        ds=(p*(dp-jnp.sum(dp*p,axis=0,keepdims=True))).astype(low)
        dq=(dot(ds,k,TN)*factor).astype(low)
        dk=(dot(ds,q)*factor).astype(low)
        dv=dot(p.astype(low),g).astype(low)
        for base,piece in ((0,dq),(D,dk),(2*D,dv)):
            here=slice(base+first,base+last)
            out_ref[:,here]=jnp.where(mask,piece,out_ref[:,here])
def attention(project,length):
    tokens=project.shape[0]
    return pl.pallas_call(attention_kernel,grid=(tokens//length,),
        in_specs=[pl.BlockSpec((length,3*D),lambda i:(i,0))],out_specs=pl.BlockSpec((length,D),lambda i:(i,0)),
        out_shape=jax.ShapeDtypeStruct((tokens,D),low),
        cost_estimate=pl.CostEstimate(flops=4*tokens*length*D,bytes_accessed=8*tokens*D,transcendentals=HEADS*tokens*length))(project)
def attention_back(project,grad,length):
    tokens=project.shape[0]
    return pl.pallas_call(attention_back_kernel,grid=(tokens//length,),
        in_specs=[pl.BlockSpec((length,3*D),lambda i:(i,0)),pl.BlockSpec((length,D),lambda i:(i,0))],out_specs=pl.BlockSpec((length,3*D),lambda i:(i,0)),
        out_shape=jax.ShapeDtypeStruct((tokens,3*D),low),
        cost_estimate=pl.CostEstimate(flops=10*tokens*length*D,bytes_accessed=14*tokens*D,transcendentals=HEADS*tokens*length))(project,grad)

C0=0.7978845608028654; C1=0.044715
def mlp_kernel(x_ref,w1_ref,w2_ref,u_ref,h_ref,f_ref):
    u=dot(x_ref[...],w1_ref[...])
    u_ref[...]=u
    h=(0.5*u*(1.0+jnp.tanh(C0*(u+C1*(u*u*u))))).astype(low)
    h_ref[...]=h
    f=dot(h,w2_ref[...])
    first=pl.program_id(0)==0
    @pl.when(first)
    def _(): f_ref[...]=f
    @pl.when(jnp.logical_not(first))
    def _(): f_ref[...]+=f
def mlp_back_kernel(g_ref,w1_ref,w2_ref,u_ref,du_ref,dx_ref):
    dh=dot(g_ref[...],w2_ref[...],NT)
    u=u_ref[...]
    sq=u*u
    t=jnp.tanh(C0*(u+C1*(sq*u)))
    slope=0.5*(1.0+t)+0.5*u*(1.0-t*t)*(C0*(1.0+3.0*C1*sq))
    du=(dh*slope).astype(low)
    du_ref[...]=du
    dx=dot(du,w1_ref[...],NT)
    first=pl.program_id(0)==0
    @pl.when(first)
    def _(): dx_ref[...]=dx
    @pl.when(jnp.logical_not(first))
    def _(): dx_ref[...]+=dx
def tile_of(ff): return 768 if ff%768==0 else ff
def mlp(x,w1,w2,tile=None):
    t,d=x.shape; ff=w1.shape[1]; tile=tile or tile_of(ff)
    whole=pl.BlockSpec((t,d),lambda i:(0,0))
    cols=pl.BlockSpec((t,tile),lambda i:(0,i))
    return pl.pallas_call(mlp_kernel,grid=(ff//tile,),
        in_specs=[whole,pl.BlockSpec((d,tile),lambda i:(0,i)),pl.BlockSpec((tile,d),lambda i:(i,0))],
        out_specs=[cols,cols,whole],
        out_shape=[jax.ShapeDtypeStruct((t,ff),jnp.float32),jax.ShapeDtypeStruct((t,ff),low),jax.ShapeDtypeStruct((t,d),jnp.float32)],
        cost_estimate=pl.CostEstimate(flops=4*t*d*ff,bytes_accessed=4*d*ff+6*t*ff+6*t*d,transcendentals=t*ff))(x,w1,w2)
def mlp_back(g,w1,w2,u,tile=None):
    t,d=g.shape; ff=w1.shape[1]; tile=tile or tile_of(ff)
    whole=pl.BlockSpec((t,d),lambda i:(0,0))
    cols=pl.BlockSpec((t,tile),lambda i:(0,i))
    return pl.pallas_call(mlp_back_kernel,grid=(ff//tile,),
        in_specs=[whole,pl.BlockSpec((d,tile),lambda i:(0,i)),pl.BlockSpec((tile,d),lambda i:(i,0)),cols],
        out_specs=[cols,whole],
        out_shape=[jax.ShapeDtypeStruct((t,ff),low),jax.ShapeDtypeStruct((t,d),jnp.float32)],
        cost_estimate=pl.CostEstimate(flops=4*t*d*ff,bytes_accessed=4*d*ff+6*t*ff+6*t*d,transcendentals=t*ff))(g,w1,w2,u)


def center_scale(values):
    center = values - jnp.mean(values, axis=-1, keepdims=True)
    scale = lax.rsqrt(jnp.mean(center * center, axis=-1, keepdims=True) + epsilon)
    return center * scale, scale


def norm_back(normed, scale, grad):
    mean_grad = jnp.mean(grad, axis=-1, keepdims=True)
    mean_dot = jnp.mean(grad * normed, axis=-1, keepdims=True)
    return (grad - mean_grad - normed * mean_dot) * scale


def matmul(left, right):
    return jnp.dot(left, right, preferred_element_type=jnp.float32)


def matmul_t(left, right):
    return lax.dot_general(
        left, right, (((1,), (1,)), ((), ())), preferred_element_type=jnp.float32
    )


def forward_layer(input_rows, modulation, weights):
    query_key_value_weight, attention_output_weight, feed_first_weight, feed_second_weight = weights
    batch_size, length, model_width = input_rows.shape
    tokens = batch_size * length
    shift_one, scale_one, gate_one, shift_two, scale_two, gate_two = modulation
    normed_one, inv_one = center_scale(input_rows)
    first_in = (normed_one * (1.0 + scale_one) + shift_one).astype(low).reshape(tokens, model_width)
    project = matmul(first_in, query_key_value_weight).astype(low)
    attended = attention(project, length)
    branch = matmul(attended, attention_output_weight).reshape(batch_size, length, model_width)
    middle_state = input_rows + gate_one * branch
    normed_two, inv_two = center_scale(middle_state)
    second_in = (
        (normed_two * (1.0 + scale_two) + shift_two).astype(low).reshape(tokens, model_width)
    )
    hidden_pre, hidden, feed_out = mlp(second_in, feed_first_weight, feed_second_weight)
    feed_out = feed_out.reshape(batch_size, length, model_width)
    result = middle_state + gate_two * feed_out
    kept = (
        first_in,
        project,
        attended,
        branch,
        middle_state,
        second_in,
        hidden_pre,
        hidden,
        feed_out,
    )
    return result, kept


def backward_layer(input_rows, modulation, weights, kept, grad_result):
    query_key_value_weight, attention_output_weight, feed_first_weight, feed_second_weight = weights
    (
        first_in,
        project,
        attended,
        branch,
        middle_state,
        second_in,
        hidden_pre,
        hidden,
        feed_out,
    ) = kept
    batch_size, length, model_width = input_rows.shape
    tokens = batch_size * length
    shift_one, scale_one, gate_one, shift_two, scale_two, gate_two = modulation
    grad_gate_two = jnp.sum(grad_result * feed_out, axis=1)
    grad_feed = (gate_two * grad_result).astype(low).reshape(tokens, model_width)
    grad_pre, grad_second = mlp_back(
        grad_feed, feed_first_weight, feed_second_weight, hidden_pre
    )
    grad_second = grad_second.reshape(batch_size, length, model_width)
    normed_two, inv_two = center_scale(middle_state)
    grad_shift_two = jnp.sum(grad_second, axis=1)
    grad_scale_two = jnp.sum(grad_second * normed_two, axis=1)
    grad_middle = grad_result + norm_back(normed_two, inv_two, grad_second * (1.0 + scale_two))
    grad_gate_one = jnp.sum(grad_middle * branch, axis=1)
    grad_branch = (gate_one * grad_middle).astype(low).reshape(tokens, model_width)
    grad_att = matmul_t(grad_branch, attention_output_weight).astype(low)
    grad_project = attention_back(project, grad_att, length)
    grad_first = matmul_t(grad_project, query_key_value_weight).reshape(
        batch_size, length, model_width
    )
    normed_one, inv_one = center_scale(input_rows)
    grad_shift_one = jnp.sum(grad_first, axis=1)
    grad_scale_one = jnp.sum(grad_first * normed_one, axis=1)
    grad_inputs = grad_middle + norm_back(normed_one, inv_one, grad_first * (1.0 + scale_one))
    grad_mod = jnp.concatenate(
        [
            grad_shift_one,
            grad_scale_one,
            grad_gate_one,
            grad_shift_two,
            grad_scale_two,
            grad_gate_two,
        ],
        axis=-1,
    ).astype(low)
    pairs = (
        (hidden, grad_feed),
        (second_in, grad_pre),
        (attended, grad_branch),
        (first_in, grad_project),
    )
    return grad_inputs, grad_mod, pairs


def bits_of(count):
    bits = count.bit_length() - 1
    assert 1 << bits == count
    return bits


def swap(value, axis, bit):
    count = lax.axis_size(axis)
    return lax.ppermute(value, axis, [(i, i ^ (1 << bit)) for i in range(count)])


def reduce_rows(left, right, reps_first):
    shard_bits = bits_of(lax.axis_size("shard"))
    rep_bits = bits_of(lax.axis_size("rep"))
    shard_stages = [("shard", bit) for bit in range(shard_bits)]
    rep_stages = [("rep", bit) for bit in range(rep_bits)]
    if reps_first:
        stages = rep_stages + shard_stages
    else:
        stages = rep_stages[:1] + shard_stages + rep_stages[1:]
    names = [("shard", bit) for bit in reversed(range(shard_bits))]
    names += [("rep", bit) for bit in reversed(range(rep_bits))]
    tokens, depth = left.shape
    inner = depth >> len(names)
    part = None
    for axis, bit in stages:
        place = names.index((axis, bit))
        mine = (lax.axis_index(axis) >> bit) & 1
        if part is None:
            spread = left.T.reshape((2,) * len(names) + (inner, tokens))
            away = lax.dynamic_index_in_dim(spread, 1 - mine, place, keepdims=False)
            stay = lax.dynamic_index_in_dim(spread, mine, place, keepdims=False)
            away = matmul(away.reshape(-1, tokens), right).astype(low)
            came = swap(away, axis, bit)
            part = (matmul(stay.reshape(-1, tokens), right) + came.astype(jnp.float32)).astype(low)
            names.pop(place)
            part = part.reshape((2,) * len(names) + (inner, right.shape[1]))
        else:
            away = lax.dynamic_index_in_dim(part, 1 - mine, place, keepdims=False)
            stay = lax.dynamic_index_in_dim(part, mine, place, keepdims=False)
            came = swap(away, axis, bit)
            part = (stay.astype(jnp.float32) + came.astype(jnp.float32)).astype(low)
            names.pop(place)
    whole = lax.all_gather(part, "rep", axis=0, tiled=True)
    return whole.astype(jnp.float32)


def exchange_shards(blocks):
    count = lax.axis_size("shard")
    me = lax.axis_index("shard")
    came = [lax.dynamic_index_in_dim(blocks, me, 0, keepdims=False)]
    for step in range(1, count):
        block = lax.dynamic_index_in_dim(blocks, (me + step) % count, 0, keepdims=False)
        came.append(
            lax.ppermute(block, "shard", [(i, (i + step) % count) for i in range(count)])
        )
    return came


MESH=pl.DeviceIdType.MESH

def gather_kernel(shards,reps,count,*refs):
    ins=refs[:count]; outs=refs[count:2*count]; bounce=refs[2*count:3*count]
    line_send,line_recv,rep_send,rep_recv,local_in,local_out=refs[3*count:]
    s=lax.axis_index("shard"); r=lax.axis_index("rep")
    bits=reps.bit_length()-1
    barrier=pltpu.get_barrier_semaphore()
    for side in (-1,1):
        there=(s+side>=0)&(s+side<shards)
        @pl.when(there)
        def _():
            pl.semaphore_signal(barrier,inc=1,device_id={"shard":s+side},device_id_type=MESH)
    for bit in range(bits):
        pl.semaphore_signal(barrier,inc=1,device_id={"rep":r^(1<<bit)},device_id_type=MESH)
    for c in range(count):
        pltpu.make_async_copy(ins[c],bounce[c],local_in.at[c]).start()
    pl.semaphore_wait(barrier,bits+jnp.minimum(s,1)+jnp.minimum(shards-1-s,1))
    sides=((0,1),(1,-1))

    def line(way,step,hop,c,owner):
        src=ins[c].at[r] if hop==0 else outs[c].at[owner,r]
        return pltpu.make_async_remote_copy(src_ref=src,dst_ref=outs[c].at[owner,r],
            send_sem=line_send.at[way,hop,c],recv_sem=line_recv.at[way,hop,c],
            device_id={"shard":s+step},device_id_type=MESH)
    def side_copy(bit,mask,c,owner):
        piece=outs[c].at[owner,r^mask]
        return pltpu.make_async_remote_copy(src_ref=piece,dst_ref=piece,
            send_sem=rep_send.at[bit,mask,owner,c],recv_sem=rep_recv.at[mask|(1<<bit),owner,c],
            device_id={"rep":r^(1<<bit)},device_id_type=MESH)
    def low_bit(mask): return bits if mask==0 else (mask&-mask).bit_length()-1
    def arrived(mask,c,owner):
        bit=low_bit(mask)
        piece=outs[c].at[owner,r^mask]
        pltpu.make_async_remote_copy(src_ref=piece,dst_ref=piece,send_sem=rep_send.at[bit,mask^(1<<bit),owner,c],
            recv_sem=rep_recv.at[mask,owner,c],device_id={"rep":r^(1<<bit)},device_id_type=MESH).wait_recv()
    for c in range(count):
        for way,step in sides:
            @pl.when((s+step>=0)&(s+step<shards))
            def _(): line(way,step,0,c,s).start()
    for c in range(count):
        pltpu.make_async_copy(ins[c],bounce[c],local_in.at[c]).wait()
        pltpu.make_async_copy(bounce[c],outs[c].at[s],local_out.at[c]).start()
    events=[(hop,c) for hop in range(1,shards) for c in range(count)]
    relays=[m for m in range(1,reps) if low_bit(m)>0]
    depth=max([m.bit_count() for m in relays],default=0)
    for index in range(len(events)+depth):
        if index<len(events):
            hop,c=events[index]
            for way,step in sides:
                owner=s-step*hop
                @pl.when((owner>=0)&(owner<shards))
                def _():
                    line(way,step,hop-1,c,owner).wait_recv()
                    if hop+1<shards:
                        @pl.when((s+step>=0)&(s+step<shards))
                        def _(): line(way,step,hop,c,owner).start()
                    for bit in reversed(range(bits)):
                        side_copy(bit,0,c,owner).start()
        for mask in relays:
            late=index-mask.bit_count()
            if 0<=late<len(events):
                hop,c=events[late]
                for way,step in sides:
                    owner=s-step*hop
                    @pl.when((owner>=0)&(owner<shards))
                    def _():
                        arrived(mask,c,owner)
                        for bit in reversed(range(low_bit(mask))):
                            side_copy(bit,mask,c,owner).start()
    for hop,c in events:
        for way,step in sides:
            owner=s-step*hop
            @pl.when((owner>=0)&(owner<shards))
            def _():
                for mask in range(1,reps):
                    if low_bit(mask)==0: arrived(mask,c,owner)
                for mask in range(reps):
                    for bit in range(low_bit(mask)): side_copy(bit,mask,c,owner).wait_send()
                if hop+1<shards:
                    @pl.when((s+step>=0)&(s+step<shards))
                    def _(): line(way,step,hop,c,owner).wait_send()
    for c in range(count):
        for way,step in sides:
            @pl.when((s+step>=0)&(s+step<shards))
            def _(): line(way,step,0,c,s).wait_send()
        pltpu.make_async_copy(bounce[c],outs[c].at[s],local_out.at[c]).wait()

def gather_all(weights):
    shards=lax.axis_size("shard"); reps=lax.axis_size("rep"); bits=reps.bit_length()-1
    assert 1<<bits==reps
    count=len(weights)
    views=[w.reshape(reps,w.shape[0]//reps,w.shape[1]) for w in weights]
    any_=pl.BlockSpec(memory_space=pl.ANY)
    outs=pl.pallas_call(functools.partial(gather_kernel,shards,reps,count),
        in_specs=[any_]*count,out_specs=[any_]*count,
        out_shape=[jax.ShapeDtypeStruct((shards,)+v.shape,v.dtype) for v in views],
        scratch_shapes=[pltpu.VMEM(v.shape,v.dtype) for v in views]+[
            pltpu.SemaphoreType.DMA((2,shards-1,count)),pltpu.SemaphoreType.DMA((2,shards-1,count)),
            pltpu.SemaphoreType.DMA((bits,reps,shards,count)),pltpu.SemaphoreType.DMA((reps,shards,count)),
            pltpu.SemaphoreType.DMA((count,)),pltpu.SemaphoreType.DMA((count,))],
        compiler_params=pltpu.CompilerParams(collective_id=1,has_side_effects=True),
        )(*views)
    return tuple(o.reshape(shards*w.shape[0],w.shape[1]) for o,w in zip(outs,weights))


def body(
    latents,
    cond,
    modulation_weight,
    query_key_value_weight,
    attention_output_weight,
    feed_first_weight,
    feed_second_weight,
    cotangent,
):
    first_section = lax.axis_index("section") == 0
    shard = lax.axis_index("shard")
    rep = lax.axis_index("rep")
    shards = lax.axis_size("shard")
    reps = lax.axis_size("rep")
    batch = latents.shape[0]
    modulation_weight = modulation_weight[0]
    rows = modulation_weight.shape[0]

    cond_float = cond.astype(jnp.float32)
    act = jax.nn.silu(cond_float).astype(low)
    came = exchange_shards(act.reshape(batch, shards, rows).transpose(1, 0, 2))
    partial = matmul(jnp.concatenate(came, axis=0), modulation_weight)
    partial = partial.reshape(shards, batch, -1)
    total = partial[0]
    for step in range(1, shards):
        total = total + lax.ppermute(
            partial[step], "shard", [(i, (i - step) % shards) for i in range(shards)]
        )
    modulation = jnp.split(total[:, None, :], 6, axis=-1)

    weights = gather_all(
        (
            query_key_value_weight[0],
            attention_output_weight[0],
            feed_first_weight[0],
            feed_second_weight[0],
        )
    )

    early, _ = forward_layer(latents.astype(jnp.float32), modulation, weights)
    incoming = lax.ppermute(early.astype(low), "section", [(0, 1)])
    layer_in = jnp.where(first_section, latents, incoming).astype(jnp.float32)
    result, kept = forward_layer(layer_in, modulation, weights)
    own_cot = cotangent.astype(jnp.float32)
    early_grad, _, _ = backward_layer(layer_in, modulation, weights, kept, own_cot)
    returning = lax.ppermute(early_grad.astype(low), "section", [(1, 0)])
    grad_result = jnp.where(first_section, returning, cotangent).astype(jnp.float32)
    grad_in, grad_mod, pairs = backward_layer(layer_in, modulation, weights, kept, grad_result)
    grad_fc2 = reduce_rows(*pairs[0], True)
    grad_fc1 = reduce_rows(*pairs[1], False)
    grad_out = reduce_rows(*pairs[2], True)
    grad_qkv = reduce_rows(*pairs[3], True)

    boundary = jnp.where(first_section, grad_in, result)[None]

    packed = jnp.concatenate([grad_mod, act], axis=-1)
    packed = lax.all_gather(packed, ("shard", "rep"), axis=0, tiled=True)
    all_mod = packed[:, : grad_mod.shape[1]]
    all_act = packed[:, grad_mod.shape[1] :]
    act_rows = lax.dynamic_slice_in_dim(all_act, shard * rows, rows, 1)
    grad_ada = lax.dot_general(
        act_rows, all_mod, (((0,), (0,)), ((), ())), preferred_element_type=jnp.float32
    )
    own_mod = lax.dynamic_index_in_dim(
        all_mod.reshape(shards, reps, batch, -1), rep, 1, keepdims=False
    ).reshape(shards * batch, -1)
    act_grad = matmul_t(own_mod, modulation_weight)
    act_grad = act_grad + lax.ppermute(act_grad, "section", [(0, 1), (1, 0)])
    act_grad = lax.all_gather(act_grad.reshape(shards, batch, rows), "shard", axis=0)
    act_grad = lax.dynamic_index_in_dim(act_grad, shard, 1, keepdims=False)
    act_total = act_grad.transpose(1, 0, 2).reshape(batch, shards * rows)
    _, silu_back = jax.vjp(jax.nn.silu, cond_float)
    grad_cond = silu_back(act_total)[0]
    return (
        boundary,
        grad_cond,
        grad_ada[None],
        grad_qkv[None],
        grad_out[None],
        grad_fc1[None],
        grad_fc2[None],
    )


def solution(mesh):
    in_specs = (
        P(("shard", "rep"), None, None),
        P(("shard", "rep"), None),
        P("section", "shard", None),
        P("section", "shard", None),
        P("section", "shard", None),
        P("section", "shard", None),
        P("section", "shard", None),
        P(("shard", "rep"), None, None),
    )
    out_specs = (
        P("section", ("shard", "rep"), None, None),
        P(("shard", "rep"), None),
        P("section", "shard", None),
        P("section", "shard", None),
        P("section", "shard", None),
        P("section", "shard", None),
        P("section", "shard", None),
    )
    return jax.shard_map(body, mesh=mesh, in_specs=in_specs, out_specs=out_specs, check_vma=False)
```

```python
import functools

import jax
import jax.numpy as jnp
from jax import lax
from jax.experimental import pallas as pl
from jax.experimental.pallas import tpu as pltpu
from jax.sharding import PartitionSpec as P

D = 1152
HEADS = 16
HEAD_DIM = 72
LANES = 128


epsilon = 1e-06
low = jnp.bfloat16


NT=(((1,),(1,)),((),())); TN=(((0,),(0,)),((),()))
def dot(a,b,dims=(((1,),(0,)),((),()))):
    return lax.dot_general(a,b,dims,preferred_element_type=jnp.float32)
def windows():
    for head in range(HEADS):
        start=head*HEAD_DIM; stop=start+HEAD_DIM
        first=start//LANES*LANES; last=-(-stop//LANES)*LANES
        yield first,last,start-first,stop-first
def head_mask(rows,first,last,begin,end):
    lane=lax.broadcasted_iota(jnp.int32,(rows,last-first),1)
    return (lane>=begin)&(lane<end)
def attention_kernel(project_ref,out_ref):
    rows=out_ref.shape[0]
    for first,last,begin,end in windows():
        mask=head_mask(rows,first,last,begin,end)
        q=project_ref[:,first:last]; k=project_ref[:,D+first:D+last]; v=project_ref[:,2*D+first:2*D+last]
        q=jnp.where(mask,q,jnp.zeros_like(q))
        s=dot(q,k,NT)*(HEAD_DIM**-0.5)
        e=jnp.exp(s-jnp.max(s,axis=1,keepdims=True))
        p=(e/jnp.sum(e,axis=1,keepdims=True)).astype(low)
        o=dot(p,v).astype(low)
        out_ref[:,first:last]=jnp.where(mask,o,out_ref[:,first:last])
def attention_back_kernel(project_ref,grad_ref,out_ref):
    rows=grad_ref.shape[0]; factor=HEAD_DIM**-0.5
    for first,last,begin,end in windows():
        mask=head_mask(rows,first,last,begin,end)
        q=project_ref[:,first:last]; k=project_ref[:,D+first:D+last]; v=project_ref[:,2*D+first:2*D+last]
        g=grad_ref[:,first:last]
        s=dot(jnp.where(mask,k,jnp.zeros_like(k)),q,NT)*factor
        e=jnp.exp(s-jnp.max(s,axis=0,keepdims=True))
        p=e/jnp.sum(e,axis=0,keepdims=True)
        dp=dot(jnp.where(mask,v,jnp.zeros_like(v)),g,NT)
        ds=(p*(dp-jnp.sum(dp*p,axis=0,keepdims=True))).astype(low)
        dq=(dot(ds,k,TN)*factor).astype(low)
        dk=(dot(ds,q)*factor).astype(low)
        dv=dot(p.astype(low),g).astype(low)
        for base,piece in ((0,dq),(D,dk),(2*D,dv)):
            here=slice(base+first,base+last)
            out_ref[:,here]=jnp.where(mask,piece,out_ref[:,here])
def attention(project,length):
    tokens=project.shape[0]
    return pl.pallas_call(attention_kernel,grid=(tokens//length,),
        in_specs=[pl.BlockSpec((length,3*D),lambda i:(i,0))],out_specs=pl.BlockSpec((length,D),lambda i:(i,0)),
        out_shape=jax.ShapeDtypeStruct((tokens,D),low),
        cost_estimate=pl.CostEstimate(flops=4*tokens*length*D,bytes_accessed=8*tokens*D,transcendentals=HEADS*tokens*length))(project)
def attention_back(project,grad,length):
    tokens=project.shape[0]
    return pl.pallas_call(attention_back_kernel,grid=(tokens//length,),
        in_specs=[pl.BlockSpec((length,3*D),lambda i:(i,0)),pl.BlockSpec((length,D),lambda i:(i,0))],out_specs=pl.BlockSpec((length,3*D),lambda i:(i,0)),
        out_shape=jax.ShapeDtypeStruct((tokens,3*D),low),
        cost_estimate=pl.CostEstimate(flops=10*tokens*length*D,bytes_accessed=14*tokens*D,transcendentals=HEADS*tokens*length))(project,grad)

C0=0.7978845608028654; C1=0.044715
def mlp_kernel(x_ref,w1_ref,w2_ref,u_ref,h_ref,f_ref):
    u=dot(x_ref[...],w1_ref[...])
    u_ref[...]=u
    h=(0.5*u*(1.0+jnp.tanh(C0*(u+C1*(u*u*u))))).astype(low)
    h_ref[...]=h
    f=dot(h,w2_ref[...])
    first=pl.program_id(0)==0
    @pl.when(first)
    def _(): f_ref[...]=f
    @pl.when(jnp.logical_not(first))
    def _(): f_ref[...]+=f
def mlp_back_kernel(g_ref,w1_ref,w2_ref,u_ref,du_ref,dx_ref):
    dh=dot(g_ref[...],w2_ref[...],NT)
    u=u_ref[...]
    sq=u*u
    t=jnp.tanh(C0*(u+C1*(sq*u)))
    slope=0.5*(1.0+t)+0.5*u*(1.0-t*t)*(C0*(1.0+3.0*C1*sq))
    du=(dh*slope).astype(low)
    du_ref[...]=du
    dx=dot(du,w1_ref[...],NT)
    first=pl.program_id(0)==0
    @pl.when(first)
    def _(): dx_ref[...]=dx
    @pl.when(jnp.logical_not(first))
    def _(): dx_ref[...]+=dx
def tile_of(ff): return 768 if ff%768==0 else ff
def mlp(x,w1,w2,tile=None):
    t,d=x.shape; ff=w1.shape[1]; tile=tile or tile_of(ff)
    whole=pl.BlockSpec((t,d),lambda i:(0,0))
    cols=pl.BlockSpec((t,tile),lambda i:(0,i))
    return pl.pallas_call(mlp_kernel,grid=(ff//tile,),
        in_specs=[whole,pl.BlockSpec((d,tile),lambda i:(0,i)),pl.BlockSpec((tile,d),lambda i:(i,0))],
        out_specs=[cols,cols,whole],
        out_shape=[jax.ShapeDtypeStruct((t,ff),jnp.float32),jax.ShapeDtypeStruct((t,ff),low),jax.ShapeDtypeStruct((t,d),jnp.float32)],
        cost_estimate=pl.CostEstimate(flops=4*t*d*ff,bytes_accessed=4*d*ff+6*t*ff+6*t*d,transcendentals=t*ff))(x,w1,w2)
def mlp_back(g,w1,w2,u,tile=None):
    t,d=g.shape; ff=w1.shape[1]; tile=tile or tile_of(ff)
    whole=pl.BlockSpec((t,d),lambda i:(0,0))
    cols=pl.BlockSpec((t,tile),lambda i:(0,i))
    return pl.pallas_call(mlp_back_kernel,grid=(ff//tile,),
        in_specs=[whole,pl.BlockSpec((d,tile),lambda i:(0,i)),pl.BlockSpec((tile,d),lambda i:(i,0)),cols],
        out_specs=[cols,whole],
        out_shape=[jax.ShapeDtypeStruct((t,ff),low),jax.ShapeDtypeStruct((t,d),jnp.float32)],
        cost_estimate=pl.CostEstimate(flops=4*t*d*ff,bytes_accessed=4*d*ff+6*t*ff+6*t*d,transcendentals=t*ff))(g,w1,w2,u)


def center_scale(values):
    center = values - jnp.mean(values, axis=-1, keepdims=True)
    scale = lax.rsqrt(jnp.mean(center * center, axis=-1, keepdims=True) + epsilon)
    return center * scale, scale


def norm_back(normed, scale, grad):
    mean_grad = jnp.mean(grad, axis=-1, keepdims=True)
    mean_dot = jnp.mean(grad * normed, axis=-1, keepdims=True)
    return (grad - mean_grad - normed * mean_dot) * scale


def matmul(left, right):
    return jnp.dot(left, right, preferred_element_type=jnp.float32)


def matmul_t(left, right):
    return lax.dot_general(
        left, right, (((1,), (1,)), ((), ())), preferred_element_type=jnp.float32
    )


def forward_layer(input_rows, modulation, weights):
    query_key_value_weight, attention_output_weight, feed_first_weight, feed_second_weight = weights
    batch_size, length, model_width = input_rows.shape
    tokens = batch_size * length
    shift_one, scale_one, gate_one, shift_two, scale_two, gate_two = modulation
    normed_one, inv_one = center_scale(input_rows)
    first_in = (normed_one * (1.0 + scale_one) + shift_one).astype(low).reshape(tokens, model_width)
    project = matmul(first_in, query_key_value_weight).astype(low)
    attended = attention(project, length)
    branch = matmul(attended, attention_output_weight).reshape(batch_size, length, model_width)
    middle_state = input_rows + gate_one * branch
    normed_two, inv_two = center_scale(middle_state)
    second_in = (
        (normed_two * (1.0 + scale_two) + shift_two).astype(low).reshape(tokens, model_width)
    )
    hidden_pre, hidden, feed_out = mlp(second_in, feed_first_weight, feed_second_weight)
    feed_out = feed_out.reshape(batch_size, length, model_width)
    result = middle_state + gate_two * feed_out
    kept = (
        first_in,
        project,
        attended,
        branch,
        middle_state,
        second_in,
        hidden_pre,
        hidden,
        feed_out,
    )
    return result, kept


def backward_layer(input_rows, modulation, weights, kept, grad_result):
    query_key_value_weight, attention_output_weight, feed_first_weight, feed_second_weight = weights
    (
        first_in,
        project,
        attended,
        branch,
        middle_state,
        second_in,
        hidden_pre,
        hidden,
        feed_out,
    ) = kept
    batch_size, length, model_width = input_rows.shape
    tokens = batch_size * length
    shift_one, scale_one, gate_one, shift_two, scale_two, gate_two = modulation
    grad_gate_two = jnp.sum(grad_result * feed_out, axis=1)
    grad_feed = (gate_two * grad_result).astype(low).reshape(tokens, model_width)
    grad_pre, grad_second = mlp_back(
        grad_feed, feed_first_weight, feed_second_weight, hidden_pre
    )
    grad_second = grad_second.reshape(batch_size, length, model_width)
    normed_two, inv_two = center_scale(middle_state)
    grad_shift_two = jnp.sum(grad_second, axis=1)
    grad_scale_two = jnp.sum(grad_second * normed_two, axis=1)
    grad_middle = grad_result + norm_back(normed_two, inv_two, grad_second * (1.0 + scale_two))
    grad_gate_one = jnp.sum(grad_middle * branch, axis=1)
    grad_branch = (gate_one * grad_middle).astype(low).reshape(tokens, model_width)
    grad_att = matmul_t(grad_branch, attention_output_weight).astype(low)
    grad_project = attention_back(project, grad_att, length)
    grad_first = matmul_t(grad_project, query_key_value_weight).reshape(
        batch_size, length, model_width
    )
    normed_one, inv_one = center_scale(input_rows)
    grad_shift_one = jnp.sum(grad_first, axis=1)
    grad_scale_one = jnp.sum(grad_first * normed_one, axis=1)
    grad_inputs = grad_middle + norm_back(normed_one, inv_one, grad_first * (1.0 + scale_one))
    grad_mod = jnp.concatenate(
        [
            grad_shift_one,
            grad_scale_one,
            grad_gate_one,
            grad_shift_two,
            grad_scale_two,
            grad_gate_two,
        ],
        axis=-1,
    ).astype(low)
    pairs = (
        (hidden, grad_feed),
        (second_in, grad_pre),
        (attended, grad_branch),
        (first_in, grad_project),
    )
    return grad_inputs, grad_mod, pairs


def bits_of(count):
    bits = count.bit_length() - 1
    assert 1 << bits == count
    return bits


def swap(value, axis, bit):
    count = lax.axis_size(axis)
    return lax.ppermute(value, axis, [(i, i ^ (1 << bit)) for i in range(count)])


def reduce_rows(left, right, reps_first):
    shard_bits = bits_of(lax.axis_size("shard"))
    rep_bits = bits_of(lax.axis_size("rep"))
    shard_stages = [("shard", bit) for bit in range(shard_bits)]
    rep_stages = [("rep", bit) for bit in range(rep_bits)]
    if reps_first:
        stages = rep_stages + shard_stages
    else:
        stages = rep_stages[:1] + shard_stages + rep_stages[1:]
    names = [("shard", bit) for bit in reversed(range(shard_bits))]
    names += [("rep", bit) for bit in reversed(range(rep_bits))]
    tokens, depth = left.shape
    inner = depth >> len(names)
    part = None
    for axis, bit in stages:
        place = names.index((axis, bit))
        mine = (lax.axis_index(axis) >> bit) & 1
        if part is None:
            spread = left.T.reshape((2,) * len(names) + (inner, tokens))
            away = lax.dynamic_index_in_dim(spread, 1 - mine, place, keepdims=False)
            stay = lax.dynamic_index_in_dim(spread, mine, place, keepdims=False)
            away = matmul(away.reshape(-1, tokens), right).astype(low)
            came = swap(away, axis, bit)
            part = (matmul(stay.reshape(-1, tokens), right) + came.astype(jnp.float32)).astype(low)
            names.pop(place)
            part = part.reshape((2,) * len(names) + (inner, right.shape[1]))
        else:
            away = lax.dynamic_index_in_dim(part, 1 - mine, place, keepdims=False)
            stay = lax.dynamic_index_in_dim(part, mine, place, keepdims=False)
            came = swap(away, axis, bit)
            part = (stay.astype(jnp.float32) + came.astype(jnp.float32)).astype(low)
            names.pop(place)
    whole = lax.all_gather(part, "rep", axis=0, tiled=True)
    return whole.astype(jnp.float32)


def exchange_shards(blocks):
    count = lax.axis_size("shard")
    me = lax.axis_index("shard")
    came = [lax.dynamic_index_in_dim(blocks, me, 0, keepdims=False)]
    for step in range(1, count):
        block = lax.dynamic_index_in_dim(blocks, (me + step) % count, 0, keepdims=False)
        came.append(
            lax.ppermute(block, "shard", [(i, (i + step) % count) for i in range(count)])
        )
    return came


MESH=pl.DeviceIdType.MESH

def gather_kernel(shards,reps,count,*refs):
    ins=refs[:count]; outs=refs[count:2*count]; bounce=refs[2*count:3*count]
    line_send,line_recv,rep_send,rep_recv,local_in,local_out=refs[3*count:]
    s=lax.axis_index("shard"); r=lax.axis_index("rep")
    bits=reps.bit_length()-1
    barrier=pltpu.get_barrier_semaphore()
    for side in (-1,1):
        there=(s+side>=0)&(s+side<shards)
        @pl.when(there)
        def _():
            pl.semaphore_signal(barrier,inc=1,device_id={"shard":s+side},device_id_type=MESH)
    for bit in range(bits):
        pl.semaphore_signal(barrier,inc=1,device_id={"rep":r^(1<<bit)},device_id_type=MESH)
    for c in range(count):
        pltpu.make_async_copy(ins[c],bounce[c],local_in.at[c]).start()
    pl.semaphore_wait(barrier,bits+jnp.minimum(s,1)+jnp.minimum(shards-1-s,1))
    sides=((0,1),(1,-1))

    def line(way,step,hop,c,owner):
        src=ins[c].at[r] if hop==0 else outs[c].at[owner,r]
        return pltpu.make_async_remote_copy(src_ref=src,dst_ref=outs[c].at[owner,r],
            send_sem=line_send.at[way,hop,c],recv_sem=line_recv.at[way,hop,c],
            device_id={"shard":s+step},device_id_type=MESH)
    def side_copy(bit,mask,c,owner):
        piece=outs[c].at[owner,r^mask]
        return pltpu.make_async_remote_copy(src_ref=piece,dst_ref=piece,
            send_sem=rep_send.at[bit,mask,owner,c],recv_sem=rep_recv.at[mask|(1<<bit),owner,c],
            device_id={"rep":r^(1<<bit)},device_id_type=MESH)
    def low_bit(mask): return bits if mask==0 else (mask&-mask).bit_length()-1
    def arrived(mask,c,owner):
        bit=low_bit(mask)
        piece=outs[c].at[owner,r^mask]
        pltpu.make_async_remote_copy(src_ref=piece,dst_ref=piece,send_sem=rep_send.at[bit,mask^(1<<bit),owner,c],
            recv_sem=rep_recv.at[mask,owner,c],device_id={"rep":r^(1<<bit)},device_id_type=MESH).wait_recv()
    for c in range(count):
        for way,step in sides:
            @pl.when((s+step>=0)&(s+step<shards))
            def _(): line(way,step,0,c,s).start()
    for c in range(count):
        pltpu.make_async_copy(ins[c],bounce[c],local_in.at[c]).wait()
        pltpu.make_async_copy(bounce[c],outs[c].at[s],local_out.at[c]).start()
    events=[(hop,c) for hop in range(1,shards) for c in range(count)]
    relays=[m for m in range(1,reps) if low_bit(m)>0]
    depth=max([m.bit_count() for m in relays],default=0)
    for index in range(len(events)+depth):
        if index<len(events):
            hop,c=events[index]
            for way,step in sides:
                owner=s-step*hop
                @pl.when((owner>=0)&(owner<shards))
                def _():
                    line(way,step,hop-1,c,owner).wait_recv()
                    if hop+1<shards:
                        @pl.when((s+step>=0)&(s+step<shards))
                        def _(): line(way,step,hop,c,owner).start()
                    for bit in reversed(range(bits)):
                        side_copy(bit,0,c,owner).start()
        for mask in relays:
            late=index-mask.bit_count()
            if 0<=late<len(events):
                hop,c=events[late]
                for way,step in sides:
                    owner=s-step*hop
                    @pl.when((owner>=0)&(owner<shards))
                    def _():
                        arrived(mask,c,owner)
                        for bit in reversed(range(low_bit(mask))):
                            side_copy(bit,mask,c,owner).start()
    for hop,c in events:
        for way,step in sides:
            owner=s-step*hop
            @pl.when((owner>=0)&(owner<shards))
            def _():
                for mask in range(1,reps):
                    if low_bit(mask)==0: arrived(mask,c,owner)
                for mask in range(reps):
                    for bit in range(low_bit(mask)): side_copy(bit,mask,c,owner).wait_send()
                if hop+1<shards:
                    @pl.when((s+step>=0)&(s+step<shards))
                    def _(): line(way,step,hop,c,owner).wait_send()
    for c in range(count):
        for way,step in sides:
            @pl.when((s+step>=0)&(s+step<shards))
            def _(): line(way,step,0,c,s).wait_send()
        pltpu.make_async_copy(bounce[c],outs[c].at[s],local_out.at[c]).wait()

def gather_all(weights):
    shards=lax.axis_size("shard"); reps=lax.axis_size("rep"); bits=reps.bit_length()-1
    assert 1<<bits==reps
    count=len(weights)
    views=[w.reshape(reps,w.shape[0]//reps,w.shape[1]) for w in weights]
    any_=pl.BlockSpec(memory_space=pl.ANY)
    outs=pl.pallas_call(functools.partial(gather_kernel,shards,reps,count),
        in_specs=[any_]*count,out_specs=[any_]*count,
        out_shape=[jax.ShapeDtypeStruct((shards,)+v.shape,v.dtype) for v in views],
        scratch_shapes=[pltpu.VMEM(v.shape,v.dtype) for v in views]+[
            pltpu.SemaphoreType.DMA((2,shards-1,count)),pltpu.SemaphoreType.DMA((2,shards-1,count)),
            pltpu.SemaphoreType.DMA((bits,reps,shards,count)),pltpu.SemaphoreType.DMA((reps,shards,count)),
            pltpu.SemaphoreType.DMA((count,)),pltpu.SemaphoreType.DMA((count,))],
        compiler_params=pltpu.CompilerParams(collective_id=1,has_side_effects=True),
        )(*views)
    return tuple(o.reshape(shards*w.shape[0],w.shape[1]) for o,w in zip(outs,weights))


NAMES=("s1","s0","r1","r0")
REP_FIRST=("r0","r1","s0","s1")
SHARD_FIRST=("r0","s0","s1","r1")
KINDS=(REP_FIRST,SHARD_FIRST,REP_FIRST)
WIDTH=D//3
LAGS=(1,2,2,2)

def block_sources(first_t,second_t,att_t,hidden_t,feed,pre,branch,project):
    pairs=[(hidden_t.at[:,j],feed) for j in range(4)]
    pairs+=[(second_t,pre.at[:,j*D:(j+1)*D]) for j in range(4)]
    pairs+=[(att_t,branch)]
    pairs+=[(first_t,project.at[:,j*D:(j+1)*D]) for j in range(3)]
    return pairs

def reduce_kernel(blocks,*refs):
    ins=refs[:8]; note=refs[8]; out=refs[9]; notes=refs[10]
    (left,right,left_sem,right_sem,part,came,send_sem,recv_sem,kept,final,
     final_sem,near_send,near_recv,far_send,far_recv,fwd_send,fwd_recv,note_send,note_recv,note_sem)=unpack(refs[11:])
    s=lax.axis_index("shard"); r=lax.axis_index("rep")
    bit={"s1":s//2,"s0":lax.rem(s,2),"r1":r//2,"r0":lax.rem(r,2)}
    peer={"s1":{"shard":lax.rem(s+2,4)},"s0":{"shard":s+1-2*lax.rem(s,2)},
          "r1":{"rep":lax.rem(r+2,4)},"r0":{"rep":r+1-2*lax.rem(r,2)}}
    across=lax.rem(r+2,4)
    barrier=pltpu.get_barrier_semaphore()
    others=[(a,b) for a in range(4) for b in range(4) if a or b]
    def note_copy(index,a,b):
        return pltpu.make_async_remote_copy(src_ref=note,dst_ref=notes.at[s*4+r],send_sem=note_send.at[index],recv_sem=note_recv.at[index],
            device_id={"shard":s^a,"rep":r^b},device_id_type=MESH)
    for a,b in others:
        pl.semaphore_signal(barrier,inc=1,device_id={"shard":s^a,"rep":r^b},device_id_type=MESH)
    sources=block_sources(*ins)
    def load(index,slot):
        for here in range(blocks):
            @pl.when(index==here)
            def _():
                a,b=sources[here]
                pltpu.make_async_copy(a,left.at[slot],left_sem.at[slot]).start()
                pltpu.make_async_copy(b,right.at[slot],right_sem.at[slot]).start()
    load(0,0)
    pl.semaphore_wait(barrier,len(others))
    for index,(a,b) in enumerate(others): note_copy(index,a,b).start()
    own_note=pltpu.make_async_copy(note,notes.at[s*4+r],note_sem)
    own_note.start()
    units=3*blocks
    ends=[sum(LAGS[:k+1]) for k in range(4)]
    last=ends[3]

    def pick(ref,slot,names,name,value):
        place=names.index(name)
        return ref.at[(slot,)+(slice(None),)*place+(value,)]
    def exchange(stage,kind,u):
        order=KINDS[kind]; name=order[stage]
        names=[n for n in NAMES if n not in order[:stage]]
        buffers=part if stage==0 else kept[stage-1][order is SHARD_FIRST]
        depth=buffers.shape[0]
        src=pick(buffers,lax.rem(u,depth),names,name,1-bit[name])
        target=came[stage][order is SHARD_FIRST]
        ring=lax.rem(u,target.shape[0])
        return pltpu.make_async_remote_copy(src_ref=src,dst_ref=target.at[ring],
            send_sem=send_sem[stage].at[ring],recv_sem=recv_sem[stage].at[ring],
            device_id=peer[name],device_id_type=MESH)
    def receive(stage,kind,u):
        order=KINDS[kind]; name=order[stage]
        names=[n for n in NAMES if n not in order[:stage]]
        exchange(stage,kind,u).wait()
        buffers=part if stage==0 else kept[stage-1][order is SHARD_FIRST]
        own=pick(buffers,lax.rem(u,buffers.shape[0]),names,name,bit[name])
        target=came[stage][order is SHARD_FIRST]
        other=target.at[lax.rem(u,target.shape[0])]
        left_over=len(names)-1
        if stage<3:
            result=kept[stage][order is SHARD_FIRST]
            slot=lax.rem(u,result.shape[0])
        for flat in range(1<<left_over):
            where=tuple((flat>>k)&1 for k in reversed(range(left_over)))
            total=own[where].astype(jnp.float32)+other[where].astype(jnp.float32)
            if stage<3: result[(slot,)+where]=total.astype(low)
            else: final[lax.rem(u,final.shape[0])]=total.astype(low)
        if stage<3: exchange(stage+1,kind,u).start()
    def place(u,who,kind):
        return out.at[u//3,who,:,kind*WIDTH:(kind+1)*WIDTH]
    def spread(kind,u):
        src=final.at[lax.rem(u,final.shape[0])]
        return (pltpu.make_async_copy(src,place(u,r,kind),final_sem.at[u]),
            pltpu.make_async_remote_copy(src_ref=src,dst_ref=place(u,r,kind),send_sem=far_send.at[u],recv_sem=far_recv.at[u],
                device_id=peer["r1"],device_id_type=MESH),
            pltpu.make_async_remote_copy(src_ref=src,dst_ref=place(u,r,kind),send_sem=near_send.at[u],recv_sem=near_recv.at[u],
                device_id=peer["r0"],device_id_type=MESH))
    def relay(kind,u):
        piece=place(u,across,kind)
        return pltpu.make_async_remote_copy(src_ref=piece,dst_ref=piece,send_sem=fwd_send.at[u],recv_sem=fwd_recv.at[u],
                device_id=peer["r0"],device_id_type=MESH)
    def compute(kind,block,u):
        slot=lax.rem(block,2)
        columns=right[slot,:,kind*WIDTH:(kind+1)*WIDTH]
        rows=left.shape[2]//4
        for shard in range(4):
            product=lax.dot_general(left[slot,shard],columns,(((1,),(0,)),((),())),preferred_element_type=jnp.float32)
            for rep in range(4):
                part[lax.rem(u,part.shape[0]),shard//2,shard%2,rep//2,rep%2]=product[rep*rows:(rep+1)*rows].astype(low)
        exchange(0,kind,u).start()

    total_steps=units+last+4
    iterations=-(-total_steps//3)
    def iteration(it,carry):
        @pl.when(it<blocks)
        def _():
            slot=lax.rem(it,2)
            pltpu.make_async_copy(left.at[slot],left.at[slot],left_sem.at[slot]).wait()
            pltpu.make_async_copy(right.at[slot],right.at[slot],right_sem.at[slot]).wait()
        for sub in range(3):
            step=3*it+sub
            def at(lag,action):
                kind=(sub-lag)%3
                unit=step-lag
                @pl.when((unit>=0)&(unit<units))
                def _(): action(kind,unit)
            def finish(kind,u):
                for copy in spread(kind,u)[:1]: copy.wait()
                for copy in spread(kind,u)[1:]: copy.wait_send()
                relay(kind,u).wait_send()
                spread(kind,u)[2].wait_recv()
                relay(kind,u).wait_recv()
            at(last+3,finish)
            def pass_on(kind,u):
                spread(kind,u)[1].wait_recv()
                relay(kind,u).start()
            at(last+2,pass_on)
            def finalize(kind,u):
                receive(3,kind,u)
                for copy in spread(kind,u): copy.start()
            at(ends[3],finalize)
            for stage in (2,1,0):
                at(ends[stage],functools.partial(receive,stage))
            if sub==0:
                load(it+1,lax.rem(it+1,2))
            at(0,lambda kind,u: compute(kind,it,u))
        return carry
    lax.fori_loop(0,iterations,iteration,0)
    own_note.wait()
    for index,(a,b) in enumerate(others): note_copy(index,a,b).wait()

def unpack(refs):
    refs=list(refs)
    left,right,left_sem,right_sem,part=refs[:5]; refs=refs[5:]
    came=[(refs[0],refs[0]),(refs[1],refs[2]),(refs[3],refs[4]),(refs[5],refs[5])]; refs=refs[6:]
    send=refs[:4]; recv=refs[4:8]; refs=refs[8:]
    kept=[(refs[0],refs[0]),(refs[1],refs[2]),(refs[3],refs[4])]; refs=refs[5:]
    return (left,right,left_sem,right_sem,part,came,send,recv,kept,*refs)

def reduce_all(first_in,second_in,attended,hidden,grad_feed,grad_pre,grad_branch,grad_project,note):
    shards=lax.axis_size("shard"); reps=lax.axis_size("rep")
    tokens=first_in.shape[0]
    rows=D//(shards*reps); group=D//shards
    blocks=12; units=3*blocks
    view=lambda a: a.T.reshape(shards,group,tokens)
    hidden_t=hidden.T.reshape(shards,4,group,tokens)
    any_=pl.BlockSpec(memory_space=pl.ANY)
    piece=(rows,WIDTH)
    two=lambda count: (2,)*count+piece
    rings=[2*lag+1 for lag in LAGS]
    vm=lambda depth,shape: pltpu.VMEM((depth,)+shape,low)
    dma=pltpu.SemaphoreType.DMA
    keep=[lag+1 for lag in LAGS]
    out,notes=pl.pallas_call(functools.partial(reduce_kernel,blocks),
        in_specs=[any_]*8+[pl.BlockSpec(memory_space=pltpu.VMEM)],out_specs=[any_,any_],
        out_shape=[jax.ShapeDtypeStruct((blocks,reps)+(rows,D),low),jax.ShapeDtypeStruct((shards*reps,)+note.shape,note.dtype)],
        scratch_shapes=[
            pltpu.VMEM((2,shards,group,tokens),low),pltpu.VMEM((2,tokens,D),low),dma((2,)),dma((2,)),
            vm(keep[0],two(4)),
            vm(rings[0],two(3)),vm(rings[1],two(2)),vm(rings[1],two(2)),vm(rings[2],two(1)),vm(rings[2],two(1)),vm(rings[3],two(0)),
            *[dma((ring,)) for ring in rings],*[dma((ring,)) for ring in rings],
            vm(keep[1],two(3)),vm(keep[2],two(2)),vm(keep[2],two(2)),vm(keep[3],two(1)),vm(keep[3],two(1)),
            vm(5,piece),
            *[dma((units,)) for _ in range(7)],dma((15,)),dma((15,)),dma(())],
        compiler_params=pltpu.CompilerParams(collective_id=2,has_side_effects=True),
        cost_estimate=pl.CostEstimate(flops=2*tokens*D*D*blocks,bytes_accessed=4*tokens*D*blocks,transcendentals=0),
        )(view(first_in),view(second_in),view(attended),hidden_t,grad_feed,grad_pre,grad_branch,grad_project,note)
    whole=out.reshape(blocks,group,D)
    side=lambda a,b: jnp.concatenate([whole[i] for i in range(a,b)],axis=1).astype(jnp.float32)
    fc2=whole[:4].reshape(4*group,D).astype(jnp.float32)
    return (fc2,side(4,8),whole[8].astype(jnp.float32),side(9,12)),notes.reshape(-1,note.shape[-1])


def body(
    latents,
    cond,
    modulation_weight,
    query_key_value_weight,
    attention_output_weight,
    feed_first_weight,
    feed_second_weight,
    cotangent,
):
    first_section = lax.axis_index("section") == 0
    shard = lax.axis_index("shard")
    rep = lax.axis_index("rep")
    shards = lax.axis_size("shard")
    reps = lax.axis_size("rep")
    batch = latents.shape[0]
    modulation_weight = modulation_weight[0]
    rows = modulation_weight.shape[0]

    cond_float = cond.astype(jnp.float32)
    act = jax.nn.silu(cond_float).astype(low)
    came = exchange_shards(act.reshape(batch, shards, rows).transpose(1, 0, 2))
    partial = matmul(jnp.concatenate(came, axis=0), modulation_weight)
    partial = partial.reshape(shards, batch, -1)
    total = partial[0]
    for step in range(1, shards):
        total = total + lax.ppermute(
            partial[step], "shard", [(i, (i - step) % shards) for i in range(shards)]
        )
    modulation = jnp.split(total[:, None, :], 6, axis=-1)

    weights = gather_all(
        (
            query_key_value_weight[0],
            attention_output_weight[0],
            feed_first_weight[0],
            feed_second_weight[0],
        )
    )

    early, _ = forward_layer(latents.astype(jnp.float32), modulation, weights)
    incoming = lax.ppermute(early.astype(low), "section", [(0, 1)])
    layer_in = jnp.where(first_section, latents, incoming).astype(jnp.float32)
    result, kept = forward_layer(layer_in, modulation, weights)
    own_cot = cotangent.astype(jnp.float32)
    early_grad, _, _ = backward_layer(layer_in, modulation, weights, kept, own_cot)
    returning = lax.ppermute(early_grad.astype(low), "section", [(1, 0)])
    grad_result = jnp.where(first_section, returning, cotangent).astype(jnp.float32)
    grad_in, grad_mod, pairs = backward_layer(layer_in, modulation, weights, kept, grad_result)
    packed = jnp.concatenate([grad_mod, act], axis=-1)
    if shards == 4 and reps == 4:
        lefts = [pair[0] for pair in reversed(pairs)]
        rights = [pair[1] for pair in pairs]
        (grad_fc2, grad_fc1, grad_out, grad_qkv), packed = reduce_all(
            lefts[0], lefts[2], lefts[1], lefts[3], *rights, packed
        )
    else:
        grad_fc2 = reduce_rows(*pairs[0], True)
        grad_fc1 = reduce_rows(*pairs[1], False)
        grad_out = reduce_rows(*pairs[2], True)
        grad_qkv = reduce_rows(*pairs[3], True)
        packed = lax.all_gather(packed, ("shard", "rep"), axis=0, tiled=True)

    boundary = jnp.where(first_section, grad_in, result)[None]

    all_mod = packed[:, : grad_mod.shape[1]]
    all_act = packed[:, grad_mod.shape[1] :]
    act_rows = lax.dynamic_slice_in_dim(all_act, shard * rows, rows, 1)
    grad_ada = lax.dot_general(
        act_rows, all_mod, (((0,), (0,)), ((), ())), preferred_element_type=jnp.float32
    )
    own_mod = lax.dynamic_index_in_dim(
        all_mod.reshape(shards, reps, batch, -1), rep, 1, keepdims=False
    ).reshape(shards * batch, -1)
    act_grad = matmul_t(own_mod, modulation_weight)
    act_grad = act_grad + lax.ppermute(act_grad, "section", [(0, 1), (1, 0)])
    came = exchange_shards(act_grad.reshape(shards, batch, rows))
    act_total = jnp.zeros((shards, batch, rows), jnp.float32)
    for step, block in enumerate(came):
        act_total = lax.dynamic_update_index_in_dim(act_total, block, (shard - step) % shards, 0)
    act_total = act_total.transpose(1, 0, 2).reshape(batch, shards * rows)
    _, silu_back = jax.vjp(jax.nn.silu, cond_float)
    grad_cond = silu_back(act_total)[0]
    return (
        boundary,
        grad_cond,
        grad_ada[None],
        grad_qkv[None],
        grad_out[None],
        grad_fc1[None],
        grad_fc2[None],
    )


def solution(mesh):
    in_specs = (
        P(("shard", "rep"), None, None),
        P(("shard", "rep"), None),
        P("section", "shard", None),
        P("section", "shard", None),
        P("section", "shard", None),
        P("section", "shard", None),
        P("section", "shard", None),
        P(("shard", "rep"), None, None),
    )
    out_specs = (
        P("section", ("shard", "rep"), None, None),
        P(("shard", "rep"), None),
        P("section", "shard", None),
        P("section", "shard", None),
        P("section", "shard", None),
        P("section", "shard", None),
        P("section", "shard", None),
    )
    return jax.shard_map(body, mesh=mesh, in_specs=in_specs, out_specs=out_specs, check_vma=False)
```

```python
import functools

import jax
import jax.numpy as jnp
from jax import lax
from jax.experimental import pallas as pl
from jax.experimental.pallas import tpu as pltpu
from jax.sharding import PartitionSpec as P


D = 1152
HEADS = 16
HEAD_DIM = 72
LANES = 128


epsilon = 1e-06
low = jnp.bfloat16


NT=(((1,),(1,)),((),())); TN=(((0,),(0,)),((),()))
def dot(a,b,dims=(((1,),(0,)),((),()))):
    return lax.dot_general(a,b,dims,preferred_element_type=jnp.float32)
def windows():
    for head in range(HEADS):
        start=head*HEAD_DIM; stop=start+HEAD_DIM
        first=start//LANES*LANES; last=-(-stop//LANES)*LANES
        yield first,last,start-first,stop-first
def head_mask(rows,first,last,begin,end):
    lane=lax.broadcasted_iota(jnp.int32,(rows,last-first),1)
    return (lane>=begin)&(lane<end)
def attention_kernel(project_ref,out_ref):
    rows=out_ref.shape[0]
    for first,last,begin,end in windows():
        mask=head_mask(rows,first,last,begin,end)
        q=project_ref[:,first:last]; k=project_ref[:,D+first:D+last]; v=project_ref[:,2*D+first:2*D+last]
        q=jnp.where(mask,q,jnp.zeros_like(q))
        s=dot(q,k,NT)*(HEAD_DIM**-0.5)
        e=jnp.exp(s-jnp.max(s,axis=1,keepdims=True))
        p=(e/jnp.sum(e,axis=1,keepdims=True)).astype(low)
        o=dot(p,v).astype(low)
        out_ref[:,first:last]=jnp.where(mask,o,out_ref[:,first:last])
def attention_back_kernel(project_ref,grad_ref,out_ref):
    rows=grad_ref.shape[0]; factor=HEAD_DIM**-0.5
    for first,last,begin,end in windows():
        mask=head_mask(rows,first,last,begin,end)
        q=project_ref[:,first:last]; k=project_ref[:,D+first:D+last]; v=project_ref[:,2*D+first:2*D+last]
        g=grad_ref[:,first:last]
        s=dot(jnp.where(mask,k,jnp.zeros_like(k)),q,NT)*factor
        e=jnp.exp(s-jnp.max(s,axis=0,keepdims=True))
        p=e/jnp.sum(e,axis=0,keepdims=True)
        dp=dot(jnp.where(mask,v,jnp.zeros_like(v)),g,NT)
        ds=(p*(dp-jnp.sum(dp*p,axis=0,keepdims=True))).astype(low)
        dq=(dot(ds,k,TN)*factor).astype(low)
        dk=(dot(ds,q)*factor).astype(low)
        dv=dot(p.astype(low),g).astype(low)
        for base,piece in ((0,dq),(D,dk),(2*D,dv)):
            here=slice(base+first,base+last)
            out_ref[:,here]=jnp.where(mask,piece,out_ref[:,here])
def attention(project,length):
    tokens=project.shape[0]
    return pl.pallas_call(attention_kernel,grid=(tokens//length,),
        in_specs=[pl.BlockSpec((length,3*D),lambda i:(i,0))],out_specs=pl.BlockSpec((length,D),lambda i:(i,0)),
        out_shape=jax.ShapeDtypeStruct((tokens,D),low),
        cost_estimate=pl.CostEstimate(flops=4*tokens*length*D,bytes_accessed=8*tokens*D,transcendentals=HEADS*tokens*length))(project)
def attention_back(project,grad,length):
    tokens=project.shape[0]
    return pl.pallas_call(attention_back_kernel,grid=(tokens//length,),
        in_specs=[pl.BlockSpec((length,3*D),lambda i:(i,0)),pl.BlockSpec((length,D),lambda i:(i,0))],out_specs=pl.BlockSpec((length,3*D),lambda i:(i,0)),
        out_shape=jax.ShapeDtypeStruct((tokens,3*D),low),
        cost_estimate=pl.CostEstimate(flops=10*tokens*length*D,bytes_accessed=14*tokens*D,transcendentals=HEADS*tokens*length))(project,grad)

C0=0.7978845608028654; C1=0.044715
def act_of(u): return (0.5*u*(1.0+jnp.tanh(C0*(u+C1*(u*u*u))))).astype(low)
def slope_of(u):
    sq=u*u
    t=jnp.tanh(C0*(u+C1*(sq*u)))
    return 0.5*(1.0+t)+0.5*u*(1.0-t*t)*(C0*(1.0+3.0*C1*sq))
def mlp_kernel(chunk,x_ref,middle_ref,gate_ref,w1_ref,w2_ref,u_ref,h_ref,f_ref,y_ref,y_low_ref):
    tile=w1_ref.shape[1]
    parts=[slice(a,a+chunk) for a in range(0,tile,chunk)]
    first=pl.program_id(0)==0
    @pl.when(first)
    def _(): f_ref[...]=jnp.zeros_like(f_ref)
    def front(p):
        u=dot(x_ref[...],w1_ref[:,p]); u_ref[:,p]=u
        return u
    def back(p,u):
        h=act_of(u); h_ref[:,p]=h
        f_ref[...]+=dot(h,w2_ref[p,:])
    prev=None
    for p in parts:
        u=front(p)
        if prev is not None: back(*prev)
        prev=(p,u)
    back(*prev)
    @pl.when(pl.program_id(0)==pl.num_programs(0)-1)
    def _():
        y=middle_ref[...]+gate_ref[...]*f_ref[...]
        y_ref[...]=y
        y_low_ref[...]=y.astype(low)
def mlp_back_kernel(chunk,g_ref,w1_ref,w2_ref,u_ref,du_ref,dx_ref):
    tile=w1_ref.shape[1]
    parts=[slice(a,a+chunk) for a in range(0,tile,chunk)]
    first=pl.program_id(0)==0
    @pl.when(first)
    def _(): dx_ref[...]=jnp.zeros_like(dx_ref)
    def front(p): return dot(g_ref[...],w2_ref[p,:],NT)
    def mid(p,dh):
        du=(dh*slope_of(u_ref[:,p])).astype(low); du_ref[:,p]=du
        return du
    prev=None
    for p in parts:
        dh=front(p)
        if prev is not None: dx_ref[...]+=dot(mid(*prev),w1_ref[:,prev[0]],NT)
        prev=(p,dh)
    dx_ref[...]+=dot(mid(*prev),w1_ref[:,prev[0]],NT)
def mlp(x,middle,gate,w1,w2,tile=1536,chunk=512):
    t,d=x.shape; ff=w1.shape[1]
    whole=pl.BlockSpec((t,d),lambda i:(0,0))
    cols=pl.BlockSpec((t,tile),lambda i:(0,i))
    made=lambda width,dtype: jax.ShapeDtypeStruct((t,width),dtype)
    return pl.pallas_call(functools.partial(mlp_kernel,chunk),grid=(ff//tile,),
        in_specs=[whole,whole,pl.BlockSpec((1,d),lambda i:(0,0)),pl.BlockSpec((d,tile),lambda i:(0,i)),pl.BlockSpec((tile,d),lambda i:(i,0))],
        out_specs=[cols,cols,whole,whole,whole],
        out_shape=[made(ff,jnp.float32),made(ff,low),made(d,jnp.float32),made(d,jnp.float32),made(d,low)],
        cost_estimate=pl.CostEstimate(flops=4*t*d*ff,bytes_accessed=4*d*ff+6*t*ff+16*t*d,transcendentals=t*ff))(x,middle,gate,w1,w2)
def mlp_back(g,w1,w2,u,tile=1536,chunk=512):
    t,d=g.shape; ff=w1.shape[1]
    whole=pl.BlockSpec((t,d),lambda i:(0,0))
    cols=pl.BlockSpec((t,tile),lambda i:(0,i))
    return pl.pallas_call(functools.partial(mlp_back_kernel,chunk),grid=(ff//tile,),
        in_specs=[whole,pl.BlockSpec((d,tile),lambda i:(0,i)),pl.BlockSpec((tile,d),lambda i:(i,0)),cols],
        out_specs=[cols,whole],
        out_shape=[jax.ShapeDtypeStruct((t,ff),low),jax.ShapeDtypeStruct((t,d),jnp.float32)],
        cost_estimate=pl.CostEstimate(flops=4*t*d*ff,bytes_accessed=4*d*ff+6*t*ff+6*t*d,transcendentals=t*ff))(g,w1,w2,u)


def center_scale(values):
    center = values - jnp.mean(values, axis=-1, keepdims=True)
    scale = lax.rsqrt(jnp.mean(center * center, axis=-1, keepdims=True) + epsilon)
    return center * scale, scale


def norm_back(normed, scale, grad):
    mean_grad = jnp.mean(grad, axis=-1, keepdims=True)
    mean_dot = jnp.mean(grad * normed, axis=-1, keepdims=True)
    return (grad - mean_grad - normed * mean_dot) * scale


def matmul(left, right):
    return jnp.dot(left, right, preferred_element_type=jnp.float32)


def matmul_t(left, right):
    return lax.dot_general(
        left, right, (((1,), (1,)), ((), ())), preferred_element_type=jnp.float32
    )


def forward_layer(input_rows, modulation, weights):
    query_key_value_weight, attention_output_weight, feed_first_weight, feed_second_weight = weights
    batch_size, length, model_width = input_rows.shape
    tokens = batch_size * length
    shift_one, scale_one, gate_one, shift_two, scale_two, gate_two = modulation
    normed_one, _ = center_scale(input_rows)
    first_in = (normed_one * (1.0 + scale_one) + shift_one).astype(low).reshape(tokens, model_width)
    project = matmul(first_in, query_key_value_weight).astype(low)
    attended = attention(project, length)
    branch = matmul(attended, attention_output_weight).reshape(batch_size, length, model_width)
    middle_state = input_rows + gate_one * branch
    normed_two, _ = center_scale(middle_state)
    second_in = (
        (normed_two * (1.0 + scale_two) + shift_two).astype(low).reshape(tokens, model_width)
    )
    shape = (batch_size, length, model_width)
    hidden_pre, hidden, feed_out, result, result_low = mlp(
        second_in,
        middle_state.reshape(tokens, model_width),
        gate_two.reshape(1, model_width),
        feed_first_weight,
        feed_second_weight,
    )
    feed_out, result, result_low = (
        value.reshape(shape) for value in (feed_out, result, result_low)
    )
    kept = (
        first_in,
        project,
        attended,
        branch,
        middle_state,
        second_in,
        hidden_pre,
        hidden,
        feed_out,
    )
    return result, result_low, kept


def backward_layer(input_rows, modulation, weights, kept, grad_result):
    query_key_value_weight, attention_output_weight, feed_first_weight, feed_second_weight = weights
    (
        first_in,
        project,
        attended,
        branch,
        middle_state,
        second_in,
        hidden_pre,
        hidden,
        feed_out,
    ) = kept
    batch_size, length, model_width = input_rows.shape
    tokens = batch_size * length
    _, scale_one, gate_one, _, scale_two, gate_two = modulation
    grad_gate_two = jnp.sum(grad_result * feed_out, axis=1)
    grad_feed = (gate_two * grad_result).astype(low).reshape(tokens, model_width)
    grad_pre, grad_second = mlp_back(
        grad_feed, feed_first_weight, feed_second_weight, hidden_pre
    )
    grad_second = grad_second.reshape(batch_size, length, model_width)
    normed_two, inv_two = center_scale(middle_state)
    grad_shift_two = jnp.sum(grad_second, axis=1)
    grad_scale_two = jnp.sum(grad_second * normed_two, axis=1)
    grad_middle = grad_result + norm_back(normed_two, inv_two, grad_second * (1.0 + scale_two))
    grad_gate_one = jnp.sum(grad_middle * branch, axis=1)
    grad_branch = (gate_one * grad_middle).astype(low).reshape(tokens, model_width)
    grad_att = matmul_t(grad_branch, attention_output_weight).astype(low)
    grad_project = attention_back(project, grad_att, length)
    grad_first = matmul_t(grad_project, query_key_value_weight).reshape(
        batch_size, length, model_width
    )
    normed_one, inv_one = center_scale(input_rows)
    grad_shift_one = jnp.sum(grad_first, axis=1)
    grad_scale_one = jnp.sum(grad_first * normed_one, axis=1)
    grad_inputs = grad_middle + norm_back(normed_one, inv_one, grad_first * (1.0 + scale_one))
    grad_mod = jnp.concatenate(
        [
            grad_shift_one,
            grad_scale_one,
            grad_gate_one,
            grad_shift_two,
            grad_scale_two,
            grad_gate_two,
        ],
        axis=-1,
    ).astype(low)
    pairs = (
        (hidden, grad_feed),
        (second_in, grad_pre),
        (attended, grad_branch),
        (first_in, grad_project),
    )
    return grad_inputs, grad_mod, pairs


def bits_of(count):
    bits = count.bit_length() - 1
    assert 1 << bits == count
    return bits


def swap(value, axis, bit):
    count = lax.axis_size(axis)
    return lax.ppermute(value, axis, [(i, i ^ (1 << bit)) for i in range(count)])


def reduce_rows(left, right, reps_first):
    shard_bits = bits_of(lax.axis_size("shard"))
    rep_bits = bits_of(lax.axis_size("rep"))
    shard_stages = [("shard", bit) for bit in range(shard_bits)]
    rep_stages = [("rep", bit) for bit in range(rep_bits)]
    if reps_first:
        stages = rep_stages + shard_stages
    else:
        stages = rep_stages[:1] + shard_stages + rep_stages[1:]
    names = [("shard", bit) for bit in reversed(range(shard_bits))]
    names += [("rep", bit) for bit in reversed(range(rep_bits))]
    tokens, depth = left.shape
    inner = depth >> len(names)
    part = None
    for axis, bit in stages:
        place = names.index((axis, bit))
        mine = (lax.axis_index(axis) >> bit) & 1
        if part is None:
            spread = left.T.reshape((2,) * len(names) + (inner, tokens))
            away = lax.dynamic_index_in_dim(spread, 1 - mine, place, keepdims=False)
            stay = lax.dynamic_index_in_dim(spread, mine, place, keepdims=False)
            away = matmul(away.reshape(-1, tokens), right).astype(low)
            came = swap(away, axis, bit)
            part = (matmul(stay.reshape(-1, tokens), right) + came.astype(jnp.float32)).astype(low)
            names.pop(place)
            part = part.reshape((2,) * len(names) + (inner, right.shape[1]))
        else:
            away = lax.dynamic_index_in_dim(part, 1 - mine, place, keepdims=False)
            stay = lax.dynamic_index_in_dim(part, mine, place, keepdims=False)
            came = swap(away, axis, bit)
            part = (stay.astype(jnp.float32) + came.astype(jnp.float32)).astype(low)
            names.pop(place)
    whole = lax.all_gather(part, "rep", axis=0, tiled=True)
    return whole.astype(jnp.float32)


def exchange_shards(blocks):
    count = lax.axis_size("shard")
    me = lax.axis_index("shard")
    came = [lax.dynamic_index_in_dim(blocks, me, 0, keepdims=False)]
    for step in range(1, count):
        block = lax.dynamic_index_in_dim(blocks, (me + step) % count, 0, keepdims=False)
        came.append(
            lax.ppermute(block, "shard", [(i, (i + step) % count) for i in range(count)])
        )
    return came


MESH=pl.DeviceIdType.MESH

def gather_kernel(shards,reps,count,*refs):
    ins=refs[:count]; outs=refs[count:2*count]; bounce=refs[2*count:3*count]
    line_send,line_recv,rep_send,rep_recv,local_in,local_out=refs[3*count:]
    s=lax.axis_index("shard"); r=lax.axis_index("rep")
    bits=reps.bit_length()-1
    barrier=pltpu.get_barrier_semaphore()
    for side in (-1,1):
        there=(s+side>=0)&(s+side<shards)
        @pl.when(there)
        def _():
            pl.semaphore_signal(barrier,inc=1,device_id={"shard":s+side},device_id_type=MESH)
    for bit in range(bits):
        pl.semaphore_signal(barrier,inc=1,device_id={"rep":r^(1<<bit)},device_id_type=MESH)
    for c in range(count):
        pltpu.make_async_copy(ins[c],bounce[c],local_in.at[c]).start()
    pl.semaphore_wait(barrier,bits+jnp.minimum(s,1)+jnp.minimum(shards-1-s,1))
    sides=((0,1),(1,-1))

    def line(way,step,hop,c,owner):
        src=ins[c].at[r] if hop==0 else outs[c].at[owner,r]
        return pltpu.make_async_remote_copy(src_ref=src,dst_ref=outs[c].at[owner,r],
            send_sem=line_send.at[way,hop,c],recv_sem=line_recv.at[way,hop,c],
            device_id={"shard":s+step},device_id_type=MESH)
    def side_copy(bit,mask,c,owner):
        piece=outs[c].at[owner,r^mask]
        return pltpu.make_async_remote_copy(src_ref=piece,dst_ref=piece,
            send_sem=rep_send.at[bit,mask,owner,c],recv_sem=rep_recv.at[mask|(1<<bit),owner,c],
            device_id={"rep":r^(1<<bit)},device_id_type=MESH)
    def low_bit(mask): return bits if mask==0 else (mask&-mask).bit_length()-1
    def arrived(mask,c,owner):
        bit=low_bit(mask)
        piece=outs[c].at[owner,r^mask]
        pltpu.make_async_remote_copy(src_ref=piece,dst_ref=piece,send_sem=rep_send.at[bit,mask^(1<<bit),owner,c],
            recv_sem=rep_recv.at[mask,owner,c],device_id={"rep":r^(1<<bit)},device_id_type=MESH).wait_recv()
    for c in range(count):
        for way,step in sides:
            @pl.when((s+step>=0)&(s+step<shards))
            def _(): line(way,step,0,c,s).start()
    for c in range(count):
        pltpu.make_async_copy(ins[c],bounce[c],local_in.at[c]).wait()
        pltpu.make_async_copy(bounce[c],outs[c].at[s],local_out.at[c]).start()
    events=[(hop,c) for hop in range(1,shards) for c in range(count)]
    relays=[m for m in range(1,reps) if low_bit(m)>0]
    depth=max([m.bit_count() for m in relays],default=0)
    for index in range(len(events)+depth):
        if index<len(events):
            hop,c=events[index]
            for way,step in sides:
                owner=s-step*hop
                @pl.when((owner>=0)&(owner<shards))
                def _():
                    line(way,step,hop-1,c,owner).wait_recv()
                    if hop+1<shards:
                        @pl.when((s+step>=0)&(s+step<shards))
                        def _(): line(way,step,hop,c,owner).start()
                    for bit in reversed(range(bits)):
                        side_copy(bit,0,c,owner).start()
        for mask in relays:
            late=index-mask.bit_count()
            if 0<=late<len(events):
                hop,c=events[late]
                for way,step in sides:
                    owner=s-step*hop
                    @pl.when((owner>=0)&(owner<shards))
                    def _():
                        arrived(mask,c,owner)
                        for bit in reversed(range(low_bit(mask))):
                            side_copy(bit,mask,c,owner).start()
    for hop,c in events:
        for way,step in sides:
            owner=s-step*hop
            @pl.when((owner>=0)&(owner<shards))
            def _():
                for mask in range(1,reps):
                    if low_bit(mask)==0: arrived(mask,c,owner)
                for mask in range(reps):
                    for bit in range(low_bit(mask)): side_copy(bit,mask,c,owner).wait_send()
                if hop+1<shards:
                    @pl.when((s+step>=0)&(s+step<shards))
                    def _(): line(way,step,hop,c,owner).wait_send()
    for c in range(count):
        for way,step in sides:
            @pl.when((s+step>=0)&(s+step<shards))
            def _(): line(way,step,0,c,s).wait_send()
        pltpu.make_async_copy(bounce[c],outs[c].at[s],local_out.at[c]).wait()

def gather_all(weights):
    shards=lax.axis_size("shard"); reps=lax.axis_size("rep"); bits=reps.bit_length()-1
    assert 1<<bits==reps
    count=len(weights)
    views=[w.reshape(reps,w.shape[0]//reps,w.shape[1]) for w in weights]
    any_=pl.BlockSpec(memory_space=pl.ANY)
    outs=pl.pallas_call(functools.partial(gather_kernel,shards,reps,count),
        in_specs=[any_]*count,out_specs=[any_]*count,
        out_shape=[jax.ShapeDtypeStruct((shards,)+v.shape,v.dtype) for v in views],
        scratch_shapes=[pltpu.VMEM(v.shape,v.dtype) for v in views]+[
            pltpu.SemaphoreType.DMA((2,shards-1,count)),pltpu.SemaphoreType.DMA((2,shards-1,count)),
            pltpu.SemaphoreType.DMA((bits,reps,shards,count)),pltpu.SemaphoreType.DMA((reps,shards,count)),
            pltpu.SemaphoreType.DMA((count,)),pltpu.SemaphoreType.DMA((count,))],
        compiler_params=pltpu.CompilerParams(collective_id=1,has_side_effects=True),
        )(*views)
    return tuple(o.reshape(shards*w.shape[0],w.shape[1]) for o,w in zip(outs,weights))


NAMES=("s1","s0","r1","r0")
REP_FIRST=("r0","r1","s0","s1")
SHARD_FIRST=("r0","s0","s1","r1")
KINDS=(REP_FIRST,SHARD_FIRST,REP_FIRST)
WIDTH=D//3
LAGS=(1,3,3,2)

def block_sources(first_t,second_t,att_t,hidden_t,feed,pre,branch,project):
    pairs=[(hidden_t.at[:,j],feed) for j in range(4)]
    pairs+=[(second_t,pre.at[:,j*D:(j+1)*D]) for j in range(4)]
    pairs+=[(att_t,branch)]
    pairs+=[(first_t,project.at[:,j*D:(j+1)*D]) for j in range(3)]
    return pairs

def reduce_kernel(blocks,*refs):
    ins=(refs[:8],refs[8:16]); note,ada,outs,notes,act_out=refs[16],refs[17],refs[18:22],refs[22],refs[23]
    (left,right,left_sem,right_sem,part,came,send_sem,recv_sem,kept,final,
     final_sem,near_send,near_recv,far_send,far_recv,fwd_send,fwd_recv,note_send,note_recv,
     notes_in,ada_in,ada_sem,_,blocks_out,blocks_in,act_send,act_recv)=unpack(refs[24:])
    c=lax.axis_index("section")
    s=lax.axis_index("shard"); r=lax.axis_index("rep")
    bit={"s1":s//2,"s0":lax.rem(s,2),"r1":r//2,"r0":lax.rem(r,2)}
    peer={"s1":{"shard":lax.rem(s+2,4)},"s0":{"shard":s+1-2*lax.rem(s,2)},
          "r1":{"rep":lax.rem(r+2,4)},"r0":{"rep":r+1-2*lax.rem(r,2)}}
    across=lax.rem(r+2,4)
    barrier=pltpu.get_barrier_semaphore()
    others=[(a,b) for a in range(4) for b in range(4) if a or b]
    def note_copy(index,a,b):
        return pltpu.make_async_remote_copy(src_ref=note,dst_ref=notes_in.at[s*4+r],send_sem=note_send.at[index],recv_sem=note_recv.at[index],
            device_id={"shard":s^a,"rep":r^b},device_id_type=MESH)
    for a,b in others:
        pl.semaphore_signal(barrier,inc=1,device_id={"shard":s^a,"rep":r^b},device_id_type=MESH)
    for a in range(4):
        pl.semaphore_signal(barrier,inc=1,device_id={"section":1-c,"shard":s^a},device_id_type=MESH)
    sources=[block_sources(*half) for half in ins]
    span=left.shape[3]//2
    def load(index,slot):
        for here in range(blocks):
            @pl.when(index==here)
            def _():
                for half in range(2):
                    a,b=sources[half][here]
                    place=pl.ds(half*span,span)
                    pltpu.make_async_copy(a,left.at[slot,:,:,place],left_sem.at[slot]).start()
                    pltpu.make_async_copy(b,right.at[slot,place],right_sem.at[slot]).start()
    load(0,0)
    pltpu.make_async_copy(ada,ada_in,ada_sem).start()
    pl.semaphore_wait(barrier,len(others)+4)
    for index,(a,b) in enumerate(others): note_copy(index,a,b).start()
    notes_in[s*4+r]=note[...]
    def act_copy(index,a,other):
        section=1-c if other else c
        return pltpu.make_async_remote_copy(src_ref=blocks_out.at[s^a],dst_ref=blocks_in.at[c,s],send_sem=act_send.at[index],
            recv_sem=act_recv.at[index],device_id={"section":section,"shard":s^a},device_id_type=MESH)
    act_peers=[(a,other) for a in range(4) for other in (False,True) if a or other]
    def share_notes():
        for index,(a,b) in enumerate(others): note_copy(index,a,b).wait()
        pltpu.make_async_copy(ada,ada_in,ada_sem).wait()
        wide=lambda index: notes_in[index].astype(jnp.float32)
        notes_out=jnp.concatenate([wide(index) for index in range(16)],axis=0).astype(low)
        notes[...]=notes_out
        mine=jnp.concatenate([wide(shard*4+r)[:,:6*D] for shard in range(4)],axis=0).astype(low)
        grads=lax.dot_general(mine,ada_in[...],(((1,),(1,)),((),())),preferred_element_type=jnp.float32)
        span=grads.shape[0]//4
        for shard in range(4): blocks_out[shard]=grads[shard*span:(shard+1)*span]
        blocks_in[c,s]=blocks_out[s]
        for index,(a,other) in enumerate(act_peers): act_copy(index,a,other).start()
    units=3*blocks
    ends=[sum(LAGS[:k+1]) for k in range(4)]
    last=ends[3]

    def pick(ref,slot,names,name,value):
        place=names.index(name)
        return ref.at[(slot,)+(slice(None),)*place+(value,)]
    def exchange(stage,kind,u):
        order=KINDS[kind]; name=order[stage]
        names=[n for n in NAMES if n not in order[:stage]]
        buffers=part if stage==0 else kept[stage-1][order is SHARD_FIRST]
        depth=buffers.shape[0]
        src=pick(buffers,lax.rem(u,depth),names,name,1-bit[name])
        target=came[stage][order is SHARD_FIRST]
        ring=lax.rem(u,target.shape[0])
        return pltpu.make_async_remote_copy(src_ref=src,dst_ref=target.at[ring],
            send_sem=send_sem[stage].at[ring],recv_sem=recv_sem[stage].at[ring],
            device_id=peer[name],device_id_type=MESH)
    def receive(stage,kind,u):
        order=KINDS[kind]; name=order[stage]
        names=[n for n in NAMES if n not in order[:stage]]
        exchange(stage,kind,u).wait()
        buffers=part if stage==0 else kept[stage-1][order is SHARD_FIRST]
        own=pick(buffers,lax.rem(u,buffers.shape[0]),names,name,bit[name])
        target=came[stage][order is SHARD_FIRST]
        other=target.at[lax.rem(u,target.shape[0])]
        left_over=len(names)-1
        if stage<3:
            result=kept[stage][order is SHARD_FIRST]
            slot=lax.rem(u,result.shape[0])
        for flat in range(1<<left_over):
            where=tuple((flat>>k)&1 for k in reversed(range(left_over)))
            total=own[where].astype(jnp.float32)+other[where].astype(jnp.float32)
            if stage<3: result[(slot,)+where]=total.astype(low)
            else: final[lax.rem(u,final.shape[0])]=total.astype(low)
        if stage<3: exchange(stage+1,kind,u).start()
    grad_qkv,grad_wout,grad_fc1,grad_fc2=outs
    anywhere=grad_fc2.at[0,0,:,:WIDTH]
    def placed(u,kind,action):
        block=u//3
        def columns(first): return pl.ds(pl.multiple_of((block-first)*D+kind*WIDTH,128),WIDTH)
        here=slice(kind*WIDTH,(kind+1)*WIDTH)
        pl.when(block<4)(lambda: action(lambda who: grad_fc2.at[block,who,:,here]))
        pl.when((block>=4)&(block<8))(lambda: action(lambda who: grad_fc1.at[who,:,columns(4)]))
        pl.when(block==8)(lambda: action(lambda who: grad_wout.at[who,:,here]))
        pl.when(block>=9)(lambda: action(lambda who: grad_qkv.at[who,:,columns(9)]))
    def spread(u,target):
        src=final.at[lax.rem(u,final.shape[0])]
        return (pltpu.make_async_copy(src,target,final_sem.at[u]),
            pltpu.make_async_remote_copy(src_ref=src,dst_ref=target,send_sem=far_send.at[u],recv_sem=far_recv.at[u],
                device_id=peer["r1"],device_id_type=MESH),
            pltpu.make_async_remote_copy(src_ref=src,dst_ref=target,send_sem=near_send.at[u],recv_sem=near_recv.at[u],
                device_id=peer["r0"],device_id_type=MESH))
    def relay(u,piece):
        return pltpu.make_async_remote_copy(src_ref=piece,dst_ref=piece,send_sem=fwd_send.at[u],recv_sem=fwd_recv.at[u],
                device_id=peer["r0"],device_id_type=MESH)
    def compute(kind,block,u):
        slot=lax.rem(block,2)
        columns=right[slot,:,kind*WIDTH:(kind+1)*WIDTH]
        rows=left.shape[2]//4
        for shard in range(4):
            product=lax.dot_general(left[slot,shard],columns,(((1,),(0,)),((),())),preferred_element_type=jnp.float32)
            for rep in range(4):
                part[lax.rem(u,part.shape[0]),shard//2,shard%2,rep//2,rep%2]=product[rep*rows:(rep+1)*rows].astype(low)
        exchange(0,kind,u).start()

    total_steps=units+last+4
    iterations=-(-total_steps//3)
    def iteration(it,carry):
        @pl.when(it<blocks)
        def _():
            slot=lax.rem(it,2)
            pltpu.make_async_copy(left.at[slot],left.at[slot],left_sem.at[slot]).wait()
            pltpu.make_async_copy(right.at[slot],right.at[slot],right_sem.at[slot]).wait()
        for sub in range(3):
            step=3*it+sub
            def at(lag,action):
                kind=(sub-lag)%3
                unit=step-lag
                @pl.when((unit>=0)&(unit<units))
                def _(): action(kind,unit)
            def finish(kind,u):
                local,far,near=spread(u,anywhere)
                local.wait(); far.wait_send(); near.wait(); relay(u,anywhere).wait()
            at(last+3,finish)
            def pass_on(kind,u):
                spread(u,anywhere)[1].wait_recv()
                placed(u,kind,lambda where: relay(u,where(across)).start())
            at(last+2,pass_on)
            def finalize(kind,u):
                receive(3,kind,u)
                def start(where):
                    for copy in spread(u,where(r)): copy.start()
                placed(u,kind,start)
            at(ends[3],finalize)
            for stage in (2,1,0):
                at(ends[stage],functools.partial(receive,stage))
            if sub==0:
                load(it+1,lax.rem(it+1,2))
                pl.when(it==3)(share_notes)
            at(0,lambda kind,u: compute(kind,it,u))
        return carry
    lax.fori_loop(0,iterations,iteration,0)
    for index,(a,other) in enumerate(act_peers): act_copy(index,a,other).wait()
    act_out[...]=blocks_in[0]+blocks_in[1]

def unpack(refs):
    refs=list(refs)
    left,right,left_sem,right_sem,part=refs[:5]; refs=refs[5:]
    came=[(refs[0],refs[0]),(refs[1],refs[2]),(refs[3],refs[4]),(refs[5],refs[5])]; refs=refs[6:]
    send=refs[:4]; recv=refs[4:8]; refs=refs[8:]
    kept=[(refs[0],refs[0]),(refs[1],refs[2]),(refs[3],refs[4])]; refs=refs[5:]
    return (left,right,left_sem,right_sem,part,came,send,recv,kept,*refs)

def reduce_all(halves,note,ada):
    shards=lax.axis_size("shard"); reps=lax.axis_size("rep")
    rows=D//(shards*reps); group=D//shards
    blocks=12; units=3*blocks
    operands=[]
    for pairs in halves:
        (hidden,feed),(second,pre),(att,branch),(first,project)=pairs
        span=hidden.shape[0]
        operands+=[a.T.reshape(shards,group,span) for a in (first,second,att)]
        operands+=[hidden.T.reshape(shards,4,group,span),feed,pre,branch,project]
    tokens=2*span
    any_=pl.BlockSpec(memory_space=pl.ANY)
    piece=(rows,WIDTH)
    two=lambda count: (2,)*count+piece
    rings=[2*lag+1 for lag in LAGS]
    vm=lambda depth,shape: pltpu.VMEM((depth,)+shape,low)
    dma=pltpu.SemaphoreType.DMA
    keep=[lag+1 for lag in LAGS]
    inside=pl.BlockSpec(memory_space=pltpu.VMEM)
    batch=note.shape[0]
    made=lambda shape,dtype: jax.ShapeDtypeStruct(shape,dtype)
    *grads,notes,act_grad=pl.pallas_call(functools.partial(reduce_kernel,blocks),
        in_specs=[any_]*16+[inside,any_],out_specs=[any_]*4+[inside,inside],
        out_shape=[made((reps,rows,3*D),low),made((reps,rows,D),low),made((reps,rows,4*D),low),made((4,reps,rows,D),low),
            made((shards*reps*batch,note.shape[1]),low),made((shards,batch,group),jnp.float32)],
        scratch_shapes=[
            pltpu.VMEM((2,shards,group,tokens),low),pltpu.VMEM((2,tokens,D),low),dma((2,)),dma((2,)),
            vm(keep[0],two(4)),
            vm(rings[0],two(3)),vm(rings[1],two(2)),vm(rings[1],two(2)),vm(rings[2],two(1)),vm(rings[2],two(1)),vm(rings[3],two(0)),
            *[dma((ring,)) for ring in rings],*[dma((ring,)) for ring in rings],
            vm(keep[1],two(3)),vm(keep[2],two(2)),vm(keep[2],two(2)),vm(keep[3],two(1)),vm(keep[3],two(1)),
            vm(5,piece),
            *[dma((units,)) for _ in range(7)],dma((15,)),dma((15,)),
            pltpu.VMEM((shards*reps,)+note.shape,low),pltpu.VMEM(ada.shape,low),dma(()),dma(()),
            pltpu.VMEM((shards,batch,group),jnp.float32),pltpu.VMEM((2,shards,batch,group),jnp.float32),dma((7,)),dma((7,))],
        compiler_params=pltpu.CompilerParams(collective_id=2,has_side_effects=True),
        cost_estimate=pl.CostEstimate(flops=2*tokens*D*D*blocks,bytes_accessed=4*tokens*D*blocks,transcendentals=0),
        )(*operands,note,ada)
    grads=[grad.reshape(-1,grad.shape[-1]).astype(jnp.float32) for grad in grads]
    return grads,notes,act_grad


def body(
    latents,
    cond,
    modulation_weight,
    query_key_value_weight,
    attention_output_weight,
    feed_first_weight,
    feed_second_weight,
    cotangent,
):
    first_section = lax.axis_index("section") == 0
    shard = lax.axis_index("shard")
    rep = lax.axis_index("rep")
    shards = lax.axis_size("shard")
    reps = lax.axis_size("rep")
    batch = latents.shape[0]
    modulation_weight = modulation_weight[0]
    rows = modulation_weight.shape[0]

    cond_float = cond.astype(jnp.float32)
    act = jax.nn.silu(cond_float).astype(low)
    came = exchange_shards(act.reshape(batch, shards, rows).transpose(1, 0, 2))
    partial = matmul(jnp.concatenate(came, axis=0), modulation_weight)
    partial = partial.reshape(shards, batch, -1)
    total = partial[0]
    for step in range(1, shards):
        total = total + lax.ppermute(
            partial[step], "shard", [(i, (i - step) % shards) for i in range(shards)]
        )
    def pick(section_zero, section_one):
        rows_of = jnp.where(
            first_section,
            total[section_zero : section_zero + 1],
            total[section_one : section_one + 1],
        )
        return jnp.split(rows_of[:, None, :], 6, axis=-1)

    weights = gather_all(
        (
            query_key_value_weight[0],
            attention_output_weight[0],
            feed_first_weight[0],
            feed_second_weight[0],
        )
    )

    forth = [(0, 1)]
    back = [(1, 0)]
    latent = (latents[:1], latents[1:])
    grad_out = (cotangent[:1], cotangent[1:])
    mod_zero, mod_one, mod_two = pick(0, 0), pick(1, 0), pick(0, 1)
    _, early, _ = forward_layer(latent[0].astype(jnp.float32), mod_zero, weights)
    incoming = lax.ppermute(early, "section", forth)
    input_one = jnp.where(first_section, latent[1], incoming).astype(jnp.float32)
    result_one, sent, kept_one = forward_layer(input_one, mod_one, weights)
    incoming = lax.ppermute(sent, "section", forth)
    early, _, _ = backward_layer(
        input_one, mod_one, weights, kept_one, grad_out[0].astype(jnp.float32)
    )
    early = early.astype(low)
    returning = lax.ppermute(early, "section", back)
    incoming, early = lax.optimization_barrier((incoming, early))
    input_two = jnp.where(first_section, latent[0], incoming).astype(jnp.float32)
    result_two, _, kept_two = forward_layer(input_two, mod_two, weights)
    grad_result = jnp.where(first_section, returning, grad_out[1]).astype(jnp.float32)
    grad_in_one, grad_mod_one, pairs_one = backward_layer(
        input_two, mod_two, weights, kept_two, grad_result
    )
    returning = lax.ppermute(grad_in_one.astype(low), "section", back)
    grad_result = jnp.where(first_section, returning, grad_out[0]).astype(jnp.float32)
    grad_in_two, grad_mod_two, pairs_two = backward_layer(
        input_one, mod_one, weights, kept_one, grad_result
    )
    grad_mod = jnp.where(
        first_section,
        jnp.concatenate([grad_mod_one, grad_mod_two], axis=0),
        jnp.concatenate([grad_mod_two, grad_mod_one], axis=0),
    )
    packed = jnp.concatenate([grad_mod, act], axis=-1)
    if shards == 4 and reps == 4:
        (grad_qkv, grad_wout, grad_fc1, grad_fc2), packed, act_grad = reduce_all(
            (pairs_one, pairs_two), packed, modulation_weight
        )
        act_total = act_grad.transpose(1, 0, 2).reshape(batch, shards * rows)
    else:
        pairs = [
            [jnp.concatenate(halves, axis=0) for halves in zip(one, two)]
            for one, two in zip(pairs_one, pairs_two)
        ]
        grad_fc2 = reduce_rows(*pairs[0], True)
        grad_fc1 = reduce_rows(*pairs[1], False)
        grad_wout = reduce_rows(*pairs[2], True)
        grad_qkv = reduce_rows(*pairs[3], True)
        packed = lax.all_gather(packed, ("shard", "rep"), axis=0, tiled=True)
        own_mod = lax.dynamic_index_in_dim(
            packed[:, : grad_mod.shape[1]].reshape(shards, reps, batch, -1), rep, 1, keepdims=False
        ).reshape(shards * batch, -1)
        act_grad = matmul_t(own_mod, modulation_weight)
        act_grad = act_grad + lax.ppermute(act_grad, "section", [(0, 1), (1, 0)])
        came = exchange_shards(act_grad.reshape(shards, batch, rows))
        act_total = jnp.zeros((shards, batch, rows), jnp.float32)
        for step, block in enumerate(came):
            act_total = lax.dynamic_update_index_in_dim(
                act_total, block, (shard - step) % shards, 0
            )
        act_total = act_total.transpose(1, 0, 2).reshape(batch, shards * rows)

    boundary = jnp.concatenate(
        [
            jnp.where(first_section, grad_in_one, result_one),
            jnp.where(first_section, grad_in_two, result_two),
        ],
        axis=0,
    )[None]

    all_mod = packed[:, : grad_mod.shape[1]]
    all_act = packed[:, grad_mod.shape[1] :]
    act_rows = lax.dynamic_slice_in_dim(all_act, shard * rows, rows, 1)
    grad_ada = lax.dot_general(
        act_rows, all_mod, (((0,), (0,)), ((), ())), preferred_element_type=jnp.float32
    )
    _, silu_back = jax.vjp(jax.nn.silu, cond_float)
    grad_cond = silu_back(act_total)[0]
    return (
        boundary,
        grad_cond,
        grad_ada[None],
        grad_qkv[None],
        grad_wout[None],
        grad_fc1[None],
        grad_fc2[None],
    )


def solution(mesh):
    in_specs = (
        P(("shard", "rep"), None, None),
        P(("shard", "rep"), None),
        P("section", "shard", None),
        P("section", "shard", None),
        P("section", "shard", None),
        P("section", "shard", None),
        P("section", "shard", None),
        P(("shard", "rep"), None, None),
    )
    out_specs = (
        P("section", ("shard", "rep"), None, None),
        P(("shard", "rep"), None),
        P("section", "shard", None),
        P("section", "shard", None),
        P("section", "shard", None),
        P("section", "shard", None),
        P("section", "shard", None),
    )

    return jax.shard_map(body, mesh=mesh, in_specs=in_specs, out_specs=out_specs, check_vma=False)
```

```python
import functools

import jax
import jax.numpy as jnp
from jax import lax
from jax.experimental import pallas as pl
from jax.experimental.pallas import tpu as pltpu
from jax.sharding import PartitionSpec as P


D = 1152
HEADS = 16
HEAD_DIM = 72
LANES = 128


low = jnp.bfloat16


NT=(((1,),(1,)),((),())); TN=(((0,),(0,)),((),()))
def dot(a,b,dims=(((1,),(0,)),((),()))):
    return lax.dot_general(a,b,dims,preferred_element_type=jnp.float32)
def windows():
    for head in range(HEADS):
        start=head*HEAD_DIM; stop=start+HEAD_DIM
        first=start//LANES*LANES; last=-(-stop//LANES)*LANES
        yield first,last,start-first,stop-first
def head_mask(rows,first,last,begin,end):
    lane=lax.broadcasted_iota(jnp.int32,(rows,last-first),1)
    return (lane>=begin)&(lane<end)
def attention_kernel(project_ref,out_ref):
    rows=out_ref.shape[0]
    for first,last,begin,end in windows():
        mask=head_mask(rows,first,last,begin,end)
        q=project_ref[:,first:last]; k=project_ref[:,D+first:D+last]; v=project_ref[:,2*D+first:2*D+last]
        q=jnp.where(mask,q,jnp.zeros_like(q))
        s=dot(q,k,NT)*(HEAD_DIM**-0.5)
        e=jnp.exp(s-jnp.max(s,axis=1,keepdims=True))
        p=(e/jnp.sum(e,axis=1,keepdims=True)).astype(low)
        o=dot(p,v).astype(low)
        out_ref[:,first:last]=jnp.where(mask,o,out_ref[:,first:last])
def attention_back_kernel(project_ref,grad_ref,out_ref):
    rows=grad_ref.shape[0]; factor=HEAD_DIM**-0.5
    for first,last,begin,end in windows():
        mask=head_mask(rows,first,last,begin,end)
        q=project_ref[:,first:last]; k=project_ref[:,D+first:D+last]; v=project_ref[:,2*D+first:2*D+last]
        g=grad_ref[:,first:last]
        s=dot(jnp.where(mask,k,jnp.zeros_like(k)),q,NT)*factor
        e=jnp.exp(s-jnp.max(s,axis=0,keepdims=True))
        p=e/jnp.sum(e,axis=0,keepdims=True)
        dp=dot(jnp.where(mask,v,jnp.zeros_like(v)),g,NT)
        ds=(p*(dp-jnp.sum(dp*p,axis=0,keepdims=True))).astype(low)
        dq=(dot(ds,k,TN)*factor).astype(low)
        dk=(dot(ds,q)*factor).astype(low)
        dv=dot(p.astype(low),g).astype(low)
        for base,piece in ((0,dq),(D,dk),(2*D,dv)):
            here=slice(base+first,base+last)
            out_ref[:,here]=jnp.where(mask,piece,out_ref[:,here])
C0=0.7978845608028654; C1=0.044715
epsilon=1e-06
FEED_GROUPS=3
FEED_CHUNK=512

def act_of(u): return (0.5*u*(1.0+jnp.tanh(C0*(u+C1*(u*u*u))))).astype(low)
def slope_of(u):
    sq=u*u
    t=jnp.tanh(C0*(u+C1*(sq*u)))
    return 0.5*(1.0+t)+0.5*u*(1.0-t*t)*(C0*(1.0+3.0*C1*sq))
def center_scale(values):
    center=values-jnp.mean(values,axis=-1,keepdims=True)
    scale=lax.rsqrt(jnp.mean(center*center,axis=-1,keepdims=True)+epsilon)
    return center*scale,scale
def norm_back(normed,scale,grad):
    mean_grad=jnp.mean(grad,axis=-1,keepdims=True)
    mean_dot=jnp.mean(grad*normed,axis=-1,keepdims=True)
    return (grad-mean_grad-normed*mean_dot)*scale
def chunks_of(span): return [slice(a,a+FEED_CHUNK) for a in range(0,span,FEED_CHUNK)]

class Copies:
    def __init__(self,sems): self.sems=sems; self.made=[]
    def start(self,src,dst):
        copy=pltpu.make_async_copy(src,dst,self.sems.at[len(self.made)])
        copy.start(); self.made.append(copy)
        return copy
    def wait_all(self):
        for copy in self.made: copy.wait()

def forward_kernel(x_ref,mod_ref,wqkv,wout,w1,w2,
        first_out,project_out,att_out,branch_out,middle_out,second_out,u_out,h_out,f_out,y_out,y_low_out,
        wqkv_v,wout_v,w1_v,w2_v,first_v,project_v,att_v,branch_v,middle_v,second_v,u_v,h_v,f_v,y_v,y_low_v,in_sems,out_sems):
    width=wqkv_v.shape[2]; group=w1_v.shape[2]
    come=Copies(in_sems); leave=Copies(out_sems)
    project_in=[come.start(wqkv.at[:,i*width:(i+1)*width],wqkv_v.at[i]) for i in range(3)]
    out_in=come.start(wout,wout_v)
    feed_in=[(come.start(w1.at[:,i*group:(i+1)*group],w1_v.at[i]),come.start(w2.at[i*group:(i+1)*group],w2_v.at[i])) for i in range(FEED_GROUPS)]
    shift_one,scale_one,gate_one,shift_two,scale_two,gate_two=(mod_ref[:,i*D:(i+1)*D] for i in range(6))
    x=x_ref[...].astype(jnp.float32)
    first_v[...]=(center_scale(x)[0]*(1.0+scale_one)+shift_one).astype(low)
    leave.start(first_v,first_out)
    for i in range(3):
        project_in[i].wait()
        project_v[:,i*width:(i+1)*width]=dot(first_v[...],wqkv_v[i]).astype(low)
    leave.start(project_v,project_out)
    attention_kernel(project_v,att_v)
    leave.start(att_v,att_out)
    out_in.wait()
    branch=dot(att_v[...],wout_v[...])
    branch_v[...]=branch
    leave.start(branch_v,branch_out)
    middle=x_ref[...].astype(jnp.float32)+gate_one*branch
    middle_v[...]=middle
    leave.start(middle_v,middle_out)
    second_v[...]=(center_scale(middle)[0]*(1.0+scale_two)+shift_two).astype(low)
    leave.start(second_v,second_out)
    for i in range(FEED_GROUPS):
        for copy in feed_in[i]: copy.wait()
        prev=None
        def back(p,u):
            h=act_of(u); h_v[i,:,p]=h
            part=dot(h,w2_v[i,p,:])
            if i==0 and p.start==0: f_v[...]=part
            else: f_v[...]+=part
        for p in chunks_of(group):
            u=dot(second_v[...],w1_v[i,:,p]); u_v[i,:,p]=u
            if prev is not None: back(*prev)
            prev=(p,u)
        back(*prev)
        leave.start(u_v.at[i],u_out.at[:,i*group:(i+1)*group])
        leave.start(h_v.at[i],h_out.at[:,i*group:(i+1)*group])
    y=middle_v[...]+gate_two*f_v[...]
    y_v[...]=y
    y_low_v[...]=y.astype(low)
    leave.start(y_low_v,y_low_out)
    leave.start(f_v,f_out)
    leave.start(y_v,y_out)
    leave.wait_all()

def backward_kernel(g_ref,mod_ref,x_ref,feed_out,middle,branch,u,project,wqkv,wout,w1,w2,
        mod_out,df_out,du_out,do_out,dproject_out,dx_out,dx_low_out,
        feed_v,middle_v,branch_v,u_v,project_v,wqkv_v,wout_v,w1_v,w2_v,df_v,du_v,do_v,datt_v,dproject_v,acc_v,dx_v,dx_low_v,in_sems,out_sems):
    group=w1_v.shape[2]
    come=Copies(in_sems); leave=Copies(out_sems)
    feed_in=[]
    for i in range(FEED_GROUPS):
        feed_in.append((come.start(w2.at[i*group:(i+1)*group],w2_v.at[i]),come.start(u.at[:,i*group:(i+1)*group],u_v.at[i]),
            come.start(w1.at[:,i*group:(i+1)*group],w1_v.at[i])))
        if i==0: feed_copy=come.start(feed_out,feed_v)
    middle_in=come.start(middle,middle_v); branch_in=come.start(branch,branch_v)
    out_in=come.start(wout,wout_v); project_in=come.start(project,project_v); qkv_in=come.start(wqkv,wqkv_v)
    _,scale_one,gate_one,_,scale_two,gate_two=(mod_ref[:,i*D:(i+1)*D] for i in range(6))
    total=lambda values: jnp.sum(values,axis=0,keepdims=True)
    df_v[...]=(gate_two*g_ref[...].astype(jnp.float32)).astype(low)
    leave.start(df_v,df_out)
    for i in range(FEED_GROUPS):
        for copy in feed_in[i]: copy.wait()
        prev=None
        def back(p,dh):
            du=(dh*slope_of(u_v[i,:,p])).astype(low); du_v[i,:,p]=du
            part=dot(du,w1_v[i,:,p],NT)
            if i==0 and p.start==0: acc_v[...]=part
            else: acc_v[...]+=part
        for p in chunks_of(group):
            dh=dot(df_v[...],w2_v[i,p,:],NT)
            if prev is not None: back(*prev)
            prev=(p,dh)
        back(*prev)
        leave.start(du_v.at[i],du_out.at[:,i*group:(i+1)*group])
    feed_copy.wait(); middle_in.wait(); branch_in.wait()
    g=g_ref[...].astype(jnp.float32)
    mod_out[:,5*D:6*D]=total(g*feed_v[...])
    dh=acc_v[...]
    normed,inverse=center_scale(middle_v[...])
    mod_out[:,3*D:4*D]=total(dh)
    mod_out[:,4*D:5*D]=total(dh*normed)
    dmiddle=g+norm_back(normed,inverse,dh*(1.0+scale_two))
    dx_v[...]=dmiddle
    mod_out[:,2*D:3*D]=total(dmiddle*branch_v[...])
    do_v[...]=(gate_one*dmiddle).astype(low)
    leave.start(do_v,do_out)
    out_in.wait()
    datt_v[...]=dot(do_v[...],wout_v[...],NT).astype(low)
    project_in.wait()
    attention_back_kernel(project_v,datt_v,dproject_v)
    leave.start(dproject_v,dproject_out)
    qkv_in.wait()
    dh=dot(dproject_v[...],wqkv_v[...],NT)
    normed,inverse=center_scale(x_ref[...].astype(jnp.float32))
    mod_out[:,0*D:1*D]=total(dh)
    mod_out[:,1*D:2*D]=total(dh*normed)
    dx=dx_v[...]+norm_back(normed,inverse,dh*(1.0+scale_one))
    dx_v[...]=dx
    dx_low_v[...]=dx.astype(low)
    leave.start(dx_low_v,dx_low_out)
    leave.start(dx_v,dx_out)
    leave.wait_all()

LAYER_VMEM=60 * 1024 * 1024
def forward_layer(x,mod,weights):
    _,_,w1,_=weights
    t,d=x.shape; ff=w1.shape[1]; group=ff//FEED_GROUPS
    made=lambda width,dtype: jax.ShapeDtypeStruct((t,width),dtype)
    f32=jnp.float32
    v=pltpu.VMEM
    any_=pl.BlockSpec(memory_space=pl.ANY); inside=pl.BlockSpec(memory_space=pltpu.VMEM)
    return pl.pallas_call(forward_kernel,in_specs=[inside,inside]+[any_]*4,out_specs=[any_]*11,
        out_shape=[made(d,low),made(3*d,low),made(d,low),made(d,f32),made(d,f32),made(d,low),made(ff,f32),made(ff,low),made(d,f32),made(d,f32),made(d,low)],
        scratch_shapes=[v((3,d,d),low),v((d,d),low),v((FEED_GROUPS,d,group),low),v((FEED_GROUPS,group,d),low),
            v((t,d),low),v((t,3*d),low),v((t,d),low),v((t,d),f32),v((t,d),f32),v((t,d),low),
            v((FEED_GROUPS,t,group),f32),v((FEED_GROUPS,t,group),low),v((t,d),f32),v((t,d),f32),v((t,d),low),
            pltpu.SemaphoreType.DMA((4+2*FEED_GROUPS,)),pltpu.SemaphoreType.DMA((9+2*FEED_GROUPS,))],
        compiler_params=pltpu.CompilerParams(vmem_limit_bytes=LAYER_VMEM),
        cost_estimate=pl.CostEstimate(flops=2*t*d*(4*d+2*ff)+4*t*t*d,bytes_accessed=2*d*(4*d+2*ff)+t*(30*d+6*ff),transcendentals=t*(ff+HEADS*t)),
        )(x,mod,*weights)
def backward_layer(g,mod,x,kept,weights):
    _,project,_,branch,middle,_,u,_,feed_out=kept
    _,_,w1,_=weights
    t,d=x.shape; ff=w1.shape[1]; group=ff//FEED_GROUPS
    made=lambda width,dtype: jax.ShapeDtypeStruct((t,width),dtype)
    f32=jnp.float32
    v=pltpu.VMEM
    any_=pl.BlockSpec(memory_space=pl.ANY); inside=pl.BlockSpec(memory_space=pltpu.VMEM)
    return pl.pallas_call(backward_kernel,in_specs=[inside]*3+[any_]*9,out_specs=[inside]+[any_]*6,
        out_shape=[jax.ShapeDtypeStruct((1,6*d),f32),made(d,low),made(ff,low),made(d,low),made(3*d,low),made(d,f32),made(d,low)],
        scratch_shapes=[v((t,d),f32),v((t,d),f32),v((t,d),f32),v((FEED_GROUPS,t,group),f32),v((t,3*d),low),
            v((d,3*d),low),v((d,d),low),v((FEED_GROUPS,d,group),low),v((FEED_GROUPS,group,d),low),
            v((t,d),low),v((FEED_GROUPS,t,group),low),v((t,d),low),v((t,d),low),v((t,3*d),low),v((t,d),f32),v((t,d),f32),v((t,d),low),
            pltpu.SemaphoreType.DMA((6+3*FEED_GROUPS,)),pltpu.SemaphoreType.DMA((5+FEED_GROUPS,))],
        compiler_params=pltpu.CompilerParams(vmem_limit_bytes=LAYER_VMEM),
        cost_estimate=pl.CostEstimate(flops=2*t*d*(4*d+2*ff)+10*t*t*d,bytes_accessed=2*d*(4*d+2*ff)+t*(30*d+6*ff),transcendentals=t*(ff+HEADS*t)),
        )(g,mod,x,feed_out,middle,branch,u,project,*weights)


def matmul(left, right):
    return jnp.dot(left, right, preferred_element_type=jnp.float32)


def matmul_t(left, right):
    return lax.dot_general(
        left, right, (((1,), (1,)), ((), ())), preferred_element_type=jnp.float32
    )


def bits_of(count):
    bits = count.bit_length() - 1
    assert 1 << bits == count
    return bits


def swap(value, axis, bit):
    count = lax.axis_size(axis)
    return lax.ppermute(value, axis, [(i, i ^ (1 << bit)) for i in range(count)])


def reduce_rows(left, right, reps_first):
    shard_bits = bits_of(lax.axis_size("shard"))
    rep_bits = bits_of(lax.axis_size("rep"))
    shard_stages = [("shard", bit) for bit in range(shard_bits)]
    rep_stages = [("rep", bit) for bit in range(rep_bits)]
    if reps_first:
        stages = rep_stages + shard_stages
    else:
        stages = rep_stages[:1] + shard_stages + rep_stages[1:]
    names = [("shard", bit) for bit in reversed(range(shard_bits))]
    names += [("rep", bit) for bit in reversed(range(rep_bits))]
    tokens, depth = left.shape
    inner = depth >> len(names)
    part = None
    for axis, bit in stages:
        place = names.index((axis, bit))
        mine = (lax.axis_index(axis) >> bit) & 1
        if part is None:
            spread = left.T.reshape((2,) * len(names) + (inner, tokens))
            away = lax.dynamic_index_in_dim(spread, 1 - mine, place, keepdims=False)
            stay = lax.dynamic_index_in_dim(spread, mine, place, keepdims=False)
            away = matmul(away.reshape(-1, tokens), right).astype(low)
            came = swap(away, axis, bit)
            part = (matmul(stay.reshape(-1, tokens), right) + came.astype(jnp.float32)).astype(low)
            names.pop(place)
            part = part.reshape((2,) * len(names) + (inner, right.shape[1]))
        else:
            away = lax.dynamic_index_in_dim(part, 1 - mine, place, keepdims=False)
            stay = lax.dynamic_index_in_dim(part, mine, place, keepdims=False)
            came = swap(away, axis, bit)
            part = (stay.astype(jnp.float32) + came.astype(jnp.float32)).astype(low)
            names.pop(place)
    whole = lax.all_gather(part, "rep", axis=0, tiled=True)
    return whole.astype(jnp.float32)


def exchange_shards(blocks):
    count = lax.axis_size("shard")
    me = lax.axis_index("shard")
    came = [lax.dynamic_index_in_dim(blocks, me, 0, keepdims=False)]
    for step in range(1, count):
        block = lax.dynamic_index_in_dim(blocks, (me + step) % count, 0, keepdims=False)
        came.append(
            lax.ppermute(block, "shard", [(i, (i + step) % count) for i in range(count)])
        )
    return came


MESH=pl.DeviceIdType.MESH

def gather_kernel(shards,reps,arrays,chunks,*refs):
    ins=refs[:arrays]; outs=refs[arrays:2*arrays]; bounce=refs[2*arrays:3*arrays]
    line_send,line_recv,rep_send,rep_recv,local_in,local_out=refs[3*arrays:]
    count=len(chunks)
    def own_piece(c,rep):
        index,rows,columns=chunks[c]
        return ins[index].at[rep,rows,columns]
    def piece_of(c,owner,rep):
        index,rows,columns=chunks[c]
        return outs[index].at[owner,rep,rows,columns]
    s=lax.axis_index("shard"); r=lax.axis_index("rep")
    bits=reps.bit_length()-1
    barrier=pltpu.get_barrier_semaphore()
    for side in (-1,1):
        there=(s+side>=0)&(s+side<shards)
        @pl.when(there)
        def _():
            pl.semaphore_signal(barrier,inc=1,device_id={"shard":s+side},device_id_type=MESH)
    for bit in range(bits):
        pl.semaphore_signal(barrier,inc=1,device_id={"rep":r^(1<<bit)},device_id_type=MESH)
    for c in range(arrays):
        pltpu.make_async_copy(ins[c],bounce[c],local_in.at[c]).start()
    pl.semaphore_wait(barrier,bits+jnp.minimum(s,1)+jnp.minimum(shards-1-s,1))
    sides=((0,1),(1,-1))

    def line(way,step,hop,c,owner):
        src=own_piece(c,r) if hop==0 else piece_of(c,owner,r)
        return pltpu.make_async_remote_copy(src_ref=src,dst_ref=piece_of(c,owner,r),
            send_sem=line_send.at[way,hop,c],recv_sem=line_recv.at[way,hop,c],
            device_id={"shard":s+step},device_id_type=MESH)
    def side_copy(bit,mask,c,owner):
        piece=piece_of(c,owner,r^mask)
        return pltpu.make_async_remote_copy(src_ref=piece,dst_ref=piece,
            send_sem=rep_send.at[bit,mask,owner,c],recv_sem=rep_recv.at[mask|(1<<bit),owner,c],
            device_id={"rep":r^(1<<bit)},device_id_type=MESH)
    def low_bit(mask): return bits if mask==0 else (mask&-mask).bit_length()-1
    def arrived(mask,c,owner):
        bit=low_bit(mask)
        piece=piece_of(c,owner,r^mask)
        pltpu.make_async_remote_copy(src_ref=piece,dst_ref=piece,send_sem=rep_send.at[bit,mask^(1<<bit),owner,c],
            recv_sem=rep_recv.at[mask,owner,c],device_id={"rep":r^(1<<bit)},device_id_type=MESH).wait_recv()
    for c in range(count):
        for way,step in sides:
            @pl.when((s+step>=0)&(s+step<shards))
            def _(): line(way,step,0,c,s).start()
    for c in range(arrays):
        pltpu.make_async_copy(ins[c],bounce[c],local_in.at[c]).wait()
        pltpu.make_async_copy(bounce[c],outs[c].at[s],local_out.at[c]).start()
    events=[(hop,c) for hop in range(1,shards) for c in range(count)]
    relays=[m for m in range(1,reps) if low_bit(m)>0]
    depth=max([m.bit_count() for m in relays],default=0)
    for index in range(len(events)+depth):
        if index<len(events):
            hop,c=events[index]
            for way,step in sides:
                owner=s-step*hop
                @pl.when((owner>=0)&(owner<shards))
                def _():
                    line(way,step,hop-1,c,owner).wait_recv()
                    if hop+1<shards:
                        @pl.when((s+step>=0)&(s+step<shards))
                        def _(): line(way,step,hop,c,owner).start()
                    for bit in reversed(range(bits)):
                        side_copy(bit,0,c,owner).start()
        for mask in relays:
            late=index-mask.bit_count()
            if 0<=late<len(events):
                hop,c=events[late]
                for way,step in sides:
                    owner=s-step*hop
                    @pl.when((owner>=0)&(owner<shards))
                    def _():
                        arrived(mask,c,owner)
                        for bit in reversed(range(low_bit(mask))):
                            side_copy(bit,mask,c,owner).start()
    for hop,c in events:
        for way,step in sides:
            owner=s-step*hop
            @pl.when((owner>=0)&(owner<shards))
            def _():
                for mask in range(1,reps):
                    if low_bit(mask)==0: arrived(mask,c,owner)
                for mask in range(reps):
                    for bit in range(low_bit(mask)): side_copy(bit,mask,c,owner).wait_send()
                if hop+1<shards:
                    @pl.when((s+step>=0)&(s+step<shards))
                    def _(): line(way,step,hop,c,owner).wait_send()
    for c in range(count):
        for way,step in sides:
            @pl.when((s+step>=0)&(s+step<shards))
            def _(): line(way,step,0,c,s).wait_send()
    for c in range(arrays):
        pltpu.make_async_copy(bounce[c],outs[c].at[s],local_out.at[c]).wait()

def gather_all(weights):
    shards=lax.axis_size("shard"); reps=lax.axis_size("rep"); bits=reps.bit_length()-1
    assert 1<<bits==reps
    arrays=len(weights)
    views=[w.reshape(reps,w.shape[0]//reps,w.shape[1]) for w in weights]
    def split(index,columns=None,rows=None):
        depth,width=views[index].shape[1:]
        return (index,slice(*(rows or (0,depth))),slice(*(columns or (0,width))))
    deep=views[3].shape[1]; halves=((0,deep//2),(deep//2,deep)) if deep%16==0 else ((0,deep),)
    chunks=[split(1),split(0,(D,3*D)),split(2,(0,2*D)),split(2,(2*D,4*D))]
    chunks+=[split(3,rows=half) for half in halves]+[split(0,(0,D))]
    count=len(chunks)
    any_=pl.BlockSpec(memory_space=pl.ANY)
    outs=pl.pallas_call(functools.partial(gather_kernel,shards,reps,arrays,chunks),
        in_specs=[any_]*arrays,out_specs=[any_]*arrays,
        out_shape=[jax.ShapeDtypeStruct((shards,)+v.shape,v.dtype) for v in views],
        scratch_shapes=[pltpu.VMEM(v.shape,v.dtype) for v in views]+[
            pltpu.SemaphoreType.DMA((2,shards-1,count)),pltpu.SemaphoreType.DMA((2,shards-1,count)),
            pltpu.SemaphoreType.DMA((bits,reps,shards,count)),pltpu.SemaphoreType.DMA((reps,shards,count)),
            pltpu.SemaphoreType.DMA((arrays,)),pltpu.SemaphoreType.DMA((arrays,))],
        compiler_params=pltpu.CompilerParams(collective_id=1,has_side_effects=True),
        )(*views)
    return tuple(o.reshape(shards*w.shape[0],w.shape[1]) for o,w in zip(outs,weights))


NAMES=("s1","s0","r1","r0")
REP_FIRST=("r0","r1","s0","s1")
SHARD_FIRST=("r0","s0","s1","r1")
KINDS=(REP_FIRST,SHARD_FIRST,REP_FIRST)
WIDTH=D//3
LAGS=(1,3,3,2)

def block_sources(first_t,second_t,att_t,hidden_t,feed,pre,branch,project):
    pairs=[(hidden_t.at[:,j],feed) for j in range(4)]
    pairs+=[(second_t,pre.at[:,j*D:(j+1)*D]) for j in range(4)]
    pairs+=[(att_t,branch)]
    pairs+=[(first_t,project.at[:,j*D:(j+1)*D]) for j in range(3)]
    return pairs

def reduce_kernel(blocks,*refs):
    ins=(refs[:8],refs[8:16]); parts,ada,outs,notes,act_out=refs[16:19],refs[19],refs[20:24],refs[24],refs[25]
    (left,right,left_sem,right_sem,part,came,send_sem,recv_sem,kept,final,
     final_sem,near_send,near_recv,far_send,far_recv,fwd_send,fwd_recv,note_send,note_recv,
     notes_in,ada_in,ada_sem,_,blocks_out,blocks_in,act_send,act_recv,note)=unpack(refs[26:])
    c=lax.axis_index("section")
    s=lax.axis_index("shard"); r=lax.axis_index("rep")
    bit={"s1":s//2,"s0":lax.rem(s,2),"r1":r//2,"r0":lax.rem(r,2)}
    peer={"s1":{"shard":lax.rem(s+2,4)},"s0":{"shard":s+1-2*lax.rem(s,2)},
          "r1":{"rep":lax.rem(r+2,4)},"r0":{"rep":r+1-2*lax.rem(r,2)}}
    across=lax.rem(r+2,4)
    one,two,act=(part[...] for part in parts)
    ours=jnp.concatenate([jnp.where(c==0,one,two),jnp.where(c==0,two,one)],axis=0).astype(low)
    note[:,:6*D]=ours
    note[:,6*D:]=act
    notes_in[s*4+r]=jnp.concatenate([ours,act],axis=1)
    barrier=pltpu.get_barrier_semaphore()
    others=[(a,b) for a in range(4) for b in range(4) if a or b]
    def note_copy(index,a,b):
        return pltpu.make_async_remote_copy(src_ref=note,dst_ref=notes_in.at[s*4+r],send_sem=note_send.at[index],recv_sem=note_recv.at[index],
            device_id={"shard":s^a,"rep":r^b},device_id_type=MESH)
    for a,b in others:
        pl.semaphore_signal(barrier,inc=1,device_id={"shard":s^a,"rep":r^b},device_id_type=MESH)
    for a in range(4):
        pl.semaphore_signal(barrier,inc=1,device_id={"section":1-c,"shard":s^a},device_id_type=MESH)
    sources=[block_sources(*half) for half in ins]
    span=left.shape[3]//2
    def load(index,slot):
        for here in range(blocks):
            @pl.when(index==here)
            def _():
                for half in range(2):
                    a,b=sources[half][here]
                    place=pl.ds(half*span,span)
                    pltpu.make_async_copy(a,left.at[slot,:,:,place],left_sem.at[slot]).start()
                    pltpu.make_async_copy(b,right.at[slot,place],right_sem.at[slot]).start()
    load(0,0)
    pltpu.make_async_copy(ada,ada_in,ada_sem).start()
    pl.semaphore_wait(barrier,len(others)+4)
    for index,(a,b) in enumerate(others): note_copy(index,a,b).start()
    def act_copy(index,a,other):
        section=1-c if other else c
        return pltpu.make_async_remote_copy(src_ref=blocks_out.at[s^a],dst_ref=blocks_in.at[c,s],send_sem=act_send.at[index],
            recv_sem=act_recv.at[index],device_id={"section":section,"shard":s^a},device_id_type=MESH)
    act_peers=[(a,other) for a in range(4) for other in (False,True) if a or other]
    def share_notes():
        for index,(a,b) in enumerate(others): note_copy(index,a,b).wait()
        pltpu.make_async_copy(ada,ada_in,ada_sem).wait()
        wide=lambda index: notes_in[index].astype(jnp.float32)
        notes_out=jnp.concatenate([wide(index) for index in range(16)],axis=0).astype(low)
        notes[...]=notes_out
        mine=jnp.concatenate([wide(shard*4+r)[:,:6*D] for shard in range(4)],axis=0).astype(low)
        grads=lax.dot_general(mine,ada_in[...],(((1,),(1,)),((),())),preferred_element_type=jnp.float32)
        span=grads.shape[0]//4
        for shard in range(4): blocks_out[shard]=grads[shard*span:(shard+1)*span]
        blocks_in[c,s]=blocks_out[s]
        for index,(a,other) in enumerate(act_peers): act_copy(index,a,other).start()
    units=3*blocks
    ends=[sum(LAGS[:k+1]) for k in range(4)]
    last=ends[3]

    def pick(ref,slot,names,name,value):
        place=names.index(name)
        return ref.at[(slot,)+(slice(None),)*place+(value,)]
    def exchange(stage,kind,u):
        order=KINDS[kind]; name=order[stage]
        names=[n for n in NAMES if n not in order[:stage]]
        buffers=part if stage==0 else kept[stage-1][order is SHARD_FIRST]
        depth=buffers.shape[0]
        src=pick(buffers,lax.rem(u,depth),names,name,1-bit[name])
        target=came[stage][order is SHARD_FIRST]
        ring=lax.rem(u,target.shape[0])
        return pltpu.make_async_remote_copy(src_ref=src,dst_ref=target.at[ring],
            send_sem=send_sem[stage].at[ring],recv_sem=recv_sem[stage].at[ring],
            device_id=peer[name],device_id_type=MESH)
    def receive(stage,kind,u):
        order=KINDS[kind]; name=order[stage]
        names=[n for n in NAMES if n not in order[:stage]]
        exchange(stage,kind,u).wait()
        buffers=part if stage==0 else kept[stage-1][order is SHARD_FIRST]
        own=pick(buffers,lax.rem(u,buffers.shape[0]),names,name,bit[name])
        target=came[stage][order is SHARD_FIRST]
        other=target.at[lax.rem(u,target.shape[0])]
        left_over=len(names)-1
        if stage<3:
            result=kept[stage][order is SHARD_FIRST]
            slot=lax.rem(u,result.shape[0])
        for flat in range(1<<left_over):
            where=tuple((flat>>k)&1 for k in reversed(range(left_over)))
            total=own[where].astype(jnp.float32)+other[where].astype(jnp.float32)
            if stage<3: result[(slot,)+where]=total.astype(low)
            else: final[lax.rem(u,final.shape[0])]=total.astype(low)
        if stage<3: exchange(stage+1,kind,u).start()
    grad_qkv,grad_wout,grad_fc1,grad_fc2=outs
    anywhere=grad_fc2.at[0,0,:,:WIDTH]
    def placed(u,kind,action):
        block=u//3
        def columns(first): return pl.ds(pl.multiple_of((block-first)*D+kind*WIDTH,128),WIDTH)
        here=slice(kind*WIDTH,(kind+1)*WIDTH)
        pl.when(block<4)(lambda: action(lambda who: grad_fc2.at[block,who,:,here]))
        pl.when((block>=4)&(block<8))(lambda: action(lambda who: grad_fc1.at[who,:,columns(4)]))
        pl.when(block==8)(lambda: action(lambda who: grad_wout.at[who,:,here]))
        pl.when(block>=9)(lambda: action(lambda who: grad_qkv.at[who,:,columns(9)]))
    def spread(u,target):
        src=final.at[lax.rem(u,final.shape[0])]
        return (pltpu.make_async_copy(src,target,final_sem.at[u]),
            pltpu.make_async_remote_copy(src_ref=src,dst_ref=target,send_sem=far_send.at[u],recv_sem=far_recv.at[u],
                device_id=peer["r1"],device_id_type=MESH),
            pltpu.make_async_remote_copy(src_ref=src,dst_ref=target,send_sem=near_send.at[u],recv_sem=near_recv.at[u],
                device_id=peer["r0"],device_id_type=MESH))
    def relay(u,piece):
        return pltpu.make_async_remote_copy(src_ref=piece,dst_ref=piece,send_sem=fwd_send.at[u],recv_sem=fwd_recv.at[u],
                device_id=peer["r0"],device_id_type=MESH)
    def compute(kind,block,u):
        slot=lax.rem(block,2)
        columns=right[slot,:,kind*WIDTH:(kind+1)*WIDTH]
        rows=left.shape[2]//4
        for shard in range(4):
            product=lax.dot_general(left[slot,shard],columns,(((1,),(0,)),((),())),preferred_element_type=jnp.float32)
            for rep in range(4):
                part[lax.rem(u,part.shape[0]),shard//2,shard%2,rep//2,rep%2]=product[rep*rows:(rep+1)*rows].astype(low)
        exchange(0,kind,u).start()

    total_steps=units+last+4
    iterations=-(-total_steps//3)
    def iteration(it,carry):
        @pl.when(it<blocks)
        def _():
            slot=lax.rem(it,2)
            pltpu.make_async_copy(left.at[slot],left.at[slot],left_sem.at[slot]).wait()
            pltpu.make_async_copy(right.at[slot],right.at[slot],right_sem.at[slot]).wait()
        for sub in range(3):
            step=3*it+sub
            def at(lag,action):
                kind=(sub-lag)%3
                unit=step-lag
                @pl.when((unit>=0)&(unit<units))
                def _(): action(kind,unit)
            def finish(kind,u):
                local,far,near=spread(u,anywhere)
                local.wait(); far.wait_send(); near.wait(); relay(u,anywhere).wait()
            at(last+3,finish)
            def pass_on(kind,u):
                spread(u,anywhere)[1].wait_recv()
                placed(u,kind,lambda where: relay(u,where(across)).start())
            at(last+2,pass_on)
            def finalize(kind,u):
                receive(3,kind,u)
                def start(where):
                    for copy in spread(u,where(r)): copy.start()
                placed(u,kind,start)
            at(ends[3],finalize)
            for stage in (2,1,0):
                at(ends[stage],functools.partial(receive,stage))
            if sub==0:
                load(it+1,lax.rem(it+1,2))
                pl.when(it==3)(share_notes)
            at(0,lambda kind,u: compute(kind,it,u))
        return carry
    lax.fori_loop(0,iterations,iteration,0)
    for index,(a,other) in enumerate(act_peers): act_copy(index,a,other).wait()
    act_out[...]=blocks_in[0]+blocks_in[1]

def unpack(refs):
    refs=list(refs)
    left,right,left_sem,right_sem,part=refs[:5]; refs=refs[5:]
    came=[(refs[0],refs[0]),(refs[1],refs[2]),(refs[3],refs[4]),(refs[5],refs[5])]; refs=refs[6:]
    send=refs[:4]; recv=refs[4:8]; refs=refs[8:]
    kept=[(refs[0],refs[0]),(refs[1],refs[2]),(refs[3],refs[4])]; refs=refs[5:]
    return (left,right,left_sem,right_sem,part,came,send,recv,kept,*refs)

def reduce_all(halves,grad_mods,act,ada):
    shards=lax.axis_size("shard"); reps=lax.axis_size("rep")
    rows=D//(shards*reps); group=D//shards
    blocks=12; units=3*blocks
    operands=[]
    for pairs in halves:
        (hidden,feed),(second,pre),(att,branch),(first,project)=pairs
        span=hidden.shape[0]
        operands+=[a.T.reshape(shards,group,span) for a in (first,second,att)]
        operands+=[hidden.T.reshape(shards,4,group,span),feed,pre,branch,project]
    tokens=2*span
    any_=pl.BlockSpec(memory_space=pl.ANY)
    piece=(rows,WIDTH)
    two=lambda count: (2,)*count+piece
    rings=[2*lag+1 for lag in LAGS]
    vm=lambda depth,shape: pltpu.VMEM((depth,)+shape,low)
    dma=pltpu.SemaphoreType.DMA
    keep=[lag+1 for lag in LAGS]
    inside=pl.BlockSpec(memory_space=pltpu.VMEM)
    batch=act.shape[0]; wide=7*D
    made=lambda shape,dtype: jax.ShapeDtypeStruct(shape,dtype)
    *grads,notes,act_grad=pl.pallas_call(functools.partial(reduce_kernel,blocks),
        in_specs=[any_]*16+[inside]*3+[any_],out_specs=[any_]*4+[inside,inside],
        out_shape=[made((reps,rows,3*D),low),made((reps,rows,D),low),made((reps,rows,4*D),low),made((4,reps,rows,D),low),
            made((shards*reps*batch,wide),low),made((shards,batch,group),jnp.float32)],
        scratch_shapes=[
            pltpu.VMEM((2,shards,group,tokens),low),pltpu.VMEM((2,tokens,D),low),dma((2,)),dma((2,)),
            vm(keep[0],two(4)),
            vm(rings[0],two(3)),vm(rings[1],two(2)),vm(rings[1],two(2)),vm(rings[2],two(1)),vm(rings[2],two(1)),vm(rings[3],two(0)),
            *[dma((ring,)) for ring in rings],*[dma((ring,)) for ring in rings],
            vm(keep[1],two(3)),vm(keep[2],two(2)),vm(keep[2],two(2)),vm(keep[3],two(1)),vm(keep[3],two(1)),
            vm(5,piece),
            *[dma((units,)) for _ in range(7)],dma((15,)),dma((15,)),
            pltpu.VMEM((shards*reps,batch,wide),low),pltpu.VMEM(ada.shape,low),dma(()),dma(()),
            pltpu.VMEM((shards,batch,group),jnp.float32),pltpu.VMEM((2,shards,batch,group),jnp.float32),dma((7,)),dma((7,)),pltpu.VMEM((batch,wide),low)],
        compiler_params=pltpu.CompilerParams(collective_id=2,has_side_effects=True),
        cost_estimate=pl.CostEstimate(flops=2*tokens*D*D*blocks,bytes_accessed=4*tokens*D*blocks,transcendentals=0),
        )(*operands,*grad_mods,act,ada)
    grads=[grad.reshape(-1,grad.shape[-1]).astype(jnp.float32) for grad in grads]
    return grads,notes,act_grad


def body(
    latents,
    cond,
    modulation_weight,
    query_key_value_weight,
    attention_output_weight,
    feed_first_weight,
    feed_second_weight,
    cotangent,
):
    first_section = lax.axis_index("section") == 0
    shard = lax.axis_index("shard")
    rep = lax.axis_index("rep")
    shards = lax.axis_size("shard")
    reps = lax.axis_size("rep")
    batch = latents.shape[0]
    modulation_weight = modulation_weight[0]
    rows = modulation_weight.shape[0]

    cond_float = cond.astype(jnp.float32)
    act = jax.nn.silu(cond_float).astype(low)
    came = exchange_shards(act.reshape(batch, shards, rows).transpose(1, 0, 2))
    partial = matmul(jnp.concatenate(came, axis=0), modulation_weight)
    partial = partial.reshape(shards, batch, -1)
    total = partial[0]
    for step in range(1, shards):
        total = total + lax.ppermute(
            partial[step], "shard", [(i, (i - step) % shards) for i in range(shards)]
        )
    weights = gather_all(
        (
            query_key_value_weight[0],
            attention_output_weight[0],
            feed_first_weight[0],
            feed_second_weight[0],
        )
    )

    forth = [(0, 1)]
    back = [(1, 0)]
    swapped = jnp.where(first_section, total[1:], total[:1])
    straight = jnp.where(first_section, total[:1], total[1:])
    *_, sent = forward_layer(latents[0], total[:1], weights)
    incoming = lax.ppermute(sent, "section", forth)
    input_one = jnp.where(first_section, latents[1], incoming)
    *kept_one, result_one, sent = forward_layer(input_one, swapped, weights)
    incoming = lax.ppermute(sent, "section", forth)
    *_, sent = backward_layer(cotangent[0], swapped, input_one, kept_one, weights)
    returning = lax.ppermute(sent, "section", back)
    incoming, sent = lax.optimization_barrier((incoming, sent))
    input_two = jnp.where(first_section, latents[0], incoming)
    *kept_two, result_two, _ = forward_layer(input_two, straight, weights)
    grad_result = jnp.where(first_section, returning, cotangent[1])
    mod_one, *grads_one, grad_in_one, sent = backward_layer(
        grad_result, straight, input_two, kept_two, weights
    )
    returning = lax.ppermute(sent, "section", back)
    grad_result = jnp.where(first_section, returning, cotangent[0])
    mod_two, *grads_two, grad_in_two, _ = backward_layer(
        grad_result, swapped, input_one, kept_one, weights
    )

    def products(kept, grads):
        first_in, _, attended, _, _, second_in, _, hidden, _ = kept
        grad_feed, grad_pre, grad_branch, grad_project = grads
        return (
            (hidden, grad_feed),
            (second_in, grad_pre),
            (attended, grad_branch),
            (first_in, grad_project),
        )

    kept_one, kept_two, _ = lax.optimization_barrier((kept_one, kept_two, sent))
    pairs_one, pairs_two = products(kept_two, grads_one), products(kept_one, grads_two)
    wide = mod_one.shape[1]
    if shards == 4 and reps == 4:
        (grad_qkv, grad_wout, grad_fc1, grad_fc2), packed, act_grad = reduce_all(
            (pairs_one, pairs_two), (mod_one, mod_two), act, modulation_weight
        )
        act_total = act_grad.transpose(1, 0, 2).reshape(batch, shards * rows)
    else:
        pairs = [
            [jnp.concatenate(halves, axis=0) for halves in zip(one, two)]
            for one, two in zip(pairs_one, pairs_two)
        ]
        grad_fc2 = reduce_rows(*pairs[0], True)
        grad_fc1 = reduce_rows(*pairs[1], False)
        grad_wout = reduce_rows(*pairs[2], True)
        grad_qkv = reduce_rows(*pairs[3], True)
        grad_mod = jnp.where(
            first_section,
            jnp.concatenate([mod_one, mod_two], axis=0),
            jnp.concatenate([mod_two, mod_one], axis=0),
        ).astype(low)
        packed = jnp.concatenate([grad_mod, act], axis=-1)
        packed = lax.all_gather(packed, ("shard", "rep"), axis=0, tiled=True)
        own_mod = lax.dynamic_index_in_dim(
            packed[:, : wide].reshape(shards, reps, batch, -1), rep, 1, keepdims=False
        ).reshape(shards * batch, -1)
        act_grad = matmul_t(own_mod, modulation_weight)
        act_grad = act_grad + lax.ppermute(act_grad, "section", [(0, 1), (1, 0)])
        came = exchange_shards(act_grad.reshape(shards, batch, rows))
        act_total = jnp.zeros((shards, batch, rows), jnp.float32)
        for step, block in enumerate(came):
            act_total = lax.dynamic_update_index_in_dim(
                act_total, block, (shard - step) % shards, 0
            )
        act_total = act_total.transpose(1, 0, 2).reshape(batch, shards * rows)

    boundary = jnp.stack(
        [
            jnp.where(first_section, grad_in_one, result_one),
            jnp.where(first_section, grad_in_two, result_two),
        ]
    )[None]

    all_mod = packed[:, : wide]
    all_act = packed[:, wide :]
    act_rows = lax.dynamic_slice_in_dim(all_act, shard * rows, rows, 1)
    grad_ada = lax.dot_general(
        act_rows, all_mod, (((0,), (0,)), ((), ())), preferred_element_type=jnp.float32
    )
    _, silu_back = jax.vjp(jax.nn.silu, cond_float)
    grad_cond = silu_back(act_total)[0]
    return (
        boundary,
        grad_cond,
        grad_ada[None],
        grad_qkv[None],
        grad_wout[None],
        grad_fc1[None],
        grad_fc2[None],
    )


def solution(mesh):
    in_specs = (
        P(("shard", "rep"), None, None),
        P(("shard", "rep"), None),
        P("section", "shard", None),
        P("section", "shard", None),
        P("section", "shard", None),
        P("section", "shard", None),
        P("section", "shard", None),
        P(("shard", "rep"), None, None),
    )
    out_specs = (
        P("section", ("shard", "rep"), None, None),
        P(("shard", "rep"), None),
        P("section", "shard", None),
        P("section", "shard", None),
        P("section", "shard", None),
        P("section", "shard", None),
        P("section", "shard", None),
    )

    return jax.shard_map(body, mesh=mesh, in_specs=in_specs, out_specs=out_specs, check_vma=False)
```

```python
import functools

import jax
import jax.numpy as jnp
from jax import lax
from jax.experimental import pallas as pl
from jax.experimental.pallas import tpu as pltpu
from jax.sharding import PartitionSpec as P


D = 1152
HEADS = 16
HEAD_DIM = 72
LANES = 128


low = jnp.bfloat16


NT=(((1,),(1,)),((),())); TN=(((0,),(0,)),((),()))
def dot(a,b,dims=(((1,),(0,)),((),()))):
    return lax.dot_general(a,b,dims,preferred_element_type=jnp.float32)
def windows():
    for head in range(HEADS):
        start=head*HEAD_DIM; stop=start+HEAD_DIM
        first=start//LANES*LANES; last=-(-stop//LANES)*LANES
        yield first,last,start-first,stop-first
def head_mask(rows,first,last,begin,end):
    lane=lax.broadcasted_iota(jnp.int32,(rows,last-first),1)
    return (lane>=begin)&(lane<end)
def attention_kernel(project_ref,out_ref):
    rows=out_ref.shape[0]
    for first,last,begin,end in windows():
        mask=head_mask(rows,first,last,begin,end)
        q=project_ref[:,first:last]; k=project_ref[:,D+first:D+last]; v=project_ref[:,2*D+first:2*D+last]
        q=jnp.where(mask,q,jnp.zeros_like(q))
        s=dot(q,k,NT)*(HEAD_DIM**-0.5)
        e=jnp.exp(s-jnp.max(s,axis=1,keepdims=True))
        p=(e/jnp.sum(e,axis=1,keepdims=True)).astype(low)
        o=dot(p,v).astype(low)
        out_ref[:,first:last]=jnp.where(mask,o,out_ref[:,first:last])
def attention_back_kernel(project_ref,grad_ref,out_ref):
    rows=grad_ref.shape[0]; factor=HEAD_DIM**-0.5
    for first,last,begin,end in windows():
        mask=head_mask(rows,first,last,begin,end)
        q=project_ref[:,first:last]; k=project_ref[:,D+first:D+last]; v=project_ref[:,2*D+first:2*D+last]
        g=grad_ref[:,first:last]
        s=dot(jnp.where(mask,k,jnp.zeros_like(k)),q,NT)*factor
        e=jnp.exp(s-jnp.max(s,axis=0,keepdims=True))
        p=e/jnp.sum(e,axis=0,keepdims=True)
        dp=dot(jnp.where(mask,v,jnp.zeros_like(v)),g,NT)
        ds=(p*(dp-jnp.sum(dp*p,axis=0,keepdims=True))).astype(low)
        dq=(dot(ds,k,TN)*factor).astype(low)
        dk=(dot(ds,q)*factor).astype(low)
        dv=dot(p.astype(low),g).astype(low)
        for base,piece in ((0,dq),(D,dk),(2*D,dv)):
            here=slice(base+first,base+last)
            out_ref[:,here]=jnp.where(mask,piece,out_ref[:,here])
C0=0.7978845608028654; C1=0.044715
epsilon=1e-06
FEED_GROUPS=3
FEED_CHUNK=512

def act_of(u): return (0.5*u*(1.0+jnp.tanh(C0*(u+C1*(u*u*u))))).astype(low)
def slope_of(u):
    sq=u*u
    t=jnp.tanh(C0*(u+C1*(sq*u)))
    return 0.5*(1.0+t)+0.5*u*(1.0-t*t)*(C0*(1.0+3.0*C1*sq))
def center_scale(values):
    center=values-jnp.mean(values,axis=-1,keepdims=True)
    scale=lax.rsqrt(jnp.mean(center*center,axis=-1,keepdims=True)+epsilon)
    return center*scale,scale
def norm_back(normed,scale,grad):
    mean_grad=jnp.mean(grad,axis=-1,keepdims=True)
    mean_dot=jnp.mean(grad*normed,axis=-1,keepdims=True)
    return (grad-mean_grad-normed*mean_dot)*scale
def chunks_of(span): return [slice(a,a+FEED_CHUNK) for a in range(0,span,FEED_CHUNK)]

class Copies:
    def __init__(self,sems): self.sems=sems; self.made=[]
    def start(self,src,dst):
        copy=pltpu.make_async_copy(src,dst,self.sems.at[len(self.made)])
        copy.start(); self.made.append(copy)
        return copy
    def wait_all(self):
        for copy in self.made: copy.wait()

def forward_kernel(x_ref,mod_ref,wqkv,wout,w1,w2,
        first_out,project_out,att_out,branch_out,middle_out,second_out,u_out,h_out,f_out,y_out,y_low_out,
        wqkv_v,wout_v,w1_v,w2_v,first_v,project_v,att_v,branch_v,middle_v,second_v,u_v,h_v,f_v,y_v,y_low_v,in_sems,out_sems):
    width=wqkv_v.shape[2]; group=w1_v.shape[2]
    come=Copies(in_sems); leave=Copies(out_sems)
    project_in=[come.start(wqkv.at[:,i*width:(i+1)*width],wqkv_v.at[i]) for i in range(3)]
    out_in=come.start(wout,wout_v)
    feed_in=[(come.start(w1.at[:,i*group:(i+1)*group],w1_v.at[i]),come.start(w2.at[i*group:(i+1)*group],w2_v.at[i])) for i in range(FEED_GROUPS)]
    shift_one,scale_one,gate_one,shift_two,scale_two,gate_two=(mod_ref[:,i*D:(i+1)*D] for i in range(6))
    x=x_ref[...].astype(jnp.float32)
    first_v[...]=(center_scale(x)[0]*(1.0+scale_one)+shift_one).astype(low)
    leave.start(first_v,first_out)
    for i in range(3):
        project_in[i].wait()
        project_v[:,i*width:(i+1)*width]=dot(first_v[...],wqkv_v[i]).astype(low)
    leave.start(project_v,project_out)
    attention_kernel(project_v,att_v)
    leave.start(att_v,att_out)
    out_in.wait()
    branch=dot(att_v[...],wout_v[...])
    branch_v[...]=branch
    leave.start(branch_v,branch_out)
    middle=x_ref[...].astype(jnp.float32)+gate_one*branch
    middle_v[...]=middle
    leave.start(middle_v,middle_out)
    second_v[...]=(center_scale(middle)[0]*(1.0+scale_two)+shift_two).astype(low)
    leave.start(second_v,second_out)
    for i in range(FEED_GROUPS):
        for copy in feed_in[i]: copy.wait()
        prev=None
        def back(p,u):
            h=act_of(u); h_v[i,:,p]=h
            part=dot(h,w2_v[i,p,:])
            if i==0 and p.start==0: f_v[...]=part
            else: f_v[...]+=part
        for p in chunks_of(group):
            u=dot(second_v[...],w1_v[i,:,p]); u_v[i,:,p]=u
            if prev is not None: back(*prev)
            prev=(p,u)
        back(*prev)
        leave.start(u_v.at[i],u_out.at[:,i*group:(i+1)*group])
        leave.start(h_v.at[i],h_out.at[:,i*group:(i+1)*group])
    y=middle_v[...]+gate_two*f_v[...]
    y_v[...]=y
    y_low_v[...]=y.astype(low)
    leave.start(y_low_v,y_low_out)
    leave.start(f_v,f_out)
    leave.start(y_v,y_out)
    leave.wait_all()

def backward_kernel(g_ref,mod_ref,x_ref,feed_out,middle,branch,u,project,wqkv,wout,w1,w2,
        mod_out,df_out,du_out,do_out,dproject_out,dx_out,dx_low_out,
        feed_v,middle_v,branch_v,u_v,project_v,wqkv_v,wout_v,w1_v,w2_v,df_v,du_v,do_v,datt_v,dproject_v,acc_v,dx_v,dx_low_v,in_sems,out_sems):
    group=w1_v.shape[2]
    come=Copies(in_sems); leave=Copies(out_sems)
    feed_in=[]
    for i in range(FEED_GROUPS):
        feed_in.append((come.start(w2.at[i*group:(i+1)*group],w2_v.at[i]),come.start(u.at[:,i*group:(i+1)*group],u_v.at[i]),
            come.start(w1.at[:,i*group:(i+1)*group],w1_v.at[i])))
        if i==0: feed_copy=come.start(feed_out,feed_v)
    middle_in=come.start(middle,middle_v); branch_in=come.start(branch,branch_v)
    out_in=come.start(wout,wout_v); project_in=come.start(project,project_v); qkv_in=come.start(wqkv,wqkv_v)
    _,scale_one,gate_one,_,scale_two,gate_two=(mod_ref[:,i*D:(i+1)*D] for i in range(6))
    total=lambda values: jnp.sum(values,axis=0,keepdims=True)
    df_v[...]=(gate_two*g_ref[...].astype(jnp.float32)).astype(low)
    leave.start(df_v,df_out)
    for i in range(FEED_GROUPS):
        for copy in feed_in[i]: copy.wait()
        prev=None
        def back(p,dh):
            du=(dh*slope_of(u_v[i,:,p])).astype(low); du_v[i,:,p]=du
            part=dot(du,w1_v[i,:,p],NT)
            if i==0 and p.start==0: acc_v[...]=part
            else: acc_v[...]+=part
        for p in chunks_of(group):
            dh=dot(df_v[...],w2_v[i,p,:],NT)
            if prev is not None: back(*prev)
            prev=(p,dh)
        back(*prev)
        leave.start(du_v.at[i],du_out.at[:,i*group:(i+1)*group])
    feed_copy.wait(); middle_in.wait(); branch_in.wait()
    g=g_ref[...].astype(jnp.float32)
    mod_out[:,5*D:6*D]=total(g*feed_v[...])
    dh=acc_v[...]
    normed,inverse=center_scale(middle_v[...])
    mod_out[:,3*D:4*D]=total(dh)
    mod_out[:,4*D:5*D]=total(dh*normed)
    dmiddle=g+norm_back(normed,inverse,dh*(1.0+scale_two))
    dx_v[...]=dmiddle
    mod_out[:,2*D:3*D]=total(dmiddle*branch_v[...])
    do_v[...]=(gate_one*dmiddle).astype(low)
    leave.start(do_v,do_out)
    out_in.wait()
    datt_v[...]=dot(do_v[...],wout_v[...],NT).astype(low)
    project_in.wait()
    attention_back_kernel(project_v,datt_v,dproject_v)
    leave.start(dproject_v,dproject_out)
    qkv_in.wait()
    dh=dot(dproject_v[...],wqkv_v[...],NT)
    normed,inverse=center_scale(x_ref[...].astype(jnp.float32))
    mod_out[:,0*D:1*D]=total(dh)
    mod_out[:,1*D:2*D]=total(dh*normed)
    dx=dx_v[...]+norm_back(normed,inverse,dh*(1.0+scale_one))
    dx_v[...]=dx
    dx_low_v[...]=dx.astype(low)
    leave.start(dx_low_v,dx_low_out)
    leave.start(dx_v,dx_out)
    leave.wait_all()

LAYER_VMEM=60 * 1024 * 1024
def forward_layer(x,mod,weights):
    _,_,w1,_=weights
    t,d=x.shape; ff=w1.shape[1]; group=ff//FEED_GROUPS
    made=lambda width,dtype: jax.ShapeDtypeStruct((t,width),dtype)
    f32=jnp.float32
    v=pltpu.VMEM
    any_=pl.BlockSpec(memory_space=pl.ANY); inside=pl.BlockSpec(memory_space=pltpu.VMEM)
    return pl.pallas_call(forward_kernel,in_specs=[inside,inside]+[any_]*4,out_specs=[any_]*11,
        out_shape=[made(d,low),made(3*d,low),made(d,low),made(d,f32),made(d,f32),made(d,low),made(ff,f32),made(ff,low),made(d,f32),made(d,f32),made(d,low)],
        scratch_shapes=[v((3,d,d),low),v((d,d),low),v((FEED_GROUPS,d,group),low),v((FEED_GROUPS,group,d),low),
            v((t,d),low),v((t,3*d),low),v((t,d),low),v((t,d),f32),v((t,d),f32),v((t,d),low),
            v((FEED_GROUPS,t,group),f32),v((FEED_GROUPS,t,group),low),v((t,d),f32),v((t,d),f32),v((t,d),low),
            pltpu.SemaphoreType.DMA((4+2*FEED_GROUPS,)),pltpu.SemaphoreType.DMA((9+2*FEED_GROUPS,))],
        compiler_params=pltpu.CompilerParams(vmem_limit_bytes=LAYER_VMEM),
        cost_estimate=pl.CostEstimate(flops=2*t*d*(4*d+2*ff)+4*t*t*d,bytes_accessed=2*d*(4*d+2*ff)+t*(30*d+6*ff),transcendentals=t*(ff+HEADS*t)),
        )(x,mod,*weights)
def backward_layer(g,mod,x,kept,weights):
    _,project,_,branch,middle,_,u,_,feed_out=kept
    _,_,w1,_=weights
    t,d=x.shape; ff=w1.shape[1]; group=ff//FEED_GROUPS
    made=lambda width,dtype: jax.ShapeDtypeStruct((t,width),dtype)
    f32=jnp.float32
    v=pltpu.VMEM
    any_=pl.BlockSpec(memory_space=pl.ANY); inside=pl.BlockSpec(memory_space=pltpu.VMEM)
    return pl.pallas_call(backward_kernel,in_specs=[inside]*3+[any_]*9,out_specs=[inside]+[any_]*6,
        out_shape=[jax.ShapeDtypeStruct((1,6*d),f32),made(d,low),made(ff,low),made(d,low),made(3*d,low),made(d,f32),made(d,low)],
        scratch_shapes=[v((t,d),f32),v((t,d),f32),v((t,d),f32),v((FEED_GROUPS,t,group),f32),v((t,3*d),low),
            v((d,3*d),low),v((d,d),low),v((FEED_GROUPS,d,group),low),v((FEED_GROUPS,group,d),low),
            v((t,d),low),v((FEED_GROUPS,t,group),low),v((t,d),low),v((t,d),low),v((t,3*d),low),v((t,d),f32),v((t,d),f32),v((t,d),low),
            pltpu.SemaphoreType.DMA((6+3*FEED_GROUPS,)),pltpu.SemaphoreType.DMA((5+FEED_GROUPS,))],
        compiler_params=pltpu.CompilerParams(vmem_limit_bytes=LAYER_VMEM),
        cost_estimate=pl.CostEstimate(flops=2*t*d*(4*d+2*ff)+10*t*t*d,bytes_accessed=2*d*(4*d+2*ff)+t*(30*d+6*ff),transcendentals=t*(ff+HEADS*t)),
        )(g,mod,x,feed_out,middle,branch,u,project,*weights)


def matmul(left, right):
    return jnp.dot(left, right, preferred_element_type=jnp.float32)


def matmul_t(left, right):
    return lax.dot_general(
        left, right, (((1,), (1,)), ((), ())), preferred_element_type=jnp.float32
    )


def bits_of(count):
    bits = count.bit_length() - 1
    assert 1 << bits == count
    return bits


def swap(value, axis, bit):
    count = lax.axis_size(axis)
    return lax.ppermute(value, axis, [(i, i ^ (1 << bit)) for i in range(count)])


def reduce_rows(left, right, reps_first):
    shard_bits = bits_of(lax.axis_size("shard"))
    rep_bits = bits_of(lax.axis_size("rep"))
    shard_stages = [("shard", bit) for bit in range(shard_bits)]
    rep_stages = [("rep", bit) for bit in range(rep_bits)]
    if reps_first:
        stages = rep_stages + shard_stages
    else:
        stages = rep_stages[:1] + shard_stages + rep_stages[1:]
    names = [("shard", bit) for bit in reversed(range(shard_bits))]
    names += [("rep", bit) for bit in reversed(range(rep_bits))]
    tokens, depth = left.shape
    inner = depth >> len(names)
    part = None
    for axis, bit in stages:
        place = names.index((axis, bit))
        mine = (lax.axis_index(axis) >> bit) & 1
        if part is None:
            spread = left.T.reshape((2,) * len(names) + (inner, tokens))
            away = lax.dynamic_index_in_dim(spread, 1 - mine, place, keepdims=False)
            stay = lax.dynamic_index_in_dim(spread, mine, place, keepdims=False)
            away = matmul(away.reshape(-1, tokens), right).astype(low)
            came = swap(away, axis, bit)
            part = (matmul(stay.reshape(-1, tokens), right) + came.astype(jnp.float32)).astype(low)
            names.pop(place)
            part = part.reshape((2,) * len(names) + (inner, right.shape[1]))
        else:
            away = lax.dynamic_index_in_dim(part, 1 - mine, place, keepdims=False)
            stay = lax.dynamic_index_in_dim(part, mine, place, keepdims=False)
            came = swap(away, axis, bit)
            part = (stay.astype(jnp.float32) + came.astype(jnp.float32)).astype(low)
            names.pop(place)
    whole = lax.all_gather(part, "rep", axis=0, tiled=True)
    return whole.astype(jnp.float32)


def exchange_shards(blocks):
    count = lax.axis_size("shard")
    me = lax.axis_index("shard")
    came = [lax.dynamic_index_in_dim(blocks, me, 0, keepdims=False)]
    for step in range(1, count):
        block = lax.dynamic_index_in_dim(blocks, (me + step) % count, 0, keepdims=False)
        came.append(
            lax.ppermute(block, "shard", [(i, (i + step) % count) for i in range(count)])
        )
    return came


MESH=pl.DeviceIdType.MESH

def gather_kernel(shards,reps,arrays,chunks,*refs):
    ins=refs[:arrays]; act,ada=refs[arrays:arrays+2]; refs=refs[arrays+2:]
    outs=refs[:arrays]; mod_out=refs[arrays]; refs=refs[arrays+1:]; bounce=refs[:arrays]
    (line_send,line_recv,rep_send,rep_recv,local_in,local_out,
     ada_v,acts_in,mod_send,mod_in,ada_sem,act_sems,mod_sems)=refs[arrays:]
    count=len(chunks)
    def own_piece(c,rep):
        index,rows,columns=chunks[c]
        return ins[index].at[rep,rows,columns]
    def piece_of(c,owner,rep):
        index,rows,columns=chunks[c]
        return outs[index].at[owner,rep,rows,columns]
    s=lax.axis_index("shard"); r=lax.axis_index("rep")
    bits=reps.bit_length()-1
    barrier=pltpu.get_barrier_semaphore()
    for other in range(1,shards):
        pl.semaphore_signal(barrier,inc=1,device_id={"shard":s^other},device_id_type=MESH)
    for bit in range(bits):
        pl.semaphore_signal(barrier,inc=1,device_id={"rep":r^(1<<bit)},device_id_type=MESH)
    for c in range(arrays):
        pltpu.make_async_copy(ins[c],bounce[c],local_in.at[c]).start()
    pltpu.make_async_copy(ada,ada_v,ada_sem).start()
    acts_in[s]=act[s]
    pl.semaphore_wait(barrier,bits+shards-1)
    def act_copy(other):
        return pltpu.make_async_remote_copy(src_ref=act.at[s^other],dst_ref=acts_in.at[s],send_sem=act_sems.at[0,other-1],
            recv_sem=act_sems.at[1,other-1],device_id={"shard":s^other},device_id_type=MESH)
    def mod_copy(other):
        return pltpu.make_async_remote_copy(src_ref=mod_send.at[s^other],dst_ref=mod_in.at[s],send_sem=mod_sems.at[0,other-1],
            recv_sem=mod_sems.at[1,other-1],device_id={"shard":s^other},device_id_type=MESH)
    for other in range(1,shards): act_copy(other).start()
    sides=((0,1),(1,-1))

    def line(way,step,hop,c,owner):
        src=own_piece(c,r) if hop==0 else piece_of(c,owner,r)
        return pltpu.make_async_remote_copy(src_ref=src,dst_ref=piece_of(c,owner,r),
            send_sem=line_send.at[way,hop,c],recv_sem=line_recv.at[way,hop,c],
            device_id={"shard":s+step},device_id_type=MESH)
    def side_copy(bit,mask,c,owner):
        piece=piece_of(c,owner,r^mask)
        return pltpu.make_async_remote_copy(src_ref=piece,dst_ref=piece,
            send_sem=rep_send.at[bit,mask,owner,c],recv_sem=rep_recv.at[mask|(1<<bit),owner,c],
            device_id={"rep":r^(1<<bit)},device_id_type=MESH)
    def low_bit(mask): return bits if mask==0 else (mask&-mask).bit_length()-1
    def arrived(mask,c,owner):
        bit=low_bit(mask)
        piece=piece_of(c,owner,r^mask)
        pltpu.make_async_remote_copy(src_ref=piece,dst_ref=piece,send_sem=rep_send.at[bit,mask^(1<<bit),owner,c],
            recv_sem=rep_recv.at[mask,owner,c],device_id={"rep":r^(1<<bit)},device_id_type=MESH).wait_recv()
    for c in range(count):
        for way,step in sides:
            @pl.when((s+step>=0)&(s+step<shards))
            def _(): line(way,step,0,c,s).start()
    for c in range(arrays):
        pltpu.make_async_copy(ins[c],bounce[c],local_in.at[c]).wait()
        pltpu.make_async_copy(bounce[c],outs[c].at[s],local_out.at[c]).start()
    for other in range(1,shards): act_copy(other).wait()
    pltpu.make_async_copy(ada,ada_v,ada_sem).wait()
    acts=jnp.concatenate([acts_in[k].astype(jnp.float32) for k in range(shards)],axis=0).astype(low)
    partial=dot(acts,ada_v[...])
    batch=act.shape[1]
    for k in range(shards): mod_send[k]=partial[k*batch:(k+1)*batch]
    mod_in[s]=mod_send[s]
    for other in range(1,shards): mod_copy(other).start()
    events=[(hop,c) for hop in range(1,shards) for c in range(count)]
    relays=[m for m in range(1,reps) if low_bit(m)>0]
    depth=max([m.bit_count() for m in relays],default=0)
    for index in range(len(events)+depth):
        if index<len(events):
            hop,c=events[index]
            for way,step in sides:
                owner=s-step*hop
                @pl.when((owner>=0)&(owner<shards))
                def _():
                    line(way,step,hop-1,c,owner).wait_recv()
                    if hop+1<shards:
                        @pl.when((s+step>=0)&(s+step<shards))
                        def _(): line(way,step,hop,c,owner).start()
                    for bit in reversed(range(bits)):
                        side_copy(bit,0,c,owner).start()
        for mask in relays:
            late=index-mask.bit_count()
            if 0<=late<len(events):
                hop,c=events[late]
                for way,step in sides:
                    owner=s-step*hop
                    @pl.when((owner>=0)&(owner<shards))
                    def _():
                        arrived(mask,c,owner)
                        for bit in reversed(range(low_bit(mask))):
                            side_copy(bit,mask,c,owner).start()
    for hop,c in events:
        for way,step in sides:
            owner=s-step*hop
            @pl.when((owner>=0)&(owner<shards))
            def _():
                for mask in range(1,reps):
                    if low_bit(mask)==0: arrived(mask,c,owner)
                for mask in range(reps):
                    for bit in range(low_bit(mask)): side_copy(bit,mask,c,owner).wait_send()
                if hop+1<shards:
                    @pl.when((s+step>=0)&(s+step<shards))
                    def _(): line(way,step,hop,c,owner).wait_send()
    for c in range(count):
        for way,step in sides:
            @pl.when((s+step>=0)&(s+step<shards))
            def _(): line(way,step,0,c,s).wait_send()
    for c in range(arrays):
        pltpu.make_async_copy(bounce[c],outs[c].at[s],local_out.at[c]).wait()
    for other in range(1,shards): mod_copy(other).wait()
    total=mod_in[0]
    for k in range(1,shards): total=total+mod_in[k]
    mod_out[...]=total

def gather_all(weights,act,ada):
    shards=lax.axis_size("shard"); reps=lax.axis_size("rep"); bits=reps.bit_length()-1
    assert 1<<bits==reps
    arrays=len(weights)
    views=[w.reshape(reps,w.shape[0]//reps,w.shape[1]) for w in weights]
    def split(index,columns=None,rows=None):
        depth,width=views[index].shape[1:]
        return (index,slice(*(rows or (0,depth))),slice(*(columns or (0,width))))
    deep=views[3].shape[1]; halves=((0,deep//2),(deep//2,deep)) if deep%16==0 else ((0,deep),)
    chunks=[split(1),split(0,(D,3*D)),split(2,(0,2*D)),split(2,(2*D,4*D))]
    chunks+=[split(3,rows=half) for half in halves]+[split(0,(0,D))]
    count=len(chunks)
    any_=pl.BlockSpec(memory_space=pl.ANY)
    inside=pl.BlockSpec(memory_space=pltpu.VMEM)
    batch=act.shape[1]
    *outs,modulation=pl.pallas_call(functools.partial(gather_kernel,shards,reps,arrays,chunks),
        in_specs=[any_]*arrays+[inside,any_],out_specs=[any_]*arrays+[inside],
        out_shape=[jax.ShapeDtypeStruct((shards,)+v.shape,v.dtype) for v in views]+[jax.ShapeDtypeStruct((batch,ada.shape[1]),jnp.float32)],
        scratch_shapes=[pltpu.VMEM(v.shape,v.dtype) for v in views]+[
            pltpu.SemaphoreType.DMA((2,shards-1,count)),pltpu.SemaphoreType.DMA((2,shards-1,count)),
            pltpu.SemaphoreType.DMA((bits,reps,shards,count)),pltpu.SemaphoreType.DMA((reps,shards,count)),
            pltpu.SemaphoreType.DMA((arrays,)),pltpu.SemaphoreType.DMA((arrays,)),
            pltpu.VMEM(ada.shape,low),pltpu.VMEM(act.shape,low),pltpu.VMEM((shards,batch,ada.shape[1]),jnp.float32),
            pltpu.VMEM((shards,batch,ada.shape[1]),jnp.float32),pltpu.SemaphoreType.DMA(()),
            pltpu.SemaphoreType.DMA((2,shards-1)),pltpu.SemaphoreType.DMA((2,shards-1))],
        compiler_params=pltpu.CompilerParams(collective_id=1,has_side_effects=True),
        )(*views,act,ada)
    return tuple(o.reshape(shards*w.shape[0],w.shape[1]) for o,w in zip(outs,weights)),modulation


NAMES=("s1","s0","r1","r0")
REP_FIRST=("r0","r1","s0","s1")
SHARD_FIRST=("r0","s0","s1","r1")
KINDS=(REP_FIRST,SHARD_FIRST,REP_FIRST)
WIDTH=D//3
LAGS=(1,3,3,2)

def block_sources(first_t,second_t,att_t,hidden_t,feed,pre,branch,project):
    pairs=[(hidden_t.at[:,j],feed) for j in range(4)]
    pairs+=[(second_t,pre.at[:,j*D:(j+1)*D]) for j in range(4)]
    pairs+=[(att_t,branch)]
    pairs+=[(first_t,project.at[:,j*D:(j+1)*D]) for j in range(3)]
    return pairs

def reduce_kernel(blocks,*refs):
    ins=(refs[:8],refs[8:16]); parts,ada,outs,notes,act_out=refs[16:19],refs[19],refs[20:24],refs[24],refs[25]
    (left,right,left_sem,right_sem,part,came,send_sem,recv_sem,kept,final,
     final_sem,near_send,near_recv,far_send,far_recv,fwd_send,fwd_recv,note_send,note_recv,
     notes_in,ada_in,ada_sem,_,blocks_out,blocks_in,act_send,act_recv,note)=unpack(refs[26:])
    c=lax.axis_index("section")
    s=lax.axis_index("shard"); r=lax.axis_index("rep")
    bit={"s1":s//2,"s0":lax.rem(s,2),"r1":r//2,"r0":lax.rem(r,2)}
    peer={"s1":{"shard":lax.rem(s+2,4)},"s0":{"shard":s+1-2*lax.rem(s,2)},
          "r1":{"rep":lax.rem(r+2,4)},"r0":{"rep":r+1-2*lax.rem(r,2)}}
    across=lax.rem(r+2,4)
    one,two,act=(part[...] for part in parts)
    ours=jnp.concatenate([jnp.where(c==0,one,two),jnp.where(c==0,two,one)],axis=0).astype(low)
    note[:,:6*D]=ours
    note[:,6*D:]=act
    notes_in[s*4+r]=jnp.concatenate([ours,act],axis=1)
    barrier=pltpu.get_barrier_semaphore()
    others=[(a,b) for a in range(4) for b in range(4) if a or b]
    def note_copy(index,a,b):
        return pltpu.make_async_remote_copy(src_ref=note,dst_ref=notes_in.at[s*4+r],send_sem=note_send.at[index],recv_sem=note_recv.at[index],
            device_id={"shard":s^a,"rep":r^b},device_id_type=MESH)
    for a,b in others:
        pl.semaphore_signal(barrier,inc=1,device_id={"shard":s^a,"rep":r^b},device_id_type=MESH)
    for a in range(4):
        pl.semaphore_signal(barrier,inc=1,device_id={"section":1-c,"shard":s^a},device_id_type=MESH)
    sources=[block_sources(*half) for half in ins]
    span=left.shape[3]//2
    def load(index,slot):
        for here in range(blocks):
            @pl.when(index==here)
            def _():
                for half in range(2):
                    a,b=sources[half][here]
                    place=pl.ds(half*span,span)
                    pltpu.make_async_copy(a,left.at[slot,:,:,place],left_sem.at[slot]).start()
                    pltpu.make_async_copy(b,right.at[slot,place],right_sem.at[slot]).start()
    load(0,0)
    pltpu.make_async_copy(ada,ada_in,ada_sem).start()
    pl.semaphore_wait(barrier,len(others)+4)
    for index,(a,b) in enumerate(others): note_copy(index,a,b).start()
    def act_copy(index,a,other):
        section=1-c if other else c
        return pltpu.make_async_remote_copy(src_ref=blocks_out.at[s^a],dst_ref=blocks_in.at[c,s],send_sem=act_send.at[index],
            recv_sem=act_recv.at[index],device_id={"section":section,"shard":s^a},device_id_type=MESH)
    act_peers=[(a,other) for a in range(4) for other in (False,True) if a or other]
    def share_notes():
        for index,(a,b) in enumerate(others): note_copy(index,a,b).wait()
        pltpu.make_async_copy(ada,ada_in,ada_sem).wait()
        wide=lambda index: notes_in[index].astype(jnp.float32)
        notes_out=jnp.concatenate([wide(index) for index in range(16)],axis=0).astype(low)
        notes[...]=notes_out
        mine=jnp.concatenate([wide(shard*4+r)[:,:6*D] for shard in range(4)],axis=0).astype(low)
        grads=lax.dot_general(mine,ada_in[...],(((1,),(1,)),((),())),preferred_element_type=jnp.float32)
        span=grads.shape[0]//4
        for shard in range(4): blocks_out[shard]=grads[shard*span:(shard+1)*span]
        blocks_in[c,s]=blocks_out[s]
        for index,(a,other) in enumerate(act_peers): act_copy(index,a,other).start()
    units=3*blocks
    ends=[sum(LAGS[:k+1]) for k in range(4)]
    last=ends[3]

    def pick(ref,slot,names,name,value):
        place=names.index(name)
        return ref.at[(slot,)+(slice(None),)*place+(value,)]
    def exchange(stage,kind,u):
        order=KINDS[kind]; name=order[stage]
        names=[n for n in NAMES if n not in order[:stage]]
        buffers=part if stage==0 else kept[stage-1][order is SHARD_FIRST]
        depth=buffers.shape[0]
        src=pick(buffers,lax.rem(u,depth),names,name,1-bit[name])
        target=came[stage][order is SHARD_FIRST]
        ring=lax.rem(u,target.shape[0])
        return pltpu.make_async_remote_copy(src_ref=src,dst_ref=target.at[ring],
            send_sem=send_sem[stage].at[ring],recv_sem=recv_sem[stage].at[ring],
            device_id=peer[name],device_id_type=MESH)
    def receive(stage,kind,u):
        order=KINDS[kind]; name=order[stage]
        names=[n for n in NAMES if n not in order[:stage]]
        exchange(stage,kind,u).wait()
        buffers=part if stage==0 else kept[stage-1][order is SHARD_FIRST]
        own=pick(buffers,lax.rem(u,buffers.shape[0]),names,name,bit[name])
        target=came[stage][order is SHARD_FIRST]
        other=target.at[lax.rem(u,target.shape[0])]
        left_over=len(names)-1
        if stage<3:
            result=kept[stage][order is SHARD_FIRST]
            slot=lax.rem(u,result.shape[0])
        for flat in range(1<<left_over):
            where=tuple((flat>>k)&1 for k in reversed(range(left_over)))
            total=own[where].astype(jnp.float32)+other[where].astype(jnp.float32)
            if stage<3: result[(slot,)+where]=total.astype(low)
            else: final[lax.rem(u,final.shape[0])]=total.astype(low)
        if stage<3: exchange(stage+1,kind,u).start()
    grad_qkv,grad_wout,grad_fc1,grad_fc2=outs
    anywhere=grad_fc2.at[0,0,:,:WIDTH]
    def placed(u,kind,action):
        block=u//3
        def columns(first): return pl.ds(pl.multiple_of((block-first)*D+kind*WIDTH,128),WIDTH)
        here=slice(kind*WIDTH,(kind+1)*WIDTH)
        pl.when(block<4)(lambda: action(lambda who: grad_fc2.at[block,who,:,here]))
        pl.when((block>=4)&(block<8))(lambda: action(lambda who: grad_fc1.at[who,:,columns(4)]))
        pl.when(block==8)(lambda: action(lambda who: grad_wout.at[who,:,here]))
        pl.when(block>=9)(lambda: action(lambda who: grad_qkv.at[who,:,columns(9)]))
    def spread(u,target):
        src=final.at[lax.rem(u,final.shape[0])]
        return (pltpu.make_async_copy(src,target,final_sem.at[u]),
            pltpu.make_async_remote_copy(src_ref=src,dst_ref=target,send_sem=far_send.at[u],recv_sem=far_recv.at[u],
                device_id=peer["r1"],device_id_type=MESH),
            pltpu.make_async_remote_copy(src_ref=src,dst_ref=target,send_sem=near_send.at[u],recv_sem=near_recv.at[u],
                device_id=peer["r0"],device_id_type=MESH))
    def relay(u,piece):
        return pltpu.make_async_remote_copy(src_ref=piece,dst_ref=piece,send_sem=fwd_send.at[u],recv_sem=fwd_recv.at[u],
                device_id=peer["r0"],device_id_type=MESH)
    def compute(kind,block,u):
        slot=lax.rem(block,2)
        columns=right[slot,:,kind*WIDTH:(kind+1)*WIDTH]
        rows=left.shape[2]//4
        for shard in range(4):
            product=lax.dot_general(left[slot,shard],columns,(((1,),(0,)),((),())),preferred_element_type=jnp.float32)
            for rep in range(4):
                part[lax.rem(u,part.shape[0]),shard//2,shard%2,rep//2,rep%2]=product[rep*rows:(rep+1)*rows].astype(low)
        exchange(0,kind,u).start()

    total_steps=units+last+4
    iterations=-(-total_steps//3)
    def iteration(it,carry):
        @pl.when(it<blocks)
        def _():
            slot=lax.rem(it,2)
            pltpu.make_async_copy(left.at[slot],left.at[slot],left_sem.at[slot]).wait()
            pltpu.make_async_copy(right.at[slot],right.at[slot],right_sem.at[slot]).wait()
        for sub in range(3):
            step=3*it+sub
            def at(lag,action):
                kind=(sub-lag)%3
                unit=step-lag
                @pl.when((unit>=0)&(unit<units))
                def _(): action(kind,unit)
            def finish(kind,u):
                local,far,near=spread(u,anywhere)
                local.wait(); far.wait_send(); near.wait(); relay(u,anywhere).wait()
            at(last+3,finish)
            def pass_on(kind,u):
                spread(u,anywhere)[1].wait_recv()
                placed(u,kind,lambda where: relay(u,where(across)).start())
            at(last+2,pass_on)
            def finalize(kind,u):
                receive(3,kind,u)
                def start(where):
                    for copy in spread(u,where(r)): copy.start()
                placed(u,kind,start)
            at(ends[3],finalize)
            for stage in (2,1,0):
                at(ends[stage],functools.partial(receive,stage))
            if sub==0:
                load(it+1,lax.rem(it+1,2))
                pl.when(it==3)(share_notes)
            at(0,lambda kind,u: compute(kind,it,u))
        return carry
    lax.fori_loop(0,iterations,iteration,0)
    for index,(a,other) in enumerate(act_peers): act_copy(index,a,other).wait()
    act_out[...]=blocks_in[0]+blocks_in[1]

def unpack(refs):
    refs=list(refs)
    left,right,left_sem,right_sem,part=refs[:5]; refs=refs[5:]
    came=[(refs[0],refs[0]),(refs[1],refs[2]),(refs[3],refs[4]),(refs[5],refs[5])]; refs=refs[6:]
    send=refs[:4]; recv=refs[4:8]; refs=refs[8:]
    kept=[(refs[0],refs[0]),(refs[1],refs[2]),(refs[3],refs[4])]; refs=refs[5:]
    return (left,right,left_sem,right_sem,part,came,send,recv,kept,*refs)

def reduce_all(halves,grad_mods,act,ada):
    shards=lax.axis_size("shard"); reps=lax.axis_size("rep")
    rows=D//(shards*reps); group=D//shards
    blocks=12; units=3*blocks
    operands=[]
    for pairs in halves:
        (hidden,feed),(second,pre),(att,branch),(first,project)=pairs
        span=hidden.shape[0]
        operands+=[a.T.reshape(shards,group,span) for a in (first,second,att)]
        operands+=[hidden.T.reshape(shards,4,group,span),feed,pre,branch,project]
    tokens=2*span
    any_=pl.BlockSpec(memory_space=pl.ANY)
    piece=(rows,WIDTH)
    two=lambda count: (2,)*count+piece
    rings=[2*lag+1 for lag in LAGS]
    vm=lambda depth,shape: pltpu.VMEM((depth,)+shape,low)
    dma=pltpu.SemaphoreType.DMA
    keep=[lag+1 for lag in LAGS]
    inside=pl.BlockSpec(memory_space=pltpu.VMEM)
    batch=act.shape[0]; wide=7*D
    made=lambda shape,dtype: jax.ShapeDtypeStruct(shape,dtype)
    *grads,notes,act_grad=pl.pallas_call(functools.partial(reduce_kernel,blocks),
        in_specs=[any_]*16+[inside]*3+[any_],out_specs=[any_]*4+[inside,inside],
        out_shape=[made((reps,rows,3*D),low),made((reps,rows,D),low),made((reps,rows,4*D),low),made((4,reps,rows,D),low),
            made((shards*reps*batch,wide),low),made((shards,batch,group),jnp.float32)],
        scratch_shapes=[
            pltpu.VMEM((2,shards,group,tokens),low),pltpu.VMEM((2,tokens,D),low),dma((2,)),dma((2,)),
            vm(keep[0],two(4)),
            vm(rings[0],two(3)),vm(rings[1],two(2)),vm(rings[1],two(2)),vm(rings[2],two(1)),vm(rings[2],two(1)),vm(rings[3],two(0)),
            *[dma((ring,)) for ring in rings],*[dma((ring,)) for ring in rings],
            vm(keep[1],two(3)),vm(keep[2],two(2)),vm(keep[2],two(2)),vm(keep[3],two(1)),vm(keep[3],two(1)),
            vm(5,piece),
            *[dma((units,)) for _ in range(7)],dma((15,)),dma((15,)),
            pltpu.VMEM((shards*reps,batch,wide),low),pltpu.VMEM(ada.shape,low),dma(()),dma(()),
            pltpu.VMEM((shards,batch,group),jnp.float32),pltpu.VMEM((2,shards,batch,group),jnp.float32),dma((7,)),dma((7,)),pltpu.VMEM((batch,wide),low)],
        compiler_params=pltpu.CompilerParams(collective_id=2,has_side_effects=True),
        cost_estimate=pl.CostEstimate(flops=2*tokens*D*D*blocks,bytes_accessed=4*tokens*D*blocks,transcendentals=0),
        )(*operands,*grad_mods,act,ada)
    grads=[grad.reshape(-1,grad.shape[-1]).astype(jnp.float32) for grad in grads]
    return grads,notes,act_grad


def body(
    latents,
    cond,
    modulation_weight,
    query_key_value_weight,
    attention_output_weight,
    feed_first_weight,
    feed_second_weight,
    cotangent,
):
    first_section = lax.axis_index("section") == 0
    shard = lax.axis_index("shard")
    rep = lax.axis_index("rep")
    shards = lax.axis_size("shard")
    reps = lax.axis_size("rep")
    batch = latents.shape[0]
    modulation_weight = modulation_weight[0]
    rows = modulation_weight.shape[0]

    cond_float = cond.astype(jnp.float32)
    act = jax.nn.silu(cond_float).astype(low)
    blocks = act.reshape(batch, shards, rows).transpose(1, 0, 2)
    weights, total = gather_all(
        (
            query_key_value_weight[0],
            attention_output_weight[0],
            feed_first_weight[0],
            feed_second_weight[0],
        ),
        blocks,
        modulation_weight,
    )

    forth = [(0, 1)]
    back = [(1, 0)]
    swapped = jnp.where(first_section, total[1:], total[:1])
    straight = jnp.where(first_section, total[:1], total[1:])
    *_, sent = forward_layer(latents[0], total[:1], weights)
    incoming = lax.ppermute(sent, "section", forth)
    input_one = jnp.where(first_section, latents[1], incoming)
    *kept_one, result_one, sent = forward_layer(input_one, swapped, weights)
    incoming = lax.ppermute(sent, "section", forth)
    *_, sent = backward_layer(cotangent[0], swapped, input_one, kept_one, weights)
    returning = lax.ppermute(sent, "section", back)
    incoming, sent = lax.optimization_barrier((incoming, sent))
    input_two = jnp.where(first_section, latents[0], incoming)
    *kept_two, result_two, _ = forward_layer(input_two, straight, weights)
    grad_result = jnp.where(first_section, returning, cotangent[1])
    mod_one, *grads_one, grad_in_one, sent = backward_layer(
        grad_result, straight, input_two, kept_two, weights
    )
    returning = lax.ppermute(sent, "section", back)
    grad_result = jnp.where(first_section, returning, cotangent[0])
    mod_two, *grads_two, grad_in_two, _ = backward_layer(
        grad_result, swapped, input_one, kept_one, weights
    )

    def products(kept, grads):
        first_in, _, attended, _, _, second_in, _, hidden, _ = kept
        grad_feed, grad_pre, grad_branch, grad_project = grads
        return (
            (hidden, grad_feed),
            (second_in, grad_pre),
            (attended, grad_branch),
            (first_in, grad_project),
        )

    kept_one, kept_two, _ = lax.optimization_barrier((kept_one, kept_two, sent))
    pairs_one, pairs_two = products(kept_two, grads_one), products(kept_one, grads_two)
    wide = mod_one.shape[1]
    if shards == 4 and reps == 4:
        (grad_qkv, grad_wout, grad_fc1, grad_fc2), packed, act_grad = reduce_all(
            (pairs_one, pairs_two), (mod_one, mod_two), act, modulation_weight
        )
        act_total = act_grad.transpose(1, 0, 2).reshape(batch, shards * rows)
    else:
        pairs = [
            [jnp.concatenate(halves, axis=0) for halves in zip(one, two)]
            for one, two in zip(pairs_one, pairs_two)
        ]
        grad_fc2 = reduce_rows(*pairs[0], True)
        grad_fc1 = reduce_rows(*pairs[1], False)
        grad_wout = reduce_rows(*pairs[2], True)
        grad_qkv = reduce_rows(*pairs[3], True)
        grad_mod = jnp.where(
            first_section,
            jnp.concatenate([mod_one, mod_two], axis=0),
            jnp.concatenate([mod_two, mod_one], axis=0),
        ).astype(low)
        packed = jnp.concatenate([grad_mod, act], axis=-1)
        packed = lax.all_gather(packed, ("shard", "rep"), axis=0, tiled=True)
        own_mod = lax.dynamic_index_in_dim(
            packed[:, : wide].reshape(shards, reps, batch, -1), rep, 1, keepdims=False
        ).reshape(shards * batch, -1)
        act_grad = matmul_t(own_mod, modulation_weight)
        act_grad = act_grad + lax.ppermute(act_grad, "section", [(0, 1), (1, 0)])
        came = exchange_shards(act_grad.reshape(shards, batch, rows))
        act_total = jnp.zeros((shards, batch, rows), jnp.float32)
        for step, block in enumerate(came):
            act_total = lax.dynamic_update_index_in_dim(
                act_total, block, (shard - step) % shards, 0
            )
        act_total = act_total.transpose(1, 0, 2).reshape(batch, shards * rows)

    boundary = jnp.stack(
        [
            jnp.where(first_section, grad_in_one, result_one),
            jnp.where(first_section, grad_in_two, result_two),
        ]
    )[None]

    all_mod = packed[:, : wide]
    all_act = packed[:, wide :]
    act_rows = lax.dynamic_slice_in_dim(all_act, shard * rows, rows, 1)
    grad_ada = lax.dot_general(
        act_rows, all_mod, (((0,), (0,)), ((), ())), preferred_element_type=jnp.float32
    )
    _, silu_back = jax.vjp(jax.nn.silu, cond_float)
    grad_cond = silu_back(act_total)[0]
    return (
        boundary,
        grad_cond,
        grad_ada[None],
        grad_qkv[None],
        grad_wout[None],
        grad_fc1[None],
        grad_fc2[None],
    )


def solution(mesh):
    in_specs = (
        P(("shard", "rep"), None, None),
        P(("shard", "rep"), None),
        P("section", "shard", None),
        P("section", "shard", None),
        P("section", "shard", None),
        P("section", "shard", None),
        P("section", "shard", None),
        P(("shard", "rep"), None, None),
    )
    out_specs = (
        P("section", ("shard", "rep"), None, None),
        P(("shard", "rep"), None),
        P("section", "shard", None),
        P("section", "shard", None),
        P("section", "shard", None),
        P("section", "shard", None),
        P("section", "shard", None),
    )

    return jax.shard_map(body, mesh=mesh, in_specs=in_specs, out_specs=out_specs, check_vma=False)
```

```python
import functools

import jax
import jax.numpy as jnp
from jax import lax
from jax.experimental import pallas as pl
from jax.experimental.pallas import tpu as pltpu
from jax.sharding import PartitionSpec as P


D = 1152
HEADS = 16
HEAD_DIM = 72
LANES = 128


low = jnp.bfloat16


NT=(((1,),(1,)),((),())); TN=(((0,),(0,)),((),()))
def dot(a,b,dims=(((1,),(0,)),((),()))):
    return lax.dot_general(a,b,dims,preferred_element_type=jnp.float32)
def windows():
    for head in range(HEADS):
        start=head*HEAD_DIM; stop=start+HEAD_DIM
        first=start//LANES*LANES; last=-(-stop//LANES)*LANES
        yield first,last,start-first,stop-first
def head_mask(rows,first,last,begin,end):
    lane=lax.broadcasted_iota(jnp.int32,(rows,last-first),1)
    return (lane>=begin)&(lane<end)
def attention_kernel(project_ref,out_ref):
    rows=out_ref.shape[0]
    for first,last,begin,end in windows():
        mask=head_mask(rows,first,last,begin,end)
        q=project_ref[:,first:last]; k=project_ref[:,D+first:D+last]; v=project_ref[:,2*D+first:2*D+last]
        q=jnp.where(mask,q,jnp.zeros_like(q))
        s=dot(q,k,NT)*(HEAD_DIM**-0.5)
        e=jnp.exp(s-jnp.max(s,axis=1,keepdims=True))
        p=(e/jnp.sum(e,axis=1,keepdims=True)).astype(low)
        o=dot(p,v).astype(low)
        out_ref[:,first:last]=jnp.where(mask,o,out_ref[:,first:last])
def attention_back_kernel(project_ref,grad_ref,out_ref):
    rows=grad_ref.shape[0]; factor=HEAD_DIM**-0.5
    for first,last,begin,end in windows():
        mask=head_mask(rows,first,last,begin,end)
        q=project_ref[:,first:last]; k=project_ref[:,D+first:D+last]; v=project_ref[:,2*D+first:2*D+last]
        g=grad_ref[:,first:last]
        s=dot(jnp.where(mask,k,jnp.zeros_like(k)),q,NT)*factor
        e=jnp.exp(s-jnp.max(s,axis=0,keepdims=True))
        p=e/jnp.sum(e,axis=0,keepdims=True)
        dp=dot(jnp.where(mask,v,jnp.zeros_like(v)),g,NT)
        ds=(p*(dp-jnp.sum(dp*p,axis=0,keepdims=True))).astype(low)
        dq=(dot(ds,k,TN)*factor).astype(low)
        dk=(dot(ds,q)*factor).astype(low)
        dv=dot(p.astype(low),g).astype(low)
        for base,piece in ((0,dq),(D,dk),(2*D,dv)):
            here=slice(base+first,base+last)
            out_ref[:,here]=jnp.where(mask,piece,out_ref[:,here])
C0=0.7978845608028654; C1=0.044715
epsilon=1e-06
FEED_GROUPS=3
FEED_CHUNK=512

def act_of(u): return (0.5*u*(1.0+jnp.tanh(C0*(u+C1*(u*u*u))))).astype(low)
def slope_of(u):
    sq=u*u
    t=jnp.tanh(C0*(u+C1*(sq*u)))
    return 0.5*(1.0+t)+0.5*u*(1.0-t*t)*(C0*(1.0+3.0*C1*sq))
def center_scale(values):
    center=values-jnp.mean(values,axis=-1,keepdims=True)
    scale=lax.rsqrt(jnp.mean(center*center,axis=-1,keepdims=True)+epsilon)
    return center*scale,scale
def norm_back(normed,scale,grad):
    mean_grad=jnp.mean(grad,axis=-1,keepdims=True)
    mean_dot=jnp.mean(grad*normed,axis=-1,keepdims=True)
    return (grad-mean_grad-normed*mean_dot)*scale
def chunks_of(span): return [slice(a,a+FEED_CHUNK) for a in range(0,span,FEED_CHUNK)]

class Copies:
    def __init__(self,sems): self.sems=sems; self.made=[]
    def start(self,src,dst):
        copy=pltpu.make_async_copy(src,dst,self.sems.at[len(self.made)])
        copy.start(); self.made.append(copy)
        return copy
    def wait_all(self):
        for copy in self.made: copy.wait()

def forward_kernel(x_ref,mod_ref,wqkv,wout,w1,w2,
        first_out,project_out,att_out,branch_out,middle_out,second_out,u_out,h_out,f_out,y_out,y_low_out,
        wqkv_v,wout_v,w1_v,w2_v,first_v,project_v,att_v,branch_v,middle_v,second_v,u_v,h_v,f_v,y_v,y_low_v,in_sems,out_sems):
    width=wqkv_v.shape[2]; group=w1_v.shape[2]
    come=Copies(in_sems); leave=Copies(out_sems)
    third=lambda i: pl.ds(pl.multiple_of(i*width,128),width)
    part_of=lambda i: pl.ds(pl.multiple_of(i*group,128),group)
    def project_copy(i): return pltpu.make_async_copy(wqkv.at[:,third(i)],wqkv_v.at[i],in_sems.at[1+i])
    def feed_copies(i):
        return (pltpu.make_async_copy(w1.at[:,part_of(i)],w1_v.at[i],in_sems.at[4+2*i]),
            pltpu.make_async_copy(w2.at[part_of(i)],w2_v.at[i],in_sems.at[5+2*i]))
    def feed_leave(i):
        return (pltpu.make_async_copy(u_v.at[i],u_out.at[:,part_of(i)],out_sems.at[9+2*i]),
            pltpu.make_async_copy(h_v.at[i],h_out.at[:,part_of(i)],out_sems.at[10+2*i]))
    for i in range(3): project_copy(i).start()
    out_in=come.start(wout,wout_v)
    for i in range(FEED_GROUPS):
        for copy in feed_copies(i): copy.start()
    shift_one,scale_one,gate_one,shift_two,scale_two,gate_two=(mod_ref[:,i*D:(i+1)*D] for i in range(6))
    x=x_ref[...].astype(jnp.float32)
    first_v[...]=(center_scale(x)[0]*(1.0+scale_one)+shift_one).astype(low)
    leave.start(first_v,first_out)
    def project_part(i,carry):
        project_copy(i).wait()
        project_v[:,third(i)]=dot(first_v[...],wqkv_v[i]).astype(low)
        return carry
    lax.fori_loop(0,3,project_part,0)
    leave.start(project_v,project_out)
    attention_kernel(project_v,att_v)
    leave.start(att_v,att_out)
    out_in.wait()
    branch=dot(att_v[...],wout_v[...])
    branch_v[...]=branch
    leave.start(branch_v,branch_out)
    middle=x_ref[...].astype(jnp.float32)+gate_one*branch
    middle_v[...]=middle
    leave.start(middle_v,middle_out)
    second_v[...]=(center_scale(middle)[0]*(1.0+scale_two)+shift_two).astype(low)
    leave.start(second_v,second_out)
    f_v[...]=jnp.zeros_like(f_v)
    def feed_part(i,carry):
        for copy in feed_copies(i): copy.wait()
        prev=None
        def back(p,u):
            h=act_of(u); h_v[i,:,p]=h
            f_v[...]+=dot(h,w2_v[i,p,:])
        for p in chunks_of(group):
            u=dot(second_v[...],w1_v[i,:,p]); u_v[i,:,p]=u
            if prev is not None: back(*prev)
            prev=(p,u)
        back(*prev)
        for copy in feed_leave(i): copy.start()
        return carry
    lax.fori_loop(0,FEED_GROUPS,feed_part,0)
    y=middle_v[...]+gate_two*f_v[...]
    y_v[...]=y
    y_low_v[...]=y.astype(low)
    leave.start(y_low_v,y_low_out)
    leave.start(f_v,f_out)
    leave.start(y_v,y_out)
    leave.wait_all()
    for i in range(FEED_GROUPS):
        for copy in feed_leave(i): copy.wait()

def backward_kernel(g_ref,mod_ref,x_ref,feed_out,middle,branch,u,project,wqkv,wout,w1,w2,
        mod_out,df_out,du_out,do_out,dproject_out,dx_out,dx_low_out,
        feed_v,middle_v,branch_v,u_v,project_v,wqkv_v,wout_v,w1_v,w2_v,df_v,du_v,do_v,datt_v,dproject_v,acc_v,dx_v,dx_low_v,in_sems,out_sems):
    group=w1_v.shape[2]
    come=Copies(in_sems); leave=Copies(out_sems)
    part_of=lambda i: pl.ds(pl.multiple_of(i*group,128),group)
    def feed_copies(i):
        return (pltpu.make_async_copy(w2.at[part_of(i)],w2_v.at[i],in_sems.at[6+3*i]),
            pltpu.make_async_copy(u.at[:,part_of(i)],u_v.at[i],in_sems.at[7+3*i]),
            pltpu.make_async_copy(w1.at[:,part_of(i)],w1_v.at[i],in_sems.at[8+3*i]))
    def feed_leave(i): return pltpu.make_async_copy(du_v.at[i],du_out.at[:,part_of(i)],out_sems.at[5+i])
    for i in range(FEED_GROUPS):
        for copy in feed_copies(i): copy.start()
        if i==0: feed_copy=come.start(feed_out,feed_v)
    middle_in=come.start(middle,middle_v); branch_in=come.start(branch,branch_v)
    out_in=come.start(wout,wout_v); project_in=come.start(project,project_v); qkv_in=come.start(wqkv,wqkv_v)
    _,scale_one,gate_one,_,scale_two,gate_two=(mod_ref[:,i*D:(i+1)*D] for i in range(6))
    total=lambda values: jnp.sum(values,axis=0,keepdims=True)
    df_v[...]=(gate_two*g_ref[...].astype(jnp.float32)).astype(low)
    leave.start(df_v,df_out)
    acc_v[...]=jnp.zeros_like(acc_v)
    def feed_part(i,carry):
        for copy in feed_copies(i): copy.wait()
        prev=None
        def back(p,dh):
            du=(dh*slope_of(u_v[i,:,p])).astype(low); du_v[i,:,p]=du
            acc_v[...]+=dot(du,w1_v[i,:,p],NT)
        for p in chunks_of(group):
            dh=dot(df_v[...],w2_v[i,p,:],NT)
            if prev is not None: back(*prev)
            prev=(p,dh)
        back(*prev)
        feed_leave(i).start()
        return carry
    lax.fori_loop(0,FEED_GROUPS,feed_part,0)
    feed_copy.wait(); middle_in.wait(); branch_in.wait()
    g=g_ref[...].astype(jnp.float32)
    mod_out[:,5*D:6*D]=total(g*feed_v[...])
    dh=acc_v[...]
    normed,inverse=center_scale(middle_v[...])
    mod_out[:,3*D:4*D]=total(dh)
    mod_out[:,4*D:5*D]=total(dh*normed)
    dmiddle=g+norm_back(normed,inverse,dh*(1.0+scale_two))
    dx_v[...]=dmiddle
    mod_out[:,2*D:3*D]=total(dmiddle*branch_v[...])
    do_v[...]=(gate_one*dmiddle).astype(low)
    leave.start(do_v,do_out)
    out_in.wait()
    datt_v[...]=dot(do_v[...],wout_v[...],NT).astype(low)
    project_in.wait()
    attention_back_kernel(project_v,datt_v,dproject_v)
    leave.start(dproject_v,dproject_out)
    qkv_in.wait()
    dh=dot(dproject_v[...],wqkv_v[...],NT)
    normed,inverse=center_scale(x_ref[...].astype(jnp.float32))
    mod_out[:,0*D:1*D]=total(dh)
    mod_out[:,1*D:2*D]=total(dh*normed)
    dx=dx_v[...]+norm_back(normed,inverse,dh*(1.0+scale_one))
    dx_v[...]=dx
    dx_low_v[...]=dx.astype(low)
    leave.start(dx_low_v,dx_low_out)
    leave.start(dx_v,dx_out)
    leave.wait_all()
    for i in range(FEED_GROUPS): feed_leave(i).wait()

LAYER_VMEM=60 * 1024 * 1024
def forward_layer(x,mod,weights):
    _,_,w1,_=weights
    t,d=x.shape; ff=w1.shape[1]; group=ff//FEED_GROUPS
    made=lambda width,dtype: jax.ShapeDtypeStruct((t,width),dtype)
    f32=jnp.float32
    v=pltpu.VMEM
    any_=pl.BlockSpec(memory_space=pl.ANY); inside=pl.BlockSpec(memory_space=pltpu.VMEM)
    return pl.pallas_call(forward_kernel,in_specs=[inside,inside]+[any_]*4,out_specs=[any_]*11,
        out_shape=[made(d,low),made(3*d,low),made(d,low),made(d,f32),made(d,f32),made(d,low),made(ff,f32),made(ff,low),made(d,f32),made(d,f32),made(d,low)],
        scratch_shapes=[v((3,d,d),low),v((d,d),low),v((FEED_GROUPS,d,group),low),v((FEED_GROUPS,group,d),low),
            v((t,d),low),v((t,3*d),low),v((t,d),low),v((t,d),f32),v((t,d),f32),v((t,d),low),
            v((FEED_GROUPS,t,group),f32),v((FEED_GROUPS,t,group),low),v((t,d),f32),v((t,d),f32),v((t,d),low),
            pltpu.SemaphoreType.DMA((4+2*FEED_GROUPS,)),pltpu.SemaphoreType.DMA((9+2*FEED_GROUPS,))],
        compiler_params=pltpu.CompilerParams(vmem_limit_bytes=LAYER_VMEM),
        cost_estimate=pl.CostEstimate(flops=2*t*d*(4*d+2*ff)+4*t*t*d,bytes_accessed=2*d*(4*d+2*ff)+t*(30*d+6*ff),transcendentals=t*(ff+HEADS*t)),
        )(x,mod,*weights)
def backward_layer(g,mod,x,kept,weights):
    _,project,_,branch,middle,_,u,_,feed_out=kept
    _,_,w1,_=weights
    t,d=x.shape; ff=w1.shape[1]; group=ff//FEED_GROUPS
    made=lambda width,dtype: jax.ShapeDtypeStruct((t,width),dtype)
    f32=jnp.float32
    v=pltpu.VMEM
    any_=pl.BlockSpec(memory_space=pl.ANY); inside=pl.BlockSpec(memory_space=pltpu.VMEM)
    return pl.pallas_call(backward_kernel,in_specs=[inside]*3+[any_]*9,out_specs=[inside]+[any_]*6,
        out_shape=[jax.ShapeDtypeStruct((1,6*d),f32),made(d,low),made(ff,low),made(d,low),made(3*d,low),made(d,f32),made(d,low)],
        scratch_shapes=[v((t,d),f32),v((t,d),f32),v((t,d),f32),v((FEED_GROUPS,t,group),f32),v((t,3*d),low),
            v((d,3*d),low),v((d,d),low),v((FEED_GROUPS,d,group),low),v((FEED_GROUPS,group,d),low),
            v((t,d),low),v((FEED_GROUPS,t,group),low),v((t,d),low),v((t,d),low),v((t,3*d),low),v((t,d),f32),v((t,d),f32),v((t,d),low),
            pltpu.SemaphoreType.DMA((6+3*FEED_GROUPS,)),pltpu.SemaphoreType.DMA((5+FEED_GROUPS,))],
        compiler_params=pltpu.CompilerParams(vmem_limit_bytes=LAYER_VMEM),
        cost_estimate=pl.CostEstimate(flops=2*t*d*(4*d+2*ff)+10*t*t*d,bytes_accessed=2*d*(4*d+2*ff)+t*(30*d+6*ff),transcendentals=t*(ff+HEADS*t)),
        )(g,mod,x,feed_out,middle,branch,u,project,*weights)


def matmul(left, right):
    return jnp.dot(left, right, preferred_element_type=jnp.float32)


def matmul_t(left, right):
    return lax.dot_general(
        left, right, (((1,), (1,)), ((), ())), preferred_element_type=jnp.float32
    )


def bits_of(count):
    bits = count.bit_length() - 1
    assert 1 << bits == count
    return bits


def swap(value, axis, bit):
    count = lax.axis_size(axis)
    return lax.ppermute(value, axis, [(i, i ^ (1 << bit)) for i in range(count)])


def reduce_rows(left, right, reps_first):
    shard_bits = bits_of(lax.axis_size("shard"))
    rep_bits = bits_of(lax.axis_size("rep"))
    shard_stages = [("shard", bit) for bit in range(shard_bits)]
    rep_stages = [("rep", bit) for bit in range(rep_bits)]
    if reps_first:
        stages = rep_stages + shard_stages
    else:
        stages = rep_stages[:1] + shard_stages + rep_stages[1:]
    names = [("shard", bit) for bit in reversed(range(shard_bits))]
    names += [("rep", bit) for bit in reversed(range(rep_bits))]
    tokens, depth = left.shape
    inner = depth >> len(names)
    part = None
    for axis, bit in stages:
        place = names.index((axis, bit))
        mine = (lax.axis_index(axis) >> bit) & 1
        if part is None:
            spread = left.T.reshape((2,) * len(names) + (inner, tokens))
            away = lax.dynamic_index_in_dim(spread, 1 - mine, place, keepdims=False)
            stay = lax.dynamic_index_in_dim(spread, mine, place, keepdims=False)
            away = matmul(away.reshape(-1, tokens), right).astype(low)
            came = swap(away, axis, bit)
            part = (matmul(stay.reshape(-1, tokens), right) + came.astype(jnp.float32)).astype(low)
            names.pop(place)
            part = part.reshape((2,) * len(names) + (inner, right.shape[1]))
        else:
            away = lax.dynamic_index_in_dim(part, 1 - mine, place, keepdims=False)
            stay = lax.dynamic_index_in_dim(part, mine, place, keepdims=False)
            came = swap(away, axis, bit)
            part = (stay.astype(jnp.float32) + came.astype(jnp.float32)).astype(low)
            names.pop(place)
    whole = lax.all_gather(part, "rep", axis=0, tiled=True)
    return whole.astype(jnp.float32)


def exchange_shards(blocks):
    count = lax.axis_size("shard")
    me = lax.axis_index("shard")
    came = [lax.dynamic_index_in_dim(blocks, me, 0, keepdims=False)]
    for step in range(1, count):
        block = lax.dynamic_index_in_dim(blocks, (me + step) % count, 0, keepdims=False)
        came.append(
            lax.ppermute(block, "shard", [(i, (i + step) % count) for i in range(count)])
        )
    return came


MESH=pl.DeviceIdType.MESH

def gather_kernel(shards,reps,arrays,chunks,*refs):
    ins=refs[:arrays]; act,ada=refs[arrays:arrays+2]; refs=refs[arrays+2:]
    outs=refs[:arrays]; mod_out=refs[arrays]; refs=refs[arrays+1:]; bounce=refs[:arrays]
    (line_send,line_recv,rep_send,rep_recv,local_in,local_out,
     ada_v,acts_in,mod_send,mod_in,ada_sem,act_sems,mod_sems)=refs[arrays:]
    count=len(chunks)
    def own_piece(c,rep):
        index,rows,columns=chunks[c]
        return ins[index].at[rep,rows,columns]
    def piece_of(c,owner,rep):
        index,rows,columns=chunks[c]
        return outs[index].at[owner,rep,rows,columns]
    s=lax.axis_index("shard"); r=lax.axis_index("rep")
    bits=reps.bit_length()-1
    barrier=pltpu.get_barrier_semaphore()
    for other in range(1,shards):
        pl.semaphore_signal(barrier,inc=1,device_id={"shard":s^other},device_id_type=MESH)
    for bit in range(bits):
        pl.semaphore_signal(barrier,inc=1,device_id={"rep":r^(1<<bit)},device_id_type=MESH)
    for c in range(arrays):
        pltpu.make_async_copy(ins[c],bounce[c],local_in.at[c]).start()
    pltpu.make_async_copy(ada,ada_v,ada_sem).start()
    acts_in[s]=act[s]
    pl.semaphore_wait(barrier,bits+shards-1)
    def act_copy(other):
        return pltpu.make_async_remote_copy(src_ref=act.at[s^other],dst_ref=acts_in.at[s],send_sem=act_sems.at[0,other-1],
            recv_sem=act_sems.at[1,other-1],device_id={"shard":s^other},device_id_type=MESH)
    def mod_copy(other):
        return pltpu.make_async_remote_copy(src_ref=mod_send.at[s^other],dst_ref=mod_in.at[s],send_sem=mod_sems.at[0,other-1],
            recv_sem=mod_sems.at[1,other-1],device_id={"shard":s^other},device_id_type=MESH)
    for other in range(1,shards): act_copy(other).start()
    sides=((0,1),(1,-1))

    def line(way,step,hop,c,owner):
        src=own_piece(c,r) if hop==0 else piece_of(c,owner,r)
        return pltpu.make_async_remote_copy(src_ref=src,dst_ref=piece_of(c,owner,r),
            send_sem=line_send.at[way,hop,c],recv_sem=line_recv.at[way,hop,c],
            device_id={"shard":s+step},device_id_type=MESH)
    def side_copy(bit,mask,c,owner):
        piece=piece_of(c,owner,r^mask)
        return pltpu.make_async_remote_copy(src_ref=piece,dst_ref=piece,
            send_sem=rep_send.at[bit,mask,owner,c],recv_sem=rep_recv.at[mask|(1<<bit),owner,c],
            device_id={"rep":r^(1<<bit)},device_id_type=MESH)
    def low_bit(mask): return bits if mask==0 else (mask&-mask).bit_length()-1
    def arrived(mask,c,owner):
        bit=low_bit(mask)
        piece=piece_of(c,owner,r^mask)
        pltpu.make_async_remote_copy(src_ref=piece,dst_ref=piece,send_sem=rep_send.at[bit,mask^(1<<bit),owner,c],
            recv_sem=rep_recv.at[mask,owner,c],device_id={"rep":r^(1<<bit)},device_id_type=MESH).wait_recv()
    for c in range(count):
        for way,step in sides:
            @pl.when((s+step>=0)&(s+step<shards))
            def _(): line(way,step,0,c,s).start()
    for c in range(arrays):
        pltpu.make_async_copy(ins[c],bounce[c],local_in.at[c]).wait()
        pltpu.make_async_copy(bounce[c],outs[c].at[s],local_out.at[c]).start()
    for other in range(1,shards): act_copy(other).wait()
    pltpu.make_async_copy(ada,ada_v,ada_sem).wait()
    acts=jnp.concatenate([acts_in[k].astype(jnp.float32) for k in range(shards)],axis=0).astype(low)
    partial=dot(acts,ada_v[...])
    batch=act.shape[1]
    for k in range(shards): mod_send[k]=partial[k*batch:(k+1)*batch]
    mod_in[s]=mod_send[s]
    for other in range(1,shards): mod_copy(other).start()
    events=[(hop,c) for hop in range(1,shards) for c in range(count)]
    relays=[m for m in range(1,reps) if low_bit(m)>0]
    depth=max([m.bit_count() for m in relays],default=0)
    for index in range(len(events)+depth):
        if index<len(events):
            hop,c=events[index]
            for way,step in sides:
                owner=s-step*hop
                @pl.when((owner>=0)&(owner<shards))
                def _():
                    line(way,step,hop-1,c,owner).wait_recv()
                    if hop+1<shards:
                        @pl.when((s+step>=0)&(s+step<shards))
                        def _(): line(way,step,hop,c,owner).start()
                    for bit in reversed(range(bits)):
                        side_copy(bit,0,c,owner).start()
        for mask in relays:
            late=index-mask.bit_count()
            if 0<=late<len(events):
                hop,c=events[late]
                for way,step in sides:
                    owner=s-step*hop
                    @pl.when((owner>=0)&(owner<shards))
                    def _():
                        arrived(mask,c,owner)
                        for bit in reversed(range(low_bit(mask))):
                            side_copy(bit,mask,c,owner).start()
    for hop,c in events:
        for way,step in sides:
            owner=s-step*hop
            @pl.when((owner>=0)&(owner<shards))
            def _():
                for mask in range(1,reps):
                    if low_bit(mask)==0: arrived(mask,c,owner)
                for mask in range(reps):
                    for bit in range(low_bit(mask)): side_copy(bit,mask,c,owner).wait_send()
                if hop+1<shards:
                    @pl.when((s+step>=0)&(s+step<shards))
                    def _(): line(way,step,hop,c,owner).wait_send()
    for c in range(count):
        for way,step in sides:
            @pl.when((s+step>=0)&(s+step<shards))
            def _(): line(way,step,0,c,s).wait_send()
    for c in range(arrays):
        pltpu.make_async_copy(bounce[c],outs[c].at[s],local_out.at[c]).wait()
    for other in range(1,shards): mod_copy(other).wait()
    total=mod_in[0]
    for k in range(1,shards): total=total+mod_in[k]
    mod_out[...]=total

def gather_all(weights,act,ada):
    shards=lax.axis_size("shard"); reps=lax.axis_size("rep"); bits=reps.bit_length()-1
    assert 1<<bits==reps
    arrays=len(weights)
    views=[w.reshape(reps,w.shape[0]//reps,w.shape[1]) for w in weights]
    def split(index,columns=None,rows=None):
        depth,width=views[index].shape[1:]
        return (index,slice(*(rows or (0,depth))),slice(*(columns or (0,width))))
    deep=views[3].shape[1]; halves=((0,deep//2),(deep//2,deep)) if deep%16==0 else ((0,deep),)
    chunks=[split(1),split(0,(D,3*D)),split(2,(0,2*D)),split(2,(2*D,4*D))]
    chunks+=[split(3,rows=half) for half in halves]+[split(0,(0,D))]
    count=len(chunks)
    any_=pl.BlockSpec(memory_space=pl.ANY)
    inside=pl.BlockSpec(memory_space=pltpu.VMEM)
    batch=act.shape[1]
    *outs,modulation=pl.pallas_call(functools.partial(gather_kernel,shards,reps,arrays,chunks),
        in_specs=[any_]*arrays+[inside,any_],out_specs=[any_]*arrays+[inside],
        out_shape=[jax.ShapeDtypeStruct((shards,)+v.shape,v.dtype) for v in views]+[jax.ShapeDtypeStruct((batch,ada.shape[1]),jnp.float32)],
        scratch_shapes=[pltpu.VMEM(v.shape,v.dtype) for v in views]+[
            pltpu.SemaphoreType.DMA((2,shards-1,count)),pltpu.SemaphoreType.DMA((2,shards-1,count)),
            pltpu.SemaphoreType.DMA((bits,reps,shards,count)),pltpu.SemaphoreType.DMA((reps,shards,count)),
            pltpu.SemaphoreType.DMA((arrays,)),pltpu.SemaphoreType.DMA((arrays,)),
            pltpu.VMEM(ada.shape,low),pltpu.VMEM(act.shape,low),pltpu.VMEM((shards,batch,ada.shape[1]),jnp.float32),
            pltpu.VMEM((shards,batch,ada.shape[1]),jnp.float32),pltpu.SemaphoreType.DMA(()),
            pltpu.SemaphoreType.DMA((2,shards-1)),pltpu.SemaphoreType.DMA((2,shards-1))],
        compiler_params=pltpu.CompilerParams(collective_id=1,has_side_effects=True),
        )(*views,act,ada)
    return tuple(o.reshape(shards*w.shape[0],w.shape[1]) for o,w in zip(outs,weights)),modulation


NAMES=("s1","s0","r1","r0")
REP_FIRST=("r0","r1","s0","s1")
SHARD_FIRST=("r0","s0","s1","r1")
KINDS=(REP_FIRST,SHARD_FIRST,REP_FIRST)
WIDTH=D//3
LAGS=(1,3,3,2)

def block_sources(first_t,second_t,att_t,hidden_t,feed,pre,branch,project):
    pairs=[(hidden_t.at[:,j],feed) for j in range(4)]
    pairs+=[(second_t,pre.at[:,j*D:(j+1)*D]) for j in range(4)]
    pairs+=[(att_t,branch)]
    pairs+=[(first_t,project.at[:,j*D:(j+1)*D]) for j in range(3)]
    return pairs

def reduce_kernel(blocks,*refs):
    ins=(refs[:8],refs[8:16]); parts,ada,outs,notes,act_out=refs[16:19],refs[19],refs[20:24],refs[24],refs[25]
    (left,right,left_sem,right_sem,part,came,send_sem,recv_sem,kept,final,
     final_sem,near_send,near_recv,far_send,far_recv,fwd_send,fwd_recv,note_send,note_recv,
     notes_in,ada_in,ada_sem,_,blocks_out,blocks_in,act_send,act_recv,note)=unpack(refs[26:])
    c=lax.axis_index("section")
    s=lax.axis_index("shard"); r=lax.axis_index("rep")
    bit={"s1":s//2,"s0":lax.rem(s,2),"r1":r//2,"r0":lax.rem(r,2)}
    peer={"s1":{"shard":lax.rem(s+2,4)},"s0":{"shard":s+1-2*lax.rem(s,2)},
          "r1":{"rep":lax.rem(r+2,4)},"r0":{"rep":r+1-2*lax.rem(r,2)}}
    across=lax.rem(r+2,4)
    one,two,act=(part[...] for part in parts)
    ours=jnp.concatenate([jnp.where(c==0,one,two),jnp.where(c==0,two,one)],axis=0).astype(low)
    note[:,:6*D]=ours
    note[:,6*D:]=act
    notes_in[s*4+r]=jnp.concatenate([ours,act],axis=1)
    barrier=pltpu.get_barrier_semaphore()
    others=[(a,b) for a in range(4) for b in range(4) if a or b]
    def note_copy(index,a,b):
        return pltpu.make_async_remote_copy(src_ref=note,dst_ref=notes_in.at[s*4+r],send_sem=note_send.at[index],recv_sem=note_recv.at[index],
            device_id={"shard":s^a,"rep":r^b},device_id_type=MESH)
    for a,b in others:
        pl.semaphore_signal(barrier,inc=1,device_id={"shard":s^a,"rep":r^b},device_id_type=MESH)
    for a in range(4):
        pl.semaphore_signal(barrier,inc=1,device_id={"section":1-c,"shard":s^a},device_id_type=MESH)
    sources=[block_sources(*half) for half in ins]
    span=left.shape[3]//2
    def load(index,slot):
        for here in range(blocks):
            @pl.when(index==here)
            def _():
                for half in range(2):
                    a,b=sources[half][here]
                    place=pl.ds(half*span,span)
                    pltpu.make_async_copy(a,left.at[slot,:,:,place],left_sem.at[slot]).start()
                    pltpu.make_async_copy(b,right.at[slot,place],right_sem.at[slot]).start()
    load(0,0)
    pltpu.make_async_copy(ada,ada_in,ada_sem).start()
    pl.semaphore_wait(barrier,len(others)+4)
    for index,(a,b) in enumerate(others): note_copy(index,a,b).start()
    def act_copy(index,a,other):
        section=1-c if other else c
        return pltpu.make_async_remote_copy(src_ref=blocks_out.at[s^a],dst_ref=blocks_in.at[c,s],send_sem=act_send.at[index],
            recv_sem=act_recv.at[index],device_id={"section":section,"shard":s^a},device_id_type=MESH)
    act_peers=[(a,other) for a in range(4) for other in (False,True) if a or other]
    def share_notes():
        for index,(a,b) in enumerate(others): note_copy(index,a,b).wait()
        pltpu.make_async_copy(ada,ada_in,ada_sem).wait()
        wide=lambda index: notes_in[index].astype(jnp.float32)
        notes_out=jnp.concatenate([wide(index) for index in range(16)],axis=0).astype(low)
        notes[...]=notes_out
        mine=jnp.concatenate([wide(shard*4+r)[:,:6*D] for shard in range(4)],axis=0).astype(low)
        grads=lax.dot_general(mine,ada_in[...],(((1,),(1,)),((),())),preferred_element_type=jnp.float32)
        span=grads.shape[0]//4
        for shard in range(4): blocks_out[shard]=grads[shard*span:(shard+1)*span]
        blocks_in[c,s]=blocks_out[s]
        for index,(a,other) in enumerate(act_peers): act_copy(index,a,other).start()
    units=3*blocks
    ends=[sum(LAGS[:k+1]) for k in range(4)]
    last=ends[3]

    def pick(ref,slot,names,name,value):
        place=names.index(name)
        return ref.at[(slot,)+(slice(None),)*place+(value,)]
    def exchange(stage,kind,u):
        order=KINDS[kind]; name=order[stage]
        names=[n for n in NAMES if n not in order[:stage]]
        buffers=part if stage==0 else kept[stage-1][order is SHARD_FIRST]
        depth=buffers.shape[0]
        src=pick(buffers,lax.rem(u,depth),names,name,1-bit[name])
        target=came[stage][order is SHARD_FIRST]
        ring=lax.rem(u,target.shape[0])
        return pltpu.make_async_remote_copy(src_ref=src,dst_ref=target.at[ring],
            send_sem=send_sem[stage].at[ring],recv_sem=recv_sem[stage].at[ring],
            device_id=peer[name],device_id_type=MESH)
    def receive(stage,kind,u):
        order=KINDS[kind]; name=order[stage]
        names=[n for n in NAMES if n not in order[:stage]]
        exchange(stage,kind,u).wait()
        buffers=part if stage==0 else kept[stage-1][order is SHARD_FIRST]
        own=pick(buffers,lax.rem(u,buffers.shape[0]),names,name,bit[name])
        target=came[stage][order is SHARD_FIRST]
        other=target.at[lax.rem(u,target.shape[0])]
        left_over=len(names)-1
        if stage<3:
            result=kept[stage][order is SHARD_FIRST]
            slot=lax.rem(u,result.shape[0])
        for flat in range(1<<left_over):
            where=tuple((flat>>k)&1 for k in reversed(range(left_over)))
            total=own[where].astype(jnp.float32)+other[where].astype(jnp.float32)
            if stage<3: result[(slot,)+where]=total.astype(low)
            else: final[lax.rem(u,final.shape[0])]=total.astype(low)
        if stage<3: exchange(stage+1,kind,u).start()
    grad_qkv,grad_wout,grad_fc1,grad_fc2=outs
    anywhere=grad_fc2.at[0,0,:,:WIDTH]
    def placed(u,kind,action):
        block=u//3
        def columns(first): return pl.ds(pl.multiple_of((block-first)*D+kind*WIDTH,128),WIDTH)
        here=slice(kind*WIDTH,(kind+1)*WIDTH)
        pl.when(block<4)(lambda: action(lambda who: grad_fc2.at[block,who,:,here]))
        pl.when((block>=4)&(block<8))(lambda: action(lambda who: grad_fc1.at[who,:,columns(4)]))
        pl.when(block==8)(lambda: action(lambda who: grad_wout.at[who,:,here]))
        pl.when(block>=9)(lambda: action(lambda who: grad_qkv.at[who,:,columns(9)]))
    def spread(u,target):
        src=final.at[lax.rem(u,final.shape[0])]
        return (pltpu.make_async_copy(src,target,final_sem.at[u]),
            pltpu.make_async_remote_copy(src_ref=src,dst_ref=target,send_sem=far_send.at[u],recv_sem=far_recv.at[u],
                device_id=peer["r1"],device_id_type=MESH),
            pltpu.make_async_remote_copy(src_ref=src,dst_ref=target,send_sem=near_send.at[u],recv_sem=near_recv.at[u],
                device_id=peer["r0"],device_id_type=MESH))
    def relay(u,piece):
        return pltpu.make_async_remote_copy(src_ref=piece,dst_ref=piece,send_sem=fwd_send.at[u],recv_sem=fwd_recv.at[u],
                device_id=peer["r0"],device_id_type=MESH)
    def compute(kind,block,u):
        slot=lax.rem(block,2)
        columns=right[slot,:,kind*WIDTH:(kind+1)*WIDTH]
        rows=left.shape[2]//4
        for shard in range(4):
            product=lax.dot_general(left[slot,shard],columns,(((1,),(0,)),((),())),preferred_element_type=jnp.float32)
            for rep in range(4):
                part[lax.rem(u,part.shape[0]),shard//2,shard%2,rep//2,rep%2]=product[rep*rows:(rep+1)*rows].astype(low)
        exchange(0,kind,u).start()

    total_steps=units+last+4
    iterations=-(-total_steps//3)
    def iteration(it,carry):
        @pl.when(it<blocks)
        def _():
            slot=lax.rem(it,2)
            pltpu.make_async_copy(left.at[slot],left.at[slot],left_sem.at[slot]).wait()
            pltpu.make_async_copy(right.at[slot],right.at[slot],right_sem.at[slot]).wait()
        for sub in range(3):
            step=3*it+sub
            def at(lag,action):
                kind=(sub-lag)%3
                unit=step-lag
                @pl.when((unit>=0)&(unit<units))
                def _(): action(kind,unit)
            def finish(kind,u):
                local,far,near=spread(u,anywhere)
                local.wait(); far.wait_send(); near.wait(); relay(u,anywhere).wait()
            at(last+3,finish)
            def pass_on(kind,u):
                spread(u,anywhere)[1].wait_recv()
                placed(u,kind,lambda where: relay(u,where(across)).start())
            at(last+2,pass_on)
            def finalize(kind,u):
                receive(3,kind,u)
                def start(where):
                    for copy in spread(u,where(r)): copy.start()
                placed(u,kind,start)
            at(ends[3],finalize)
            for stage in (2,1,0):
                at(ends[stage],functools.partial(receive,stage))
            if sub==0:
                load(it+1,lax.rem(it+1,2))
                pl.when(it==3)(share_notes)
            at(0,lambda kind,u: compute(kind,it,u))
        return carry
    lax.fori_loop(0,iterations,iteration,0)
    for index,(a,other) in enumerate(act_peers): act_copy(index,a,other).wait()
    act_out[...]=blocks_in[0]+blocks_in[1]

def unpack(refs):
    refs=list(refs)
    left,right,left_sem,right_sem,part=refs[:5]; refs=refs[5:]
    came=[(refs[0],refs[0]),(refs[1],refs[2]),(refs[3],refs[4]),(refs[5],refs[5])]; refs=refs[6:]
    send=refs[:4]; recv=refs[4:8]; refs=refs[8:]
    kept=[(refs[0],refs[0]),(refs[1],refs[2]),(refs[3],refs[4])]; refs=refs[5:]
    return (left,right,left_sem,right_sem,part,came,send,recv,kept,*refs)

def reduce_all(halves,grad_mods,act,ada):
    shards=lax.axis_size("shard"); reps=lax.axis_size("rep")
    rows=D//(shards*reps); group=D//shards
    blocks=12; units=3*blocks
    operands=[]
    for pairs in halves:
        (hidden,feed),(second,pre),(att,branch),(first,project)=pairs
        span=hidden.shape[0]
        operands+=[a.T.reshape(shards,group,span) for a in (first,second,att)]
        operands+=[hidden.T.reshape(shards,4,group,span),feed,pre,branch,project]
    tokens=2*span
    any_=pl.BlockSpec(memory_space=pl.ANY)
    piece=(rows,WIDTH)
    two=lambda count: (2,)*count+piece
    rings=[2*lag+1 for lag in LAGS]
    vm=lambda depth,shape: pltpu.VMEM((depth,)+shape,low)
    dma=pltpu.SemaphoreType.DMA
    keep=[lag+1 for lag in LAGS]
    inside=pl.BlockSpec(memory_space=pltpu.VMEM)
    batch=act.shape[0]; wide=7*D
    made=lambda shape,dtype: jax.ShapeDtypeStruct(shape,dtype)
    *grads,notes,act_grad=pl.pallas_call(functools.partial(reduce_kernel,blocks),
        in_specs=[any_]*16+[inside]*3+[any_],out_specs=[any_]*4+[inside,inside],
        out_shape=[made((reps,rows,3*D),low),made((reps,rows,D),low),made((reps,rows,4*D),low),made((4,reps,rows,D),low),
            made((shards*reps*batch,wide),low),made((shards,batch,group),jnp.float32)],
        scratch_shapes=[
            pltpu.VMEM((2,shards,group,tokens),low),pltpu.VMEM((2,tokens,D),low),dma((2,)),dma((2,)),
            vm(keep[0],two(4)),
            vm(rings[0],two(3)),vm(rings[1],two(2)),vm(rings[1],two(2)),vm(rings[2],two(1)),vm(rings[2],two(1)),vm(rings[3],two(0)),
            *[dma((ring,)) for ring in rings],*[dma((ring,)) for ring in rings],
            vm(keep[1],two(3)),vm(keep[2],two(2)),vm(keep[2],two(2)),vm(keep[3],two(1)),vm(keep[3],two(1)),
            vm(5,piece),
            *[dma((units,)) for _ in range(7)],dma((15,)),dma((15,)),
            pltpu.VMEM((shards*reps,batch,wide),low),pltpu.VMEM(ada.shape,low),dma(()),dma(()),
            pltpu.VMEM((shards,batch,group),jnp.float32),pltpu.VMEM((2,shards,batch,group),jnp.float32),dma((7,)),dma((7,)),pltpu.VMEM((batch,wide),low)],
        compiler_params=pltpu.CompilerParams(collective_id=2,has_side_effects=True),
        cost_estimate=pl.CostEstimate(flops=2*tokens*D*D*blocks,bytes_accessed=4*tokens*D*blocks,transcendentals=0),
        )(*operands,*grad_mods,act,ada)
    grads=[grad.reshape(-1,grad.shape[-1]).astype(jnp.float32) for grad in grads]
    return grads,notes,act_grad


def body(
    latents,
    cond,
    modulation_weight,
    query_key_value_weight,
    attention_output_weight,
    feed_first_weight,
    feed_second_weight,
    cotangent,
):
    first_section = lax.axis_index("section") == 0
    shard = lax.axis_index("shard")
    rep = lax.axis_index("rep")
    shards = lax.axis_size("shard")
    reps = lax.axis_size("rep")
    batch = latents.shape[0]
    modulation_weight = modulation_weight[0]
    rows = modulation_weight.shape[0]

    cond_float = cond.astype(jnp.float32)
    act = jax.nn.silu(cond_float).astype(low)
    blocks = act.reshape(batch, shards, rows).transpose(1, 0, 2)
    weights, total = gather_all(
        (
            query_key_value_weight[0],
            attention_output_weight[0],
            feed_first_weight[0],
            feed_second_weight[0],
        ),
        blocks,
        modulation_weight,
    )

    forth = [(0, 1)]
    back = [(1, 0)]
    swapped = jnp.where(first_section, total[1:], total[:1])
    straight = jnp.where(first_section, total[:1], total[1:])
    *_, sent = forward_layer(latents[0], total[:1], weights)
    incoming = lax.ppermute(sent, "section", forth)
    input_one = jnp.where(first_section, latents[1], incoming)
    *kept_one, result_one, sent = forward_layer(input_one, swapped, weights)
    incoming = lax.ppermute(sent, "section", forth)
    *_, sent = backward_layer(cotangent[0], swapped, input_one, kept_one, weights)
    returning = lax.ppermute(sent, "section", back)
    incoming, sent = lax.optimization_barrier((incoming, sent))
    input_two = jnp.where(first_section, latents[0], incoming)
    *kept_two, result_two, _ = forward_layer(input_two, straight, weights)
    grad_result = jnp.where(first_section, returning, cotangent[1])
    mod_one, *grads_one, grad_in_one, sent = backward_layer(
        grad_result, straight, input_two, kept_two, weights
    )
    returning = lax.ppermute(sent, "section", back)
    grad_result = jnp.where(first_section, returning, cotangent[0])
    mod_two, *grads_two, grad_in_two, _ = backward_layer(
        grad_result, swapped, input_one, kept_one, weights
    )

    def products(kept, grads):
        first_in, _, attended, _, _, second_in, _, hidden, _ = kept
        grad_feed, grad_pre, grad_branch, grad_project = grads
        return (
            (hidden, grad_feed),
            (second_in, grad_pre),
            (attended, grad_branch),
            (first_in, grad_project),
        )

    kept_one, kept_two, _ = lax.optimization_barrier((kept_one, kept_two, sent))
    pairs_one, pairs_two = products(kept_two, grads_one), products(kept_one, grads_two)
    wide = mod_one.shape[1]
    if shards == 4 and reps == 4:
        (grad_qkv, grad_wout, grad_fc1, grad_fc2), packed, act_grad = reduce_all(
            (pairs_one, pairs_two), (mod_one, mod_two), act, modulation_weight
        )
        act_total = act_grad.transpose(1, 0, 2).reshape(batch, shards * rows)
    else:
        pairs = [
            [jnp.concatenate(halves, axis=0) for halves in zip(one, two)]
            for one, two in zip(pairs_one, pairs_two)
        ]
        grad_fc2 = reduce_rows(*pairs[0], True)
        grad_fc1 = reduce_rows(*pairs[1], False)
        grad_wout = reduce_rows(*pairs[2], True)
        grad_qkv = reduce_rows(*pairs[3], True)
        grad_mod = jnp.where(
            first_section,
            jnp.concatenate([mod_one, mod_two], axis=0),
            jnp.concatenate([mod_two, mod_one], axis=0),
        ).astype(low)
        packed = jnp.concatenate([grad_mod, act], axis=-1)
        packed = lax.all_gather(packed, ("shard", "rep"), axis=0, tiled=True)
        own_mod = lax.dynamic_index_in_dim(
            packed[:, : wide].reshape(shards, reps, batch, -1), rep, 1, keepdims=False
        ).reshape(shards * batch, -1)
        act_grad = matmul_t(own_mod, modulation_weight)
        act_grad = act_grad + lax.ppermute(act_grad, "section", [(0, 1), (1, 0)])
        came = exchange_shards(act_grad.reshape(shards, batch, rows))
        act_total = jnp.zeros((shards, batch, rows), jnp.float32)
        for step, block in enumerate(came):
            act_total = lax.dynamic_update_index_in_dim(
                act_total, block, (shard - step) % shards, 0
            )
        act_total = act_total.transpose(1, 0, 2).reshape(batch, shards * rows)

    boundary = jnp.stack(
        [
            jnp.where(first_section, grad_in_one, result_one),
            jnp.where(first_section, grad_in_two, result_two),
        ]
    )[None]

    all_mod = packed[:, : wide]
    all_act = packed[:, wide :]
    act_rows = lax.dynamic_slice_in_dim(all_act, shard * rows, rows, 1)
    grad_ada = lax.dot_general(
        act_rows, all_mod, (((0,), (0,)), ((), ())), preferred_element_type=jnp.float32
    )
    _, silu_back = jax.vjp(jax.nn.silu, cond_float)
    grad_cond = silu_back(act_total)[0]
    return (
        boundary,
        grad_cond,
        grad_ada[None],
        grad_qkv[None],
        grad_wout[None],
        grad_fc1[None],
        grad_fc2[None],
    )


def solution(mesh):
    in_specs = (
        P(("shard", "rep"), None, None),
        P(("shard", "rep"), None),
        P("section", "shard", None),
        P("section", "shard", None),
        P("section", "shard", None),
        P("section", "shard", None),
        P("section", "shard", None),
        P(("shard", "rep"), None, None),
    )
    out_specs = (
        P("section", ("shard", "rep"), None, None),
        P(("shard", "rep"), None),
        P("section", "shard", None),
        P("section", "shard", None),
        P("section", "shard", None),
        P("section", "shard", None),
        P("section", "shard", None),
    )

    return jax.shard_map(body, mesh=mesh, in_specs=in_specs, out_specs=out_specs, check_vma=False)
```

```python
import functools

import jax
import jax.numpy as jnp
from jax import lax
from jax.experimental import pallas as pl
from jax.experimental.pallas import tpu as pltpu
from jax.sharding import PartitionSpec as P


D = 1152
HEADS = 16
HEAD_DIM = 72
LANES = 128


low = jnp.bfloat16


NT=(((1,),(1,)),((),())); TN=(((0,),(0,)),((),()))
def dot(a,b,dims=(((1,),(0,)),((),()))):
    return lax.dot_general(a,b,dims,preferred_element_type=jnp.float32)
def windows():
    for head in range(HEADS):
        start=head*HEAD_DIM; stop=start+HEAD_DIM
        first=start//LANES*LANES; last=-(-stop//LANES)*LANES
        yield first,last,start-first,stop-first
def head_mask(rows,first,last,begin,end):
    lane=lax.broadcasted_iota(jnp.int32,(rows,last-first),1)
    return (lane>=begin)&(lane<end)
def attention_kernel(project_ref,out_ref):
    rows=out_ref.shape[0]
    for first,last,begin,end in windows():
        mask=head_mask(rows,first,last,begin,end)
        q=project_ref[:,first:last]; k=project_ref[:,D+first:D+last]; v=project_ref[:,2*D+first:2*D+last]
        q=jnp.where(mask,q,jnp.zeros_like(q))
        s=dot(q,k,NT)*(HEAD_DIM**-0.5)
        e=jnp.exp(s-jnp.max(s,axis=1,keepdims=True))
        p=(e/jnp.sum(e,axis=1,keepdims=True)).astype(low)
        o=dot(p,v).astype(low)
        out_ref[:,first:last]=jnp.where(mask,o,out_ref[:,first:last])
def attention_back_kernel(project_ref,grad_ref,out_ref):
    rows=grad_ref.shape[0]; factor=HEAD_DIM**-0.5
    for first,last,begin,end in windows():
        mask=head_mask(rows,first,last,begin,end)
        q=project_ref[:,first:last]; k=project_ref[:,D+first:D+last]; v=project_ref[:,2*D+first:2*D+last]
        g=grad_ref[:,first:last]
        s=dot(jnp.where(mask,k,jnp.zeros_like(k)),q,NT)*factor
        e=jnp.exp(s-jnp.max(s,axis=0,keepdims=True))
        p=e/jnp.sum(e,axis=0,keepdims=True)
        dp=dot(jnp.where(mask,v,jnp.zeros_like(v)),g,NT)
        ds=(p*(dp-jnp.sum(dp*p,axis=0,keepdims=True))).astype(low)
        dq=(dot(ds,k,TN)*factor).astype(low)
        dk=(dot(ds,q)*factor).astype(low)
        dv=dot(p.astype(low),g).astype(low)
        for base,piece in ((0,dq),(D,dk),(2*D,dv)):
            here=slice(base+first,base+last)
            out_ref[:,here]=jnp.where(mask,piece,out_ref[:,here])
C0=0.7978845608028654; C1=0.044715
epsilon=1e-06
FEED_GROUPS=3
FEED_CHUNK=512

def act_of(u): return (0.5*u*(1.0+jnp.tanh(C0*(u+C1*(u*u*u))))).astype(low)
def slope_of(u):
    sq=u*u
    t=jnp.tanh(C0*(u+C1*(sq*u)))
    return 0.5*(1.0+t)+0.5*u*(1.0-t*t)*(C0*(1.0+3.0*C1*sq))
def center_scale(values):
    center=values-jnp.mean(values,axis=-1,keepdims=True)
    scale=lax.rsqrt(jnp.mean(center*center,axis=-1,keepdims=True)+epsilon)
    return center*scale,scale
def norm_back(normed,scale,grad):
    mean_grad=jnp.mean(grad,axis=-1,keepdims=True)
    mean_dot=jnp.mean(grad*normed,axis=-1,keepdims=True)
    return (grad-mean_grad-normed*mean_dot)*scale
def chunks_of(span): return [slice(a,a+FEED_CHUNK) for a in range(0,span,FEED_CHUNK)]

def by_section(zero,one):
    return jnp.where(lax.axis_index("section")==0,zero,one)

class Copies:
    def __init__(self,sems): self.sems=sems; self.made=[]
    def start(self,src,dst):
        copy=pltpu.make_async_copy(src,dst,self.sems.at[len(self.made)])
        copy.start(); self.made.append(copy)
        return copy
    def wait_all(self):
        for copy in self.made: copy.wait()

def forward_kernel(rows,places,x_zero,x_one,mod_ref,wqkv,wout,w1,w2,
        first_out,project_out,att_out,branch_out,middle_out,second_out,u_out,h_out,f_out,y_out,y_low_out,
        wqkv_v,wout_v,w1_v,w2_v,first_v,project_v,att_v,branch_v,middle_v,second_v,u_v,h_v,f_v,y_v,y_low_v,in_sems,out_sems):
    width=wqkv_v.shape[2]; group=w1_v.shape[2]
    x_zero,x_one=at_latent((x_zero,x_one),places)
    come=Copies(in_sems); leave=Copies(out_sems)
    third=lambda i: pl.ds(pl.multiple_of(i*width,128),width)
    part_of=lambda i: pl.ds(pl.multiple_of(i*group,128),group)
    def project_copy(i): return pltpu.make_async_copy(wqkv.at[:,third(i)],wqkv_v.at[i],in_sems.at[1+i])
    def feed_copies(i):
        return (pltpu.make_async_copy(w1.at[:,part_of(i)],w1_v.at[i],in_sems.at[4+2*i]),
            pltpu.make_async_copy(w2.at[part_of(i)],w2_v.at[i],in_sems.at[5+2*i]))
    def feed_leave(i):
        return (pltpu.make_async_copy(u_v.at[i],u_out.at[:,part_of(i)],out_sems.at[9+2*i]),
            pltpu.make_async_copy(h_v.at[i],h_out.at[:,part_of(i)],out_sems.at[10+2*i]))
    for i in range(3): project_copy(i).start()
    out_in=come.start(wout,wout_v)
    for i in range(FEED_GROUPS):
        for copy in feed_copies(i): copy.start()
    shift_one,scale_one,gate_one,shift_two,scale_two,gate_two=(
        by_section(mod_ref[rows[0]:rows[0]+1,i*D:(i+1)*D],mod_ref[rows[1]:rows[1]+1,i*D:(i+1)*D]) for i in range(6))
    x=by_section(x_zero[...],x_one[...]).astype(jnp.float32)
    first_v[...]=(center_scale(x)[0]*(1.0+scale_one)+shift_one).astype(low)
    leave.start(first_v,first_out)
    def project_part(i,carry):
        project_copy(i).wait()
        project_v[:,third(i)]=dot(first_v[...],wqkv_v[i]).astype(low)
        return carry
    lax.fori_loop(0,3,project_part,0)
    leave.start(project_v,project_out)
    attention_kernel(project_v,att_v)
    leave.start(att_v,att_out)
    out_in.wait()
    branch=dot(att_v[...],wout_v[...])
    branch_v[...]=branch
    leave.start(branch_v,branch_out)
    middle=by_section(x_zero[...],x_one[...]).astype(jnp.float32)+gate_one*branch
    middle_v[...]=middle
    leave.start(middle_v,middle_out)
    second_v[...]=(center_scale(middle)[0]*(1.0+scale_two)+shift_two).astype(low)
    leave.start(second_v,second_out)
    f_v[...]=jnp.zeros_like(f_v)
    def feed_part(i,carry):
        for copy in feed_copies(i): copy.wait()
        prev=None
        def back(p,u):
            h=act_of(u); h_v[i,:,p]=h
            f_v[...]+=dot(h,w2_v[i,p,:])
        for p in chunks_of(group):
            u=dot(second_v[...],w1_v[i,:,p]); u_v[i,:,p]=u
            if prev is not None: back(*prev)
            prev=(p,u)
        back(*prev)
        for copy in feed_leave(i): copy.start()
        return carry
    lax.fori_loop(0,FEED_GROUPS,feed_part,0)
    y=middle_v[...]+gate_two*f_v[...]
    y_v[...]=y
    y_low_v[...]=y.astype(low)
    leave.start(y_low_v,y_low_out)
    leave.start(f_v,f_out)
    leave.start(y_v,y_out)
    leave.wait_all()
    for i in range(FEED_GROUPS):
        for copy in feed_leave(i): copy.wait()

def backward_kernel(rows,places,g_zero,g_one,mod_ref,x_zero,x_one,feed_out,middle,branch,u,project,wqkv,wout,w1,w2,
        mod_out,df_out,du_out,do_out,dproject_out,dx_out,dx_low_out,
        feed_v,middle_v,branch_v,u_v,project_v,wqkv_v,wout_v,w1_v,w2_v,df_v,du_v,do_v,datt_v,dproject_v,acc_v,dx_v,dx_low_v,in_sems,out_sems):
    g_zero,g_one,x_zero,x_one=at_latent((g_zero,g_one,x_zero,x_one),places)
    group=w1_v.shape[2]
    come=Copies(in_sems); leave=Copies(out_sems)
    part_of=lambda i: pl.ds(pl.multiple_of(i*group,128),group)
    def feed_copies(i):
        return (pltpu.make_async_copy(w2.at[part_of(i)],w2_v.at[i],in_sems.at[6+3*i]),
            pltpu.make_async_copy(u.at[:,part_of(i)],u_v.at[i],in_sems.at[7+3*i]),
            pltpu.make_async_copy(w1.at[:,part_of(i)],w1_v.at[i],in_sems.at[8+3*i]))
    def feed_leave(i): return pltpu.make_async_copy(du_v.at[i],du_out.at[:,part_of(i)],out_sems.at[5+i])
    for i in range(FEED_GROUPS):
        for copy in feed_copies(i): copy.start()
        if i==0: feed_copy=come.start(feed_out,feed_v)
    middle_in=come.start(middle,middle_v); branch_in=come.start(branch,branch_v)
    out_in=come.start(wout,wout_v); project_in=come.start(project,project_v); qkv_in=come.start(wqkv,wqkv_v)
    _,scale_one,gate_one,_,scale_two,gate_two=(
        by_section(mod_ref[rows[0]:rows[0]+1,i*D:(i+1)*D],mod_ref[rows[1]:rows[1]+1,i*D:(i+1)*D]) for i in range(6))
    total=lambda values: jnp.sum(values,axis=0,keepdims=True)
    df_v[...]=(gate_two*by_section(g_zero[...],g_one[...]).astype(jnp.float32)).astype(low)
    leave.start(df_v,df_out)
    acc_v[...]=jnp.zeros_like(acc_v)
    def feed_part(i,carry):
        for copy in feed_copies(i): copy.wait()
        prev=None
        def back(p,dh):
            du=(dh*slope_of(u_v[i,:,p])).astype(low); du_v[i,:,p]=du
            acc_v[...]+=dot(du,w1_v[i,:,p],NT)
        for p in chunks_of(group):
            dh=dot(df_v[...],w2_v[i,p,:],NT)
            if prev is not None: back(*prev)
            prev=(p,dh)
        back(*prev)
        feed_leave(i).start()
        return carry
    lax.fori_loop(0,FEED_GROUPS,feed_part,0)
    feed_copy.wait(); middle_in.wait(); branch_in.wait()
    g=by_section(g_zero[...],g_one[...]).astype(jnp.float32)
    mod_out[:,5*D:6*D]=total(g*feed_v[...])
    dh=acc_v[...]
    normed,inverse=center_scale(middle_v[...])
    mod_out[:,3*D:4*D]=total(dh)
    mod_out[:,4*D:5*D]=total(dh*normed)
    dmiddle=g+norm_back(normed,inverse,dh*(1.0+scale_two))
    dx_v[...]=dmiddle
    mod_out[:,2*D:3*D]=total(dmiddle*branch_v[...])
    do_v[...]=(gate_one*dmiddle).astype(low)
    leave.start(do_v,do_out)
    out_in.wait()
    datt_v[...]=dot(do_v[...],wout_v[...],NT).astype(low)
    project_in.wait()
    attention_back_kernel(project_v,datt_v,dproject_v)
    leave.start(dproject_v,dproject_out)
    qkv_in.wait()
    dh=dot(dproject_v[...],wqkv_v[...],NT)
    normed,inverse=center_scale(by_section(x_zero[...],x_one[...]).astype(jnp.float32))
    mod_out[:,0*D:1*D]=total(dh)
    mod_out[:,1*D:2*D]=total(dh*normed)
    dx=dx_v[...]+norm_back(normed,inverse,dh*(1.0+scale_one))
    dx_v[...]=dx
    dx_low_v[...]=dx.astype(low)
    leave.start(dx_low_v,dx_low_out)
    leave.start(dx_v,dx_out)
    leave.wait_all()
    for i in range(FEED_GROUPS): feed_leave(i).wait()

LAYER_VMEM=60 * 1024 * 1024
def one_latent(source):
    return source if isinstance(source,tuple) else (source,None)
def at_latent(refs,places):
    return [ref if place is None else ref.at[place] for ref,place in zip(refs,places)]
def forward_layer(inputs,mod,rows,weights):
    _,_,w1,_=weights
    operands,places=zip(*(one_latent(source) for source in inputs))
    t,d=operands[0].shape[-2:]; ff=w1.shape[1]; group=ff//FEED_GROUPS
    made=lambda width,dtype: jax.ShapeDtypeStruct((t,width),dtype)
    f32=jnp.float32
    v=pltpu.VMEM
    any_=pl.BlockSpec(memory_space=pl.ANY); inside=pl.BlockSpec(memory_space=pltpu.VMEM)
    return pl.pallas_call(functools.partial(forward_kernel,rows,places),in_specs=[inside]*3+[any_]*4,out_specs=[any_]*11,
        out_shape=[made(d,low),made(3*d,low),made(d,low),made(d,f32),made(d,f32),made(d,low),made(ff,f32),made(ff,low),made(d,f32),made(d,f32),made(d,low)],
        scratch_shapes=[v((3,d,d),low),v((d,d),low),v((FEED_GROUPS,d,group),low),v((FEED_GROUPS,group,d),low),
            v((t,d),low),v((t,3*d),low),v((t,d),low),v((t,d),f32),v((t,d),f32),v((t,d),low),
            v((FEED_GROUPS,t,group),f32),v((FEED_GROUPS,t,group),low),v((t,d),f32),v((t,d),f32),v((t,d),low),
            pltpu.SemaphoreType.DMA((4+2*FEED_GROUPS,)),pltpu.SemaphoreType.DMA((9+2*FEED_GROUPS,))],
        compiler_params=pltpu.CompilerParams(vmem_limit_bytes=LAYER_VMEM),
        cost_estimate=pl.CostEstimate(flops=2*t*d*(4*d+2*ff)+4*t*t*d,bytes_accessed=2*d*(4*d+2*ff)+t*(30*d+6*ff),transcendentals=t*(ff+HEADS*t)),
        )(*operands,mod,*weights)
def backward_layer(grads,mod,rows,inputs,kept,weights):
    _,project,_,branch,middle,_,u,_,feed_out=kept
    _,_,w1,_=weights
    operands,places=zip(*(one_latent(source) for source in (*grads,*inputs)))
    t,d=operands[2].shape[-2:]; ff=w1.shape[1]; group=ff//FEED_GROUPS
    made=lambda width,dtype: jax.ShapeDtypeStruct((t,width),dtype)
    f32=jnp.float32
    v=pltpu.VMEM
    any_=pl.BlockSpec(memory_space=pl.ANY); inside=pl.BlockSpec(memory_space=pltpu.VMEM)
    return pl.pallas_call(functools.partial(backward_kernel,rows,places),in_specs=[inside]*5+[any_]*9,out_specs=[inside]+[any_]*6,
        out_shape=[jax.ShapeDtypeStruct((1,6*d),f32),made(d,low),made(ff,low),made(d,low),made(3*d,low),made(d,f32),made(d,low)],
        scratch_shapes=[v((t,d),f32),v((t,d),f32),v((t,d),f32),v((FEED_GROUPS,t,group),f32),v((t,3*d),low),
            v((d,3*d),low),v((d,d),low),v((FEED_GROUPS,d,group),low),v((FEED_GROUPS,group,d),low),
            v((t,d),low),v((FEED_GROUPS,t,group),low),v((t,d),low),v((t,d),low),v((t,3*d),low),v((t,d),f32),v((t,d),f32),v((t,d),low),
            pltpu.SemaphoreType.DMA((6+3*FEED_GROUPS,)),pltpu.SemaphoreType.DMA((5+FEED_GROUPS,))],
        compiler_params=pltpu.CompilerParams(vmem_limit_bytes=LAYER_VMEM),
        cost_estimate=pl.CostEstimate(flops=2*t*d*(4*d+2*ff)+10*t*t*d,bytes_accessed=2*d*(4*d+2*ff)+t*(30*d+6*ff),transcendentals=t*(ff+HEADS*t)),
        )(*operands[:2],mod,*operands[2:],feed_out,middle,branch,u,project,*weights)


def matmul(left, right):
    return jnp.dot(left, right, preferred_element_type=jnp.float32)


def matmul_t(left, right):
    return lax.dot_general(
        left, right, (((1,), (1,)), ((), ())), preferred_element_type=jnp.float32
    )


def bits_of(count):
    bits = count.bit_length() - 1
    assert 1 << bits == count
    return bits


def swap(value, axis, bit):
    count = lax.axis_size(axis)
    return lax.ppermute(value, axis, [(i, i ^ (1 << bit)) for i in range(count)])


def reduce_rows(left, right, reps_first):
    shard_bits = bits_of(lax.axis_size("shard"))
    rep_bits = bits_of(lax.axis_size("rep"))
    shard_stages = [("shard", bit) for bit in range(shard_bits)]
    rep_stages = [("rep", bit) for bit in range(rep_bits)]
    if reps_first:
        stages = rep_stages + shard_stages
    else:
        stages = rep_stages[:1] + shard_stages + rep_stages[1:]
    names = [("shard", bit) for bit in reversed(range(shard_bits))]
    names += [("rep", bit) for bit in reversed(range(rep_bits))]
    tokens, depth = left.shape
    inner = depth >> len(names)
    part = None
    for axis, bit in stages:
        place = names.index((axis, bit))
        mine = (lax.axis_index(axis) >> bit) & 1
        if part is None:
            spread = left.T.reshape((2,) * len(names) + (inner, tokens))
            away = lax.dynamic_index_in_dim(spread, 1 - mine, place, keepdims=False)
            stay = lax.dynamic_index_in_dim(spread, mine, place, keepdims=False)
            away = matmul(away.reshape(-1, tokens), right).astype(low)
            came = swap(away, axis, bit)
            part = (matmul(stay.reshape(-1, tokens), right) + came.astype(jnp.float32)).astype(low)
            names.pop(place)
            part = part.reshape((2,) * len(names) + (inner, right.shape[1]))
        else:
            away = lax.dynamic_index_in_dim(part, 1 - mine, place, keepdims=False)
            stay = lax.dynamic_index_in_dim(part, mine, place, keepdims=False)
            came = swap(away, axis, bit)
            part = (stay.astype(jnp.float32) + came.astype(jnp.float32)).astype(low)
            names.pop(place)
    whole = lax.all_gather(part, "rep", axis=0, tiled=True)
    return whole.astype(jnp.float32)


def exchange_shards(blocks):
    count = lax.axis_size("shard")
    me = lax.axis_index("shard")
    came = [lax.dynamic_index_in_dim(blocks, me, 0, keepdims=False)]
    for step in range(1, count):
        block = lax.dynamic_index_in_dim(blocks, (me + step) % count, 0, keepdims=False)
        came.append(
            lax.ppermute(block, "shard", [(i, (i + step) % count) for i in range(count)])
        )
    return came


MESH=pl.DeviceIdType.MESH

def gather_kernel(shards,reps,arrays,chunks,*refs):
    ins=refs[:arrays]; act,ada=refs[arrays:arrays+2]; refs=refs[arrays+2:]
    outs=refs[:arrays]; mod_out=refs[arrays]; refs=refs[arrays+1:]; bounce=refs[:arrays]
    (line_send,line_recv,rep_send,rep_recv,local_in,local_out,
     ada_v,acts_in,mod_send,mod_in,ada_sem,act_sems,mod_sems)=refs[arrays:]
    count=len(chunks)
    def own_piece(c,rep):
        index,rows,columns=chunks[c]
        return ins[index].at[rep,rows,columns]
    def piece_of(c,owner,rep):
        index,rows,columns=chunks[c]
        return outs[index].at[owner,rep,rows,columns]
    s=lax.axis_index("shard"); r=lax.axis_index("rep")
    bits=reps.bit_length()-1
    barrier=pltpu.get_barrier_semaphore()
    for other in range(1,shards):
        pl.semaphore_signal(barrier,inc=1,device_id={"shard":s^other},device_id_type=MESH)
    for bit in range(bits):
        pl.semaphore_signal(barrier,inc=1,device_id={"rep":r^(1<<bit)},device_id_type=MESH)
    for c in range(arrays):
        pltpu.make_async_copy(ins[c],bounce[c],local_in.at[c]).start()
    pltpu.make_async_copy(ada,ada_v,ada_sem).start()
    acts_in[s]=act[s]
    pl.semaphore_wait(barrier,bits+shards-1)
    def act_copy(other):
        return pltpu.make_async_remote_copy(src_ref=act.at[s^other],dst_ref=acts_in.at[s],send_sem=act_sems.at[0,other-1],
            recv_sem=act_sems.at[1,other-1],device_id={"shard":s^other},device_id_type=MESH)
    def mod_copy(other):
        return pltpu.make_async_remote_copy(src_ref=mod_send.at[s^other],dst_ref=mod_in.at[s],send_sem=mod_sems.at[0,other-1],
            recv_sem=mod_sems.at[1,other-1],device_id={"shard":s^other},device_id_type=MESH)
    for other in range(1,shards): act_copy(other).start()
    sides=((0,1),(1,-1))

    def line(way,step,hop,c,owner):
        src=own_piece(c,r) if hop==0 else piece_of(c,owner,r)
        return pltpu.make_async_remote_copy(src_ref=src,dst_ref=piece_of(c,owner,r),
            send_sem=line_send.at[way,hop,c],recv_sem=line_recv.at[way,hop,c],
            device_id={"shard":s+step},device_id_type=MESH)
    def side_copy(bit,mask,c,owner):
        piece=piece_of(c,owner,r^mask)
        return pltpu.make_async_remote_copy(src_ref=piece,dst_ref=piece,
            send_sem=rep_send.at[bit,mask,owner,c],recv_sem=rep_recv.at[mask|(1<<bit),owner,c],
            device_id={"rep":r^(1<<bit)},device_id_type=MESH)
    def low_bit(mask): return bits if mask==0 else (mask&-mask).bit_length()-1
    def arrived(mask,c,owner):
        bit=low_bit(mask)
        piece=piece_of(c,owner,r^mask)
        pltpu.make_async_remote_copy(src_ref=piece,dst_ref=piece,send_sem=rep_send.at[bit,mask^(1<<bit),owner,c],
            recv_sem=rep_recv.at[mask,owner,c],device_id={"rep":r^(1<<bit)},device_id_type=MESH).wait_recv()
    for c in range(count):
        for way,step in sides:
            @pl.when((s+step>=0)&(s+step<shards))
            def _(): line(way,step,0,c,s).start()
    for c in range(arrays):
        pltpu.make_async_copy(ins[c],bounce[c],local_in.at[c]).wait()
        pltpu.make_async_copy(bounce[c],outs[c].at[s],local_out.at[c]).start()
    for other in range(1,shards): act_copy(other).wait()
    pltpu.make_async_copy(ada,ada_v,ada_sem).wait()
    acts=jnp.concatenate([acts_in[k].astype(jnp.float32) for k in range(shards)],axis=0).astype(low)
    partial=dot(acts,ada_v[...])
    batch=act.shape[1]
    for k in range(shards): mod_send[k]=partial[k*batch:(k+1)*batch]
    mod_in[s]=mod_send[s]
    for other in range(1,shards): mod_copy(other).start()
    events=[(hop,c) for hop in range(1,shards) for c in range(count)]
    relays=[m for m in range(1,reps) if low_bit(m)>0]
    depth=max([m.bit_count() for m in relays],default=0)
    for index in range(len(events)+depth):
        if index<len(events):
            hop,c=events[index]
            for way,step in sides:
                owner=s-step*hop
                @pl.when((owner>=0)&(owner<shards))
                def _():
                    line(way,step,hop-1,c,owner).wait_recv()
                    if hop+1<shards:
                        @pl.when((s+step>=0)&(s+step<shards))
                        def _(): line(way,step,hop,c,owner).start()
                    for bit in reversed(range(bits)):
                        side_copy(bit,0,c,owner).start()
        for mask in relays:
            late=index-mask.bit_count()
            if 0<=late<len(events):
                hop,c=events[late]
                for way,step in sides:
                    owner=s-step*hop
                    @pl.when((owner>=0)&(owner<shards))
                    def _():
                        arrived(mask,c,owner)
                        for bit in reversed(range(low_bit(mask))):
                            side_copy(bit,mask,c,owner).start()
    for hop,c in events:
        for way,step in sides:
            owner=s-step*hop
            @pl.when((owner>=0)&(owner<shards))
            def _():
                for mask in range(1,reps):
                    if low_bit(mask)==0: arrived(mask,c,owner)
                for mask in range(reps):
                    for bit in range(low_bit(mask)): side_copy(bit,mask,c,owner).wait_send()
                if hop+1<shards:
                    @pl.when((s+step>=0)&(s+step<shards))
                    def _(): line(way,step,hop,c,owner).wait_send()
    for c in range(count):
        for way,step in sides:
            @pl.when((s+step>=0)&(s+step<shards))
            def _(): line(way,step,0,c,s).wait_send()
    for c in range(arrays):
        pltpu.make_async_copy(bounce[c],outs[c].at[s],local_out.at[c]).wait()
    for other in range(1,shards): mod_copy(other).wait()
    total=mod_in[0]
    for k in range(1,shards): total=total+mod_in[k]
    mod_out[...]=total

def gather_all(weights,act,ada):
    shards=lax.axis_size("shard"); reps=lax.axis_size("rep"); bits=reps.bit_length()-1
    assert 1<<bits==reps
    arrays=len(weights)
    views=[w.reshape(reps,w.shape[0]//reps,w.shape[1]) for w in weights]
    def split(index,columns=None,rows=None):
        depth,width=views[index].shape[1:]
        return (index,slice(*(rows or (0,depth))),slice(*(columns or (0,width))))
    deep=views[3].shape[1]; halves=((0,deep//2),(deep//2,deep)) if deep%16==0 else ((0,deep),)
    chunks=[split(1),split(0,(D,3*D)),split(2,(0,2*D)),split(2,(2*D,4*D))]
    chunks+=[split(3,rows=half) for half in halves]+[split(0,(0,D))]
    count=len(chunks)
    any_=pl.BlockSpec(memory_space=pl.ANY)
    inside=pl.BlockSpec(memory_space=pltpu.VMEM)
    batch=act.shape[1]
    *outs,modulation=pl.pallas_call(functools.partial(gather_kernel,shards,reps,arrays,chunks),
        in_specs=[any_]*arrays+[inside,any_],out_specs=[any_]*arrays+[inside],
        out_shape=[jax.ShapeDtypeStruct((shards,)+v.shape,v.dtype) for v in views]+[jax.ShapeDtypeStruct((batch,ada.shape[1]),jnp.float32)],
        scratch_shapes=[pltpu.VMEM(v.shape,v.dtype) for v in views]+[
            pltpu.SemaphoreType.DMA((2,shards-1,count)),pltpu.SemaphoreType.DMA((2,shards-1,count)),
            pltpu.SemaphoreType.DMA((bits,reps,shards,count)),pltpu.SemaphoreType.DMA((reps,shards,count)),
            pltpu.SemaphoreType.DMA((arrays,)),pltpu.SemaphoreType.DMA((arrays,)),
            pltpu.VMEM(ada.shape,low),pltpu.VMEM(act.shape,low),pltpu.VMEM((shards,batch,ada.shape[1]),jnp.float32),
            pltpu.VMEM((shards,batch,ada.shape[1]),jnp.float32),pltpu.SemaphoreType.DMA(()),
            pltpu.SemaphoreType.DMA((2,shards-1)),pltpu.SemaphoreType.DMA((2,shards-1))],
        compiler_params=pltpu.CompilerParams(collective_id=1,has_side_effects=True),
        )(*views,act,ada)
    return tuple(o.reshape(shards*w.shape[0],w.shape[1]) for o,w in zip(outs,weights)),modulation


NAMES=("s1","s0","r1","r0")
REP_FIRST=("r0","r1","s0","s1")
SHARD_FIRST=("r0","s0","s1","r1")
KINDS=(REP_FIRST,SHARD_FIRST,REP_FIRST)
WIDTH=D//3
LAGS=(1,3,3,2)

def block_sources(first_t,second_t,att_t,hidden_t,feed,pre,branch,project):
    pairs=[(hidden_t.at[:,j],feed) for j in range(4)]
    pairs+=[(second_t,pre.at[:,j*D:(j+1)*D]) for j in range(4)]
    pairs+=[(att_t,branch)]
    pairs+=[(first_t,project.at[:,j*D:(j+1)*D]) for j in range(3)]
    return pairs

def reduce_kernel(blocks,*refs):
    ins=(refs[:8],refs[8:16]); parts,ada,outs,notes,act_out=refs[16:19],refs[19],refs[20:24],refs[24],refs[25]
    (left,right,left_sem,right_sem,part,came,send_sem,recv_sem,kept,final,
     final_sem,near_send,near_recv,far_send,far_recv,fwd_send,fwd_recv,note_send,note_recv,
     notes_in,ada_in,ada_sem,_,blocks_out,blocks_in,act_send,act_recv,note)=unpack(refs[26:])
    c=lax.axis_index("section")
    s=lax.axis_index("shard"); r=lax.axis_index("rep")
    bit={"s1":s//2,"s0":lax.rem(s,2),"r1":r//2,"r0":lax.rem(r,2)}
    peer={"s1":{"shard":lax.rem(s+2,4)},"s0":{"shard":s+1-2*lax.rem(s,2)},
          "r1":{"rep":lax.rem(r+2,4)},"r0":{"rep":r+1-2*lax.rem(r,2)}}
    across=lax.rem(r+2,4)
    one,two,act=(part[...] for part in parts)
    ours=jnp.concatenate([jnp.where(c==0,one,two),jnp.where(c==0,two,one)],axis=0).astype(low)
    note[:,:6*D]=ours
    note[:,6*D:]=act
    notes_in[s*4+r]=jnp.concatenate([ours,act],axis=1)
    barrier=pltpu.get_barrier_semaphore()
    others=[(a,b) for a in range(4) for b in range(4) if a or b]
    def note_copy(index,a,b):
        return pltpu.make_async_remote_copy(src_ref=note,dst_ref=notes_in.at[s*4+r],send_sem=note_send.at[index],recv_sem=note_recv.at[index],
            device_id={"shard":s^a,"rep":r^b},device_id_type=MESH)
    for a,b in others:
        pl.semaphore_signal(barrier,inc=1,device_id={"shard":s^a,"rep":r^b},device_id_type=MESH)
    for a in range(4):
        pl.semaphore_signal(barrier,inc=1,device_id={"section":1-c,"shard":s^a},device_id_type=MESH)
    sources=[block_sources(*half) for half in ins]
    span=left.shape[3]//2
    def load(index,slot):
        for here in range(blocks):
            @pl.when(index==here)
            def _():
                for half in range(2):
                    a,b=sources[half][here]
                    place=pl.ds(half*span,span)
                    pltpu.make_async_copy(a,left.at[slot,:,:,place],left_sem.at[slot]).start()
                    pltpu.make_async_copy(b,right.at[slot,place],right_sem.at[slot]).start()
    load(0,0)
    pltpu.make_async_copy(ada,ada_in,ada_sem).start()
    pl.semaphore_wait(barrier,len(others)+4)
    for index,(a,b) in enumerate(others): note_copy(index,a,b).start()
    def act_copy(index,a,other):
        section=1-c if other else c
        return pltpu.make_async_remote_copy(src_ref=blocks_out.at[s^a],dst_ref=blocks_in.at[c,s],send_sem=act_send.at[index],
            recv_sem=act_recv.at[index],device_id={"section":section,"shard":s^a},device_id_type=MESH)
    act_peers=[(a,other) for a in range(4) for other in (False,True) if a or other]
    def share_notes():
        for index,(a,b) in enumerate(others): note_copy(index,a,b).wait()
        pltpu.make_async_copy(ada,ada_in,ada_sem).wait()
        wide=lambda index: notes_in[index].astype(jnp.float32)
        notes_out=jnp.concatenate([wide(index) for index in range(16)],axis=0).astype(low)
        notes[...]=notes_out
        mine=jnp.concatenate([wide(shard*4+r)[:,:6*D] for shard in range(4)],axis=0).astype(low)
        grads=lax.dot_general(mine,ada_in[...],(((1,),(1,)),((),())),preferred_element_type=jnp.float32)
        span=grads.shape[0]//4
        for shard in range(4): blocks_out[shard]=grads[shard*span:(shard+1)*span]
        blocks_in[c,s]=blocks_out[s]
        for index,(a,other) in enumerate(act_peers): act_copy(index,a,other).start()
    units=3*blocks
    ends=[sum(LAGS[:k+1]) for k in range(4)]
    last=ends[3]

    def pick(ref,slot,names,name,value):
        place=names.index(name)
        return ref.at[(slot,)+(slice(None),)*place+(value,)]
    def exchange(stage,kind,u):
        order=KINDS[kind]; name=order[stage]
        names=[n for n in NAMES if n not in order[:stage]]
        buffers=part if stage==0 else kept[stage-1][order is SHARD_FIRST]
        depth=buffers.shape[0]
        src=pick(buffers,lax.rem(u,depth),names,name,1-bit[name])
        target=came[stage][order is SHARD_FIRST]
        ring=lax.rem(u,target.shape[0])
        return pltpu.make_async_remote_copy(src_ref=src,dst_ref=target.at[ring],
            send_sem=send_sem[stage].at[ring],recv_sem=recv_sem[stage].at[ring],
            device_id=peer[name],device_id_type=MESH)
    def receive(stage,kind,u):
        order=KINDS[kind]; name=order[stage]
        names=[n for n in NAMES if n not in order[:stage]]
        exchange(stage,kind,u).wait()
        buffers=part if stage==0 else kept[stage-1][order is SHARD_FIRST]
        own=pick(buffers,lax.rem(u,buffers.shape[0]),names,name,bit[name])
        target=came[stage][order is SHARD_FIRST]
        other=target.at[lax.rem(u,target.shape[0])]
        left_over=len(names)-1
        if stage<3:
            result=kept[stage][order is SHARD_FIRST]
            slot=lax.rem(u,result.shape[0])
        for flat in range(1<<left_over):
            where=tuple((flat>>k)&1 for k in reversed(range(left_over)))
            total=own[where].astype(jnp.float32)+other[where].astype(jnp.float32)
            if stage<3: result[(slot,)+where]=total.astype(low)
            else: final[lax.rem(u,final.shape[0])]=total.astype(low)
        if stage<3: exchange(stage+1,kind,u).start()
    grad_qkv,grad_wout,grad_fc1,grad_fc2=outs
    anywhere=grad_fc2.at[0,0,:,:WIDTH]
    def placed(u,kind,action):
        block=u//3
        def columns(first): return pl.ds(pl.multiple_of((block-first)*D+kind*WIDTH,128),WIDTH)
        here=slice(kind*WIDTH,(kind+1)*WIDTH)
        pl.when(block<4)(lambda: action(lambda who: grad_fc2.at[block,who,:,here]))
        pl.when((block>=4)&(block<8))(lambda: action(lambda who: grad_fc1.at[who,:,columns(4)]))
        pl.when(block==8)(lambda: action(lambda who: grad_wout.at[who,:,here]))
        pl.when(block>=9)(lambda: action(lambda who: grad_qkv.at[who,:,columns(9)]))
    def spread(u,target):
        src=final.at[lax.rem(u,final.shape[0])]
        return (pltpu.make_async_copy(src,target,final_sem.at[u]),
            pltpu.make_async_remote_copy(src_ref=src,dst_ref=target,send_sem=far_send.at[u],recv_sem=far_recv.at[u],
                device_id=peer["r1"],device_id_type=MESH),
            pltpu.make_async_remote_copy(src_ref=src,dst_ref=target,send_sem=near_send.at[u],recv_sem=near_recv.at[u],
                device_id=peer["r0"],device_id_type=MESH))
    def relay(u,piece):
        return pltpu.make_async_remote_copy(src_ref=piece,dst_ref=piece,send_sem=fwd_send.at[u],recv_sem=fwd_recv.at[u],
                device_id=peer["r0"],device_id_type=MESH)
    def compute(kind,block,u):
        slot=lax.rem(block,2)
        columns=right[slot,:,kind*WIDTH:(kind+1)*WIDTH]
        rows=left.shape[2]//4
        for shard in range(4):
            product=lax.dot_general(left[slot,shard],columns,(((1,),(0,)),((),())),preferred_element_type=jnp.float32)
            for rep in range(4):
                part[lax.rem(u,part.shape[0]),shard//2,shard%2,rep//2,rep%2]=product[rep*rows:(rep+1)*rows].astype(low)
        exchange(0,kind,u).start()

    total_steps=units+last+4
    iterations=-(-total_steps//3)
    def iteration(it,carry):
        @pl.when(it<blocks)
        def _():
            slot=lax.rem(it,2)
            pltpu.make_async_copy(left.at[slot],left.at[slot],left_sem.at[slot]).wait()
            pltpu.make_async_copy(right.at[slot],right.at[slot],right_sem.at[slot]).wait()
        for sub in range(3):
            step=3*it+sub
            def at(lag,action):
                kind=(sub-lag)%3
                unit=step-lag
                @pl.when((unit>=0)&(unit<units))
                def _(): action(kind,unit)
            def finish(kind,u):
                local,far,near=spread(u,anywhere)
                local.wait(); far.wait_send(); near.wait(); relay(u,anywhere).wait()
            at(last+3,finish)
            def pass_on(kind,u):
                spread(u,anywhere)[1].wait_recv()
                placed(u,kind,lambda where: relay(u,where(across)).start())
            at(last+2,pass_on)
            def finalize(kind,u):
                receive(3,kind,u)
                def start(where):
                    for copy in spread(u,where(r)): copy.start()
                placed(u,kind,start)
            at(ends[3],finalize)
            for stage in (2,1,0):
                at(ends[stage],functools.partial(receive,stage))
            if sub==0:
                load(it+1,lax.rem(it+1,2))
                pl.when(it==3)(share_notes)
            at(0,lambda kind,u: compute(kind,it,u))
        return carry
    lax.fori_loop(0,iterations,iteration,0)
    for index,(a,other) in enumerate(act_peers): act_copy(index,a,other).wait()
    act_out[...]=blocks_in[0]+blocks_in[1]

def unpack(refs):
    refs=list(refs)
    left,right,left_sem,right_sem,part=refs[:5]; refs=refs[5:]
    came=[(refs[0],refs[0]),(refs[1],refs[2]),(refs[3],refs[4]),(refs[5],refs[5])]; refs=refs[6:]
    send=refs[:4]; recv=refs[4:8]; refs=refs[8:]
    kept=[(refs[0],refs[0]),(refs[1],refs[2]),(refs[3],refs[4])]; refs=refs[5:]
    return (left,right,left_sem,right_sem,part,came,send,recv,kept,*refs)

def reduce_all(halves,grad_mods,act,ada):
    shards=lax.axis_size("shard"); reps=lax.axis_size("rep")
    rows=D//(shards*reps); group=D//shards
    blocks=12; units=3*blocks
    operands=[]
    for pairs in halves:
        (hidden,feed),(second,pre),(att,branch),(first,project)=pairs
        span=hidden.shape[0]
        operands+=[a.T.reshape(shards,group,span) for a in (first,second,att)]
        operands+=[hidden.T.reshape(shards,4,group,span),feed,pre,branch,project]
    tokens=2*span
    any_=pl.BlockSpec(memory_space=pl.ANY)
    piece=(rows,WIDTH)
    two=lambda count: (2,)*count+piece
    rings=[2*lag+1 for lag in LAGS]
    vm=lambda depth,shape: pltpu.VMEM((depth,)+shape,low)
    dma=pltpu.SemaphoreType.DMA
    keep=[lag+1 for lag in LAGS]
    inside=pl.BlockSpec(memory_space=pltpu.VMEM)
    batch=act.shape[0]; wide=7*D
    made=lambda shape,dtype: jax.ShapeDtypeStruct(shape,dtype)
    *grads,notes,act_grad=pl.pallas_call(functools.partial(reduce_kernel,blocks),
        in_specs=[any_]*16+[inside]*3+[any_],out_specs=[any_]*4+[inside,inside],
        out_shape=[made((reps,rows,3*D),low),made((reps,rows,D),low),made((reps,rows,4*D),low),made((4,reps,rows,D),low),
            made((shards*reps*batch,wide),low),made((shards,batch,group),jnp.float32)],
        scratch_shapes=[
            pltpu.VMEM((2,shards,group,tokens),low),pltpu.VMEM((2,tokens,D),low),dma((2,)),dma((2,)),
            vm(keep[0],two(4)),
            vm(rings[0],two(3)),vm(rings[1],two(2)),vm(rings[1],two(2)),vm(rings[2],two(1)),vm(rings[2],two(1)),vm(rings[3],two(0)),
            *[dma((ring,)) for ring in rings],*[dma((ring,)) for ring in rings],
            vm(keep[1],two(3)),vm(keep[2],two(2)),vm(keep[2],two(2)),vm(keep[3],two(1)),vm(keep[3],two(1)),
            vm(5,piece),
            *[dma((units,)) for _ in range(7)],dma((15,)),dma((15,)),
            pltpu.VMEM((shards*reps,batch,wide),low),pltpu.VMEM(ada.shape,low),dma(()),dma(()),
            pltpu.VMEM((shards,batch,group),jnp.float32),pltpu.VMEM((2,shards,batch,group),jnp.float32),dma((7,)),dma((7,)),pltpu.VMEM((batch,wide),low)],
        compiler_params=pltpu.CompilerParams(collective_id=2,has_side_effects=True),
        cost_estimate=pl.CostEstimate(flops=2*tokens*D*D*blocks,bytes_accessed=4*tokens*D*blocks,transcendentals=0),
        )(*operands,*grad_mods,act,ada)
    grads=[grad.reshape(-1,grad.shape[-1]).astype(jnp.float32) for grad in grads]
    return grads,notes,act_grad


def body(
    latents,
    cond,
    modulation_weight,
    query_key_value_weight,
    attention_output_weight,
    feed_first_weight,
    feed_second_weight,
    cotangent,
):
    first_section = lax.axis_index("section") == 0
    shard = lax.axis_index("shard")
    rep = lax.axis_index("rep")
    shards = lax.axis_size("shard")
    reps = lax.axis_size("rep")
    batch = latents.shape[0]
    modulation_weight = modulation_weight[0]
    rows = modulation_weight.shape[0]

    cond_float = cond.astype(jnp.float32)
    act = jax.nn.silu(cond_float).astype(low)
    blocks = act.reshape(batch, shards, rows).transpose(1, 0, 2)
    weights, total = gather_all(
        (
            query_key_value_weight[0],
            attention_output_weight[0],
            feed_first_weight[0],
            feed_second_weight[0],
        ),
        blocks,
        modulation_weight,
    )

    forth = [(0, 1)]
    back = [(1, 0)]
    first, second = (latents, 0), (latents, 1)
    straight, swapped = (0, 1), (1, 0)
    *_, sent = forward_layer((first, first), total, (0, 0), weights)
    inputs_one = (second, lax.ppermute(sent, "section", forth))
    *kept_one, result_one, sent = forward_layer(inputs_one, total, swapped, weights)
    incoming = lax.ppermute(sent, "section", forth)
    own = (cotangent, 0)
    *_, sent = backward_layer((own, own), total, swapped, inputs_one, kept_one, weights)
    returning = lax.ppermute(sent, "section", back)
    incoming, sent = lax.optimization_barrier((incoming, sent))
    inputs_two = (first, incoming)
    *kept_two, result_two, _ = forward_layer(inputs_two, total, straight, weights)
    mod_one, *grads_one, grad_in_one, sent = backward_layer(
        (returning, (cotangent, 1)), total, straight, inputs_two, kept_two, weights
    )
    returning = lax.ppermute(sent, "section", back)
    mod_two, *grads_two, grad_in_two, _ = backward_layer(
        (returning, (cotangent, 0)), total, swapped, inputs_one, kept_one, weights
    )

    def products(kept, grads):
        first_in, _, attended, _, _, second_in, _, hidden, _ = kept
        grad_feed, grad_pre, grad_branch, grad_project = grads
        return (
            (hidden, grad_feed),
            (second_in, grad_pre),
            (attended, grad_branch),
            (first_in, grad_project),
        )

    kept_one, kept_two, _ = lax.optimization_barrier((kept_one, kept_two, sent))
    pairs_one, pairs_two = products(kept_two, grads_one), products(kept_one, grads_two)
    wide = mod_one.shape[1]
    if shards == 4 and reps == 4:
        (grad_qkv, grad_wout, grad_fc1, grad_fc2), packed, act_grad = reduce_all(
            (pairs_one, pairs_two), (mod_one, mod_two), act, modulation_weight
        )
        act_total = act_grad.transpose(1, 0, 2).reshape(batch, shards * rows)
    else:
        pairs = [
            [jnp.concatenate(halves, axis=0) for halves in zip(one, two)]
            for one, two in zip(pairs_one, pairs_two)
        ]
        grad_fc2 = reduce_rows(*pairs[0], True)
        grad_fc1 = reduce_rows(*pairs[1], False)
        grad_wout = reduce_rows(*pairs[2], True)
        grad_qkv = reduce_rows(*pairs[3], True)
        grad_mod = jnp.where(
            first_section,
            jnp.concatenate([mod_one, mod_two], axis=0),
            jnp.concatenate([mod_two, mod_one], axis=0),
        ).astype(low)
        packed = jnp.concatenate([grad_mod, act], axis=-1)
        packed = lax.all_gather(packed, ("shard", "rep"), axis=0, tiled=True)
        own_mod = lax.dynamic_index_in_dim(
            packed[:, : wide].reshape(shards, reps, batch, -1), rep, 1, keepdims=False
        ).reshape(shards * batch, -1)
        act_grad = matmul_t(own_mod, modulation_weight)
        act_grad = act_grad + lax.ppermute(act_grad, "section", [(0, 1), (1, 0)])
        came = exchange_shards(act_grad.reshape(shards, batch, rows))
        act_total = jnp.zeros((shards, batch, rows), jnp.float32)
        for step, block in enumerate(came):
            act_total = lax.dynamic_update_index_in_dim(
                act_total, block, (shard - step) % shards, 0
            )
        act_total = act_total.transpose(1, 0, 2).reshape(batch, shards * rows)

    boundary = jnp.stack(
        [
            jnp.where(first_section, grad_in_one, result_one),
            jnp.where(first_section, grad_in_two, result_two),
        ]
    )[None]

    all_mod = packed[:, : wide]
    all_act = packed[:, wide :]
    act_rows = lax.dynamic_slice_in_dim(all_act, shard * rows, rows, 1)
    grad_ada = lax.dot_general(
        act_rows, all_mod, (((0,), (0,)), ((), ())), preferred_element_type=jnp.float32
    )
    _, silu_back = jax.vjp(jax.nn.silu, cond_float)
    grad_cond = silu_back(act_total)[0]
    return (
        boundary,
        grad_cond,
        grad_ada[None],
        grad_qkv[None],
        grad_wout[None],
        grad_fc1[None],
        grad_fc2[None],
    )


def solution(mesh):
    in_specs = (
        P(("shard", "rep"), None, None),
        P(("shard", "rep"), None),
        P("section", "shard", None),
        P("section", "shard", None),
        P("section", "shard", None),
        P("section", "shard", None),
        P("section", "shard", None),
        P(("shard", "rep"), None, None),
    )
    out_specs = (
        P("section", ("shard", "rep"), None, None),
        P(("shard", "rep"), None),
        P("section", "shard", None),
        P("section", "shard", None),
        P("section", "shard", None),
        P("section", "shard", None),
        P("section", "shard", None),
    )

    return jax.shard_map(body, mesh=mesh, in_specs=in_specs, out_specs=out_specs, check_vma=False)
```
